32 devices in a mesh: shell: 2 (over x), pix: 16 (over z, y, core).
Axes of the slice: x: 2, y: 2, z: 4, core: 2. Of those that a mesh axis runs over, the one named last changes fastest.
Arguments:
- block_tile: int32 [4, 1024], P('shell'), may hold values from 0 to 2047, as said below
- cell_index: int32 [4, 1024, 512], P('shell', 'pix'), may hold values from 0 to 2047
- masses: bfloat16 [4, 1024, 512], P('shell', 'pix'), may hold values from 0.125 to 8, as said below
- plane_coef: float32 [4], P('shell'), may hold values from 0.1 to 0.4
- plane_dist: float32 [4], P('shell'), may hold values from 0.2 to 1
- source_inv: float32 [4], P('shell'), may hold values from 0.5 to 1
Outputs:
- convergence: float32 [4, 2048, 2048], P('shell', 'pix')
- shear_one: float32 [4, 2048, 2048], P('shell', 'pix')
- shear_two: float32 [4, 2048, 2048], P('shell', 'pix')
The draws below stay inside these ranges and needn't reach their ends.
Inputs may be any that keep to these rules, and one draw needn't show every extreme that they name: `block_tile`: each row is 16 aligned runs of 64 entries, one run per index of pix. The entries of a run are distinct, and at most 8 of them lie in one index's rows of tiles (tile b lies in the rows of index b // 128). In every plane some index receives exactly 8 tiles from every run. `masses`: positive particle weights.
All inputs are finite; a program needn't handle non-finite values.
Results may differ from the reference program's by a relative error of at most 0.0003.
Values sent between devices are 32-bit elements; how exact they have to be, the bound alone decides.
A program may use at most 64 MiB of HBM per device.

```python
import math
import jax
import jax.numpy as jnp
from jax import lax

L = 2048
TR = 16
TC = 128
LT = 64
BPT = 4
PLANES = 4
TILES = 2048
TPO = 128
CAP = 8
N_PIX = 16


def draw_block_tile(key, part):
    owners = TILES // TPO
    slot_count = owners * CAP
    key_full = jax.random.fold_in(key, 11)
    key_order = jax.random.fold_in(key, 12)
    key_base = jax.random.fold_in(key, 13)
    full_owner = jax.random.randint(key_full, (PLANES, 1, 1), 0, owners)
    slot_ids = jnp.arange(slot_count)
    scores = jax.random.randint(key_order, (PLANES, owners, slot_count), 0, 1 << 20) * slot_count + slot_ids
    scores = jnp.where((slot_ids // CAP)[None, None, :] == full_owner, scores - (1 << 30), scores)
    chosen = jnp.argsort(scores, axis=-1)[:, :, :LT]
    owner_id = chosen // CAP
    rank_id = chosen % CAP
    base = jax.random.randint(key_base, (PLANES, owners, owners), 0, TPO)
    offset = jnp.take_along_axis(base, owner_id, axis=-1)
    tile_id = owner_id * TPO + (offset + rank_id) % TPO
    return tile_id.reshape(PLANES, owners * LT).astype(jnp.int32)


def draw_masses(key, part):
    owners = TILES // TPO
    scale_key = jax.random.fold_in(key, 21)
    single_key = jax.random.fold_in(key, 22)
    device_scale = jnp.exp(jax.random.uniform(scale_key, (PLANES, owners, 1, 1), jnp.float32, math.log(0.25), math.log(4.0)))
    particle = jnp.exp(jax.random.uniform(single_key, (PLANES, owners, LT, BPT * 128), jnp.float32, math.log(0.5), math.log(2.0)))
    return (device_scale * particle).reshape(PLANES, owners * LT, BPT * 128).astype(jnp.bfloat16)


def place_ends(result, own_key, low, high):
    extent = result.shape
    index_at = [jax.random.randint(jax.random.fold_in(own_key, axis), (), 0, extent[axis]) for axis in range(len(extent))]
    result = result.at[tuple(index_at)].set(low)
    longest = extent.index(max(extent))
    index_at[longest] = (index_at[longest] + 1) % extent[longest]
    return result.at[tuple(index_at)].set(high)


def levels(key, shape, split, least, top_value):
    factor_of = 1.0
    for axis_at, parts in split:
        heights = jax.random.uniform(jax.random.fold_in(jax.random.fold_in(key, 6), axis_at), (parts,), jnp.float32, least / len(split), top_value / len(split))
        factor_of = factor_of * jnp.repeat(jnp.exp(heights), shape[axis_at] // parts).reshape((-1,) + (1,) * (len(shape) - 1 - axis_at))
    return factor_of


def setup_inputs(seed: int = 0) -> dict:
    splits = jax.random.split(jax.random.key(seed), 7)
    return {
        "block_tile": draw_block_tile(jax.random.fold_in(splits[6], 71), 0),
        "cell_index": place_ends(jax.random.randint(splits[1], (PLANES, N_PIX * LT, BPT * 128), 0, TR * TC), jax.random.fold_in(splits[1], 1), 0, (TR * TC) - 1).astype(jnp.int32),
        "masses": draw_masses(jax.random.fold_in(splits[6], 71), 0),
        "plane_coef": jnp.clip(jnp.exp(math.log(0.4) - 1.3862944 * jax.random.uniform(splits[3], (PLANES,), jnp.float32) ** levels(splits[3], (PLANES,), ((0, 2),), -0.2, 0.2)), 0.1, 0.4),
        "plane_dist": jnp.clip(jnp.exp(math.log(1.0) - 1.609438 * jax.random.uniform(splits[4], (PLANES,), jnp.float32) ** levels(splits[4], (PLANES,), ((0, 2),), -0.2, 0.2)), 0.2, 1.0),
        "source_inv": jnp.clip(jnp.exp(math.log(1.0) - 0.6931472 * jax.random.uniform(splits[5], (PLANES,), jnp.float32) ** levels(splits[5], (PLANES,), ((0, 2),), -0.2, 0.2)), 0.5, 1.0),
    }


def reference(block_tile, cell_index, masses, plane_coef, plane_dist, source_inv):
    tiles_wide = L // TC

    def deposit(item):
        tile_ids, cell_ids, weights = item
        tile_col = tile_ids[:, None]
        pixel_row = (tile_col // tiles_wide) * TR + cell_ids // TC
        pixel_col = (tile_col % tiles_wide) * TC + cell_ids % TC
        flat_index = (pixel_row * L + pixel_col).reshape(-1).astype(jnp.int32)
        plane_sum = jnp.zeros((L * L,), jnp.float32).at[flat_index].add(weights.reshape(-1).astype(jnp.float32))
        plane_sum = plane_sum.reshape(L, L)
        mean_mass = jnp.sum(plane_sum) / (L * L)
        return plane_sum / mean_mass - 1.0

    contrast = lax.map(deposit, (block_tile, cell_index, masses))
    near_sum = jnp.cumsum(plane_coef[:, None, None] * contrast, axis=0)
    far_sum = jnp.cumsum((plane_coef * plane_dist)[:, None, None] * contrast, axis=0)
    convergence = near_sum - source_inv[:, None, None] * far_sum

    frequency = jnp.arange(L)
    signed = jnp.where(frequency >= L // 2, frequency - L, frequency).astype(jnp.float32)
    keep_mask = (frequency != L // 2).astype(jnp.float32)
    wave_x = signed[None, :]
    wave_y = signed[:, None]
    wave_power = jnp.maximum(wave_x * wave_x + wave_y * wave_y, 1.0)
    both_keep = keep_mask[None, :] * keep_mask[:, None]
    kernel_one = both_keep * (wave_x * wave_x - wave_y * wave_y) / wave_power
    kernel_two = both_keep * 2.0 * wave_x * wave_y / wave_power

    def shear(field):
        spectrum = jnp.fft.fft2(field)
        first = jnp.real(jnp.fft.ifft2(spectrum * kernel_one)).astype(jnp.float32)
        second = jnp.real(jnp.fft.ifft2(spectrum * kernel_two)).astype(jnp.float32)
        return first, second

    shear_one, shear_two = lax.map(shear, convergence)
    return convergence, shear_one, shear_two
```

```python
from functools import partial
import math

import jax
import jax.numpy as jnp
from jax import lax
from jax.experimental import pallas as pl
from jax.experimental.pallas import tpu as pltpu
from jax.sharding import PartitionSpec as P
import numpy as np

L = 2048
TR = 16
TC = 128


HIGHEST = lax.Precision.HIGHEST


def entering(value, axis, join, neutral):
    count, mine = (lax.axis_size(axis), lax.axis_index(axis))
    pieces = jax.tree.map(lambda part: lax.all_gather(part, axis), value)
    running = jax.tree.map(
        lambda part, zero: jnp.full_like(part, 0) + jnp.asarray(zero, part.dtype), value, neutral
    )

    def lap(position, running):
        longer = join(running, jax.tree.map(lambda part: part[position], pieces))
        return jax.tree.map(lambda new, old: jnp.where(position < mine, new, old), longer, running)

    return lax.fori_loop(0, count - 1, lap, running)


def dft_table(left_size, right_size, period, sign_value):
    left_idx = jnp.arange(left_size)[:, None]
    right_idx = jnp.arange(right_size)[None, :]
    angle = 2.0 * math.pi / period * (left_idx * right_idx % period).astype(jnp.float32)
    return (jnp.cos(angle), sign_value * jnp.sin(angle))


def mix_outer(table, real_part, imag_part):
    cosine, sine_part = table
    contract = partial(jnp.einsum, "ab,...bc->...ac", precision=HIGHEST)
    return (
        contract(cosine, real_part) - contract(sine_part, imag_part),
        contract(sine_part, real_part) + contract(cosine, imag_part),
    )


def mix_inner(table, real_part, imag_part):
    cosine, sine_part = table
    product = partial(jnp.matmul, precision=HIGHEST)
    return (
        product(real_part, cosine) - product(imag_part, sine_part),
        product(real_part, sine_part) + product(imag_part, cosine),
    )


def twist(table, real_part, imag_part):
    cosine, sine_part = table
    return (real_part * cosine - imag_part * sine_part, real_part * sine_part + imag_part * cosine)


def transform_last(real_part, imag_part, sign_value):
    length = real_part.shape[-1]
    inner = math.gcd(length, 128)
    outer = length // inner
    leading = real_part.shape[:-1]
    real_part = real_part.reshape(leading + (outer, inner))
    imag_part = imag_part.reshape(leading + (outer, inner))
    outer_table = dft_table(outer, outer, outer, sign_value)
    inner_table = dft_table(inner, inner, inner, sign_value)
    twiddle = dft_table(outer, inner, length, sign_value)
    if sign_value < 0:
        real_part, imag_part = mix_outer(outer_table, real_part, imag_part)
        real_part, imag_part = twist(twiddle, real_part, imag_part)
        real_part, imag_part = mix_inner(inner_table, real_part, imag_part)
    else:
        real_part, imag_part = mix_inner(inner_table, real_part, imag_part)
        real_part, imag_part = twist(twiddle, real_part, imag_part)
        real_part, imag_part = mix_outer(outer_table, real_part, imag_part)
    return (real_part.reshape(leading + (length,)), imag_part.reshape(leading + (length,)))


def frequency_of(position, length):
    inner = math.gcd(length, 128)
    outer = length // inner
    frequency = position // inner + outer * (position % inner)
    signed = jnp.where(frequency >= length // 2, frequency - length, frequency).astype(jnp.float32)
    keep_mask = (frequency != length // 2).astype(jnp.float32)
    return (signed, keep_mask)


def add_pairs(earlier_pair, later_pair):
    return (earlier_pair[0] + later_pair[0], earlier_pair[1] + later_pair[1])


def deposit_group(item):
    cell_ids, weights = item
    tile_rows = cell_ids // TC
    tile_cols = cell_ids % TC
    row_hot = jnp.where(
        tile_rows[:, None, :] == jnp.arange(TR)[None, :, None],
        weights[:, None, :],
        jnp.zeros((), jnp.bfloat16),
    )
    col_hot = (tile_cols[:, :, None] == jnp.arange(TC)[None, None, :]).astype(jnp.bfloat16)
    return jnp.einsum("grk,gkc->grc", row_hot, col_hot, preferred_element_type=jnp.float32)


def rows_to_sending(packed, groups, slab, cols_own):
    count, fields = (packed.shape[0], packed.shape[1])
    return (
        packed.reshape(count, fields, slab, groups, cols_own)
        .transpose(3, 0, 1, 4, 2)
        .reshape(groups, count, fields, cols_own * slab)
    )


def arrived_to_columns(arrived, groups, slab, cols_own):
    count, fields = (arrived.shape[1], arrived.shape[2])
    return (
        arrived.reshape(groups, count, fields, cols_own, slab)
        .transpose(1, 2, 3, 0, 4)
        .reshape(count, fields, cols_own, groups * slab)
    )


def columns_to_sending(stacked, groups, slab, cols_own):
    count, fields = (stacked.shape[0], stacked.shape[1])
    return (
        stacked.reshape(count, fields, cols_own, groups, slab)
        .transpose(3, 0, 1, 2, 4)
        .reshape(groups, count, fields, cols_own * slab)
    )


def landed_to_rows(landed, groups, slab, cols_own):
    count, fields = (landed.shape[1], landed.shape[2])
    return (
        landed.reshape(groups, count, fields, cols_own, slab)
        .transpose(1, 2, 4, 0, 3)
        .reshape(count, fields, slab, groups * cols_own)
    )


def local(block_tile, cell_index, masses, plane_coef, plane_dist, source_inv):
    groups = lax.axis_size("pix")
    my_index = lax.axis_index("pix")
    planes, local_tiles, per_tile = cell_index.shape
    slab = L // groups
    per_owner = slab // TR * (L // TC)
    cap = max(1, 2 * local_tiles // groups)
    flat = TR * TC
    batch_tiles = 8
    deposited = lax.map(
        deposit_group,
        (cell_index.reshape(-1, batch_tiles, per_tile), masses.reshape(-1, batch_tiles, per_tile)),
    )
    tile_sums = deposited.reshape(planes, local_tiles, flat)
    table = block_tile.reshape(planes, groups, local_tiles)
    owner = table // per_owner
    earlier = jnp.arange(local_tiles)[:, None] < jnp.arange(local_tiles)[None, :]
    same_owner = owner[:, :, :, None] == owner[:, :, None, :]
    rank = jnp.sum(jnp.where(same_owner & earlier[None, None], 1, 0), axis=2)
    slot = owner * cap + rank
    my_slots = lax.dynamic_index_in_dim(slot, my_index, axis=1, keepdims=False)
    slot_grid = jnp.arange(groups)[:, None] * cap + jnp.arange(cap)[None, :]
    send_hot = (my_slots[:, None, None, :] == slot_grid[None, :, :, None]).astype(jnp.float32)
    outgoing = jnp.einsum("pnct,ptf->npcf", send_hot, tile_sums, precision=HIGHEST)
    incoming = lax.all_to_all(outgoing, "pix", split_axis=0, concat_axis=0, tiled=True)
    local_index = table - my_index * per_owner
    is_mine = owner == my_index
    tile_hot = (is_mine[..., None] & (local_index[..., None] == jnp.arange(per_owner))).astype(
        jnp.float32
    )
    slot_hot = (rank[..., None] == jnp.arange(cap)).astype(jnp.float32)
    placing = jnp.einsum("pstl,pstc->plsc", tile_hot, slot_hot, precision=HIGHEST)
    slab_tiles = jnp.einsum("plsc,spcf->plf", placing, incoming, precision=HIGHEST)
    density = (
        slab_tiles.reshape(planes, slab // TR, L // TC, TR, TC)
        .transpose(0, 1, 3, 2, 4)
        .reshape(planes, slab, L)
    )
    total = lax.psum(jnp.sum(density, axis=(1, 2)), "pix")
    contrast = density / (total / (L * L))[:, None, None] - 1.0
    near_local = jnp.cumsum(plane_coef[:, None, None] * contrast, axis=0)
    far_local = jnp.cumsum((plane_coef * plane_dist)[:, None, None] * contrast, axis=0)
    blank = jnp.zeros((slab, L), jnp.float32)
    near_before, far_before = entering(
        (near_local[-1], far_local[-1]), "shell", add_pairs, (blank, blank)
    )
    convergence = near_before + near_local - source_inv[:, None, None] * (far_before + far_local)
    cols_own = L // groups
    wave_x, keep_x = frequency_of(my_index * cols_own + jnp.arange(cols_own), L)
    wave_y, keep_y = frequency_of(jnp.arange(L), L)
    wave_x = wave_x[:, None]
    wave_y = wave_y[None, :]
    both_keep = keep_x[:, None] * keep_y[None, :]
    wave_power = jnp.maximum(wave_x * wave_x + wave_y * wave_y, 1.0)
    kernel_one = both_keep * (wave_x * wave_x - wave_y * wave_y) / wave_power
    kernel_two = both_keep * 2.0 * wave_x * wave_y / wave_power
    scale = 1.0 / (L * L)
    spec_real, spec_imag = transform_last(convergence[0::2], convergence[1::2], -1.0)
    sending = rows_to_sending(jnp.stack([spec_real, spec_imag], axis=1), groups, slab, cols_own)
    arrived = lax.all_to_all(sending, "pix", split_axis=0, concat_axis=0, tiled=True)
    columns = arrived_to_columns(arrived, groups, slab, cols_own)
    row_real, row_imag = transform_last(columns[:, 0], columns[:, 1], -1.0)
    first_real, first_imag = transform_last(row_real * kernel_one, row_imag * kernel_one, 1.0)
    second_real, second_imag = transform_last(row_real * kernel_two, row_imag * kernel_two, 1.0)
    stacked = jnp.stack([first_real, first_imag, second_real, second_imag], axis=1)
    landed = lax.all_to_all(
        columns_to_sending(stacked, groups, slab, cols_own),
        "pix",
        split_axis=0,
        concat_axis=0,
        tiled=True,
    )
    row_layout = landed_to_rows(landed, groups, slab, cols_own)
    even_one, odd_one = transform_last(row_layout[:, 0], row_layout[:, 1], 1.0)
    even_two, odd_two = transform_last(row_layout[:, 2], row_layout[:, 3], 1.0)
    shear_one = jnp.stack([even_one, odd_one], axis=1).reshape(planes, slab, L)
    shear_two = jnp.stack([even_two, odd_two], axis=1).reshape(planes, slab, L)
    return (convergence, shear_one * scale, shear_two * scale)


INNER = 128
OUTER = L // INNER
HALF_BLOCKS = OUTER // 2
CHUNKS = 4
MESH = pl.DeviceIdType.MESH


def block_columns():
    cols = np.zeros((HALF_BLOCKS, INNER), np.int64)
    for b in range(HALF_BLOCKS - 1):
        cols[b] = b + 1 + OUTER * np.arange(INNER)
    half = np.arange(INNER // 2)
    cols[-1] = np.concatenate([OUTER * half, HALF_BLOCKS + OUTER * half])
    return cols


def split_table(table):
    high = table.astype(jnp.bfloat16)
    low = (table - high.astype(np.float64)).astype(jnp.bfloat16)
    return high, low


def row_tables():
    n2 = np.arange(INNER)
    out = np.zeros((HALF_BLOCKS, 2 * INNER, 2 * INNER))
    cols = block_columns()
    for b in range(HALF_BLOCKS):
        angle = 2 * np.pi / L * ((n2[:, None] * cols[b][None, :]) % L)
        co, si = np.cos(angle), np.sin(angle)
        if b < HALF_BLOCKS - 1:
            out[b] = np.block([[co, -si], [si, co]])
        else:
            h = INNER // 2
            out[b, :INNER, :h] = co[:, :h]
            out[b, :INNER, INNER : INNER + h] = -si[:, :h]
            out[b, INNER:, h:INNER] = co[:, h:]
            out[b, INNER:, INNER + h :] = -si[:, h:]
    return split_table(out)


def column_tables():
    idx = np.arange(INNER)
    angle = 2 * np.pi / INNER * ((idx[:, None] * idx[None, :]) % INNER)
    co, si = np.cos(angle), np.sin(angle)
    return split_table(np.block([[co, si], [-si, co]]))


def twiddle_tables():
    angle = 2 * np.pi / L * (np.arange(OUTER)[:, None] * np.arange(INNER)[None, :])
    return np.cos(angle).astype(np.float32), (-np.sin(angle)).astype(np.float32)


def times_root(value, k, n, sign):
    re, im = value
    k = k % n
    if k == 0:
        return value
    if 4 * k == n:
        return (-im, re) if sign > 0 else (im, -re)
    angle = 2 * math.pi * k / n
    c, s = math.cos(angle), sign * math.sin(angle)
    if 8 * k == n or 8 * k == 3 * n:
        if c > 0:
            return ((re - im) * c, (re + im) * c) if sign > 0 else ((re + im) * c, (im - re) * c)
        c = -c
        return ((re + im) * -c, (re - im) * c) if sign > 0 else ((im - re) * c, (re + im) * -c)
    return (re * c - im * s, re * s + im * c)


def fft_list(values, sign):
    n = len(values)
    if n == 1:
        return values
    even = fft_list(values[0::2], sign)
    odd = fft_list(values[1::2], sign)
    odd = [times_root(v, k, n, sign) for k, v in enumerate(odd)]
    return [(a[0] + b[0], a[1] + b[1]) for a, b in zip(even, odd)] + [
        (a[0] - b[0], a[1] - b[1]) for a, b in zip(even, odd)
    ]


def split_value(value):
    high = value.astype(jnp.bfloat16)
    return high, (value - high.astype(jnp.float32)).astype(jnp.bfloat16)


def three_pass(left, right, dims):
    dot = lambda a, b: lax.dot_general(a, b, (dims, ((), ())), preferred_element_type=jnp.float32)
    return dot(left[0], right[0]) + (dot(left[0], right[1]) + dot(left[1], right[0]))


def pack_kernel(slot_ref, list_ref, *out_refs):
    planes, tiles, size, _ = list_ref.shape
    groups, rows, _ = out_refs[0].shape
    cap = rows // size - 1
    for p in range(planes):
        out_ref = out_refs[p]
        out_ref[...] = jnp.zeros_like(out_ref)
        total = jnp.sum(list_ref[p, :, size // 2 :, :], axis=(0, 1))
        total = jnp.sum(total.reshape(1, TC), axis=1, keepdims=True)
        out_ref[:, cap * size :, :] = jnp.broadcast_to(total[None], (groups, size, TC))

        def tile(t, _):
            slot = slot_ref[p, t]
            rows_at = pl.ds(pl.multiple_of((slot % cap) * size, size), size)
            out_ref[slot // cap, rows_at, :] = list_ref[p, t]
            return 0

        lax.fori_loop(0, tiles, tile, 0)


def assemble_kernel(size, mix_ref, *refs):
    count = (len(refs) - 2) // 2
    places, lists = refs[:count], refs[count : 2 * count]
    conv_ref, held = refs[2 * count :]
    groups, rows, _ = lists[0].shape
    cap = rows // size - 1
    tiles = held.shape[1] - 1
    half = size // 2
    held[...] = jnp.zeros_like(held)
    as_small = lambda ids: ids.astype(jnp.float32).astype(jnp.bfloat16)
    row_id = as_small(lax.broadcasted_iota(jnp.int32, (TR, TC), 0))
    col_id = as_small(lax.broadcasted_iota(jnp.int32, (TC, TC), 0))
    one, zero = jnp.ones((), jnp.bfloat16), jnp.zeros((), jnp.bfloat16)
    factors = []
    for q in range(count):
        place_ref, in_ref = places[q], lists[q]

        def source(s, _):
            for c in range(cap):
                at = place_ref[s * cap + c]
                entry = in_ref[s, c * size : (c + 1) * size, :]
                cells = entry[:half].astype(jnp.int32)
                cell_rows, cell_cols = as_small(cells // TC), as_small(cells % TC)
                weights = entry[half:].astype(jnp.bfloat16)
                row_hot, col_hot = [], []
                for i in range(half):
                    row_hot.append(jnp.where(row_id == cell_rows[i : i + 1], weights[i : i + 1], zero))
                    col_hot.append(jnp.where(col_id == cell_cols[i : i + 1], one, zero))
                held[q, at] = held[q, at] + lax.dot_general(
                    jnp.concatenate(row_hot, axis=1),
                    jnp.concatenate(col_hot, axis=1),
                    (((1,), (1,)), ((), ())),
                    preferred_element_type=jnp.float32,
                )
            return 0

        lax.fori_loop(0, groups, source, 0)
        total = in_ref[0, cap * size : cap * size + 1, 0:1]
        for s in range(1, groups):
            total = total + in_ref[s, cap * size : cap * size + 1, 0:1]
        factors.append((L * L) / total)

    def chunk(t, _):
        rows = pl.ds(pl.multiple_of(t * TR, TR), TR)
        for n in range(OUTER):
            at = t * OUTER + n
            fields = [held[q, at] * factors[q] - 1.0 for q in range(count)]
            for i in range(conv_ref.shape[0]):
                value = mix_ref[i, 0] * fields[0]
                for j in range(1, count):
                    value = value + mix_ref[i, j] * fields[j]
                conv_ref[i, rows, n * INNER : (n + 1) * INNER] = value
        return 0

    lax.fori_loop(0, tiles // OUTER, chunk, 0)


def signal_all(peers):
    barrier = pltpu.get_barrier_semaphore()
    for peer in peers:
        pl.semaphore_signal(barrier, inc=1, device_id=peer, device_id_type=MESH)
    pl.semaphore_wait(barrier, len(peers))


def swap_lists_kernel(*refs):
    planes = (len(refs) - 5) // 3
    out_refs, in_refs, far_refs = refs[:planes], refs[planes : 2 * planes], refs[2 * planes : 3 * planes]
    send, recv, pass_send, pass_recv, own_sem = refs[3 * planes :]
    groups = out_refs[0].shape[0]
    me, shell = lax.axis_index("pix"), lax.axis_index("shell")
    signal_all([{"pix": (me + o) % groups} for o in range(1, groups)] + [{"shell": 1 - shell}])

    def direct(p, o):
        to = (me + o) % groups
        return pltpu.make_async_remote_copy(
            src_ref=out_refs[p].at[to],
            dst_ref=in_refs[p].at[me],
            send_sem=send.at[p, o],
            recv_sem=recv.at[p, o],
            device_id={"pix": to},
            device_id_type=MESH,
        )

    def landing(p, o):
        source = (me + groups - o) % groups
        return pltpu.make_async_remote_copy(
            src_ref=out_refs[p].at[source],
            dst_ref=in_refs[p].at[source],
            send_sem=send.at[p, o],
            recv_sem=recv.at[p, o],
            device_id={"pix": source},
            device_id_type=MESH,
        )

    def onward(p, o):
        source = (me + groups - o) % groups
        return pltpu.make_async_remote_copy(
            src_ref=in_refs[p].at[source],
            dst_ref=far_refs[p].at[source],
            send_sem=pass_send.at[p, o],
            recv_sem=pass_recv.at[p, o],
            device_id={"shell": 1 - shell},
            device_id_type=MESH,
        )

    def own(p):
        return pltpu.make_async_copy(out_refs[p].at[me], in_refs[p].at[me], own_sem.at[p])

    for p in range(planes):
        for j in range(1, groups):
            direct(p, (j + groups // 2 - 1) % (groups - 1) + 1).start()
        own(p).start()
    for p in range(planes):
        own(p).wait()
        onward(p, 0).start()
        for j in range(1, groups):
            o = (j + groups // 2 - 1) % (groups - 1) + 1
            landing(p, o).wait_recv()
            onward(p, o).start()
    for p in range(planes):
        for o in range(groups):
            onward(p, o).wait()
            if o:
                direct(p, o).wait_send()


def shear_kernel(
    conv_ref, col_ref, twr_ref, twi_ref, high_ref, low_ref, colh_ref, coll_ref, backh_ref, backl_ref,
    one_ref, two_ref, held_row, sending, arrived, held, twist_in, kern, back, leaving, landed, held_inv,
    fsend, frecv, rsend, rrecv,
):
    groups, _, slab, _ = sending.shape
    span = held_row.shape[2]
    chunks = slab // span
    me = lax.axis_index("pix")
    signal_all([{"pix": (me + o) % groups} for o in range(1, groups)])

    def rows_of(c):
        return pl.ds(pl.multiple_of(c * span, span), span)

    def go_copy(c, o, peer, slot):
        return pltpu.make_async_remote_copy(
            src_ref=sending.at[peer, :, rows_of(c), :],
            dst_ref=arrived.at[slot, :, rows_of(c), :],
            send_sem=fsend.at[c, o],
            recv_sem=frecv.at[c, o],
            device_id={"pix": peer},
            device_id_type=MESH,
        )

    def back_copy(f, c, o, peer, slot):
        return pltpu.make_async_remote_copy(
            src_ref=leaving.at[peer, f, :, rows_of(c), :],
            dst_ref=landed.at[slot, f, :, rows_of(c), :],
            send_sem=rsend.at[f, c, o],
            recv_sem=rrecv.at[f, c, o],
            device_id={"pix": peer},
            device_id_type=MESH,
        )

    def to_peer(o):
        return (me + o) % groups

    def from_peer(o):
        return (me + groups - o) % groups

    def each_peer(action):
        def step(j, _):
            action((j + groups // 2 - 1) % (groups - 1) + 1)
            return 0

        lax.fori_loop(1, groups, step, 0)

    def forward_rows(c, _):
        def radix(t, _):
            rows = pl.ds(pl.multiple_of(c * span + t * 8, 8), 8)
            near = pl.ds(pl.multiple_of(t * 8, 8), 8)
            z = fft_list(
                [
                    tuple(conv_ref[i, rows, n * INNER : (n + 1) * INNER] for i in range(2))
                    for n in range(OUTER)
                ],
                -1,
            )
            for k in range(1, HALF_BLOCKS):
                (ar, ai), (br, bi) = z[k], z[OUTER - k]
                held_row[k - 1, 0, near, :INNER] = 0.5 * (ar + br)
                held_row[k - 1, 0, near, INNER:] = 0.5 * (ai - bi)
                held_row[k - 1, 1, near, :INNER] = 0.5 * (ai + bi)
                held_row[k - 1, 1, near, INNER:] = 0.5 * (br - ar)
            for p in range(2):
                held_row[HALF_BLOCKS - 1, p, near, :INNER] = z[0][p]
                held_row[HALF_BLOCKS - 1, p, near, INNER:] = z[HALF_BLOCKS][p]
            return 0

        lax.fori_loop(0, span // 8, radix, 0)

        def block(j, _):
            b = (me // 2 + 1 + j) % HALF_BLOCKS
            value = held_row[b].reshape(2 * span, 2 * INNER)
            result = three_pass(split_value(value), (high_ref[b], low_ref[b]), ((1,), (0,)))
            for p in range(2):
                for half in range(2):
                    sending[2 * b + p, half, rows_of(c), :] = result[
                        p * span : (p + 1) * span, half * INNER : (half + 1) * INNER
                    ]
            return 0

        lax.fori_loop(0, HALF_BLOCKS, block, 0)
        each_peer(lambda o: go_copy(c, o, to_peer(o), me).start())
        for half in range(2):
            arrived[me, half, rows_of(c), :] = sending[me, half, rows_of(c), :]
        return 0

    lax.fori_loop(0, chunks, forward_rows, 0)

    signed_v = col_ref[0:1]
    weight = col_ref[1:2]
    inner_id = lax.broadcasted_iota(jnp.int32, (INNER, INNER), 0)

    def prepare(k, _):
        for i, ref in enumerate((twr_ref, twi_ref)):
            twist_in[i, k] = jnp.broadcast_to(ref[pl.ds(k, 1), :], (INNER, INNER)).T
        u = k + OUTER * inner_id
        signed_u = jnp.where(u >= L // 2, u - L, u).astype(jnp.float32)
        scale = jnp.where(u == L // 2, 0.0, weight)
        uu, vv = signed_u * signed_u, signed_v * signed_v
        over = scale / jnp.maximum(uu + vv, 1.0)
        kern[0, k] = (vv - uu) * over
        kern[1, k] = 2.0 * signed_v * signed_u * over
        return 0

    lax.fori_loop(0, OUTER, prepare, 0)

    def forward_columns(c, _):
        each_peer(lambda o: go_copy(c, o, from_peer(o), from_peer(o)).wait_recv())

        def radix(t, _):
            rows = pl.ds(pl.multiple_of(c * span + t * 8, 8), 8)
            z = fft_list([(arrived[n, 0, rows, :], arrived[n, 1, rows, :]) for n in range(OUTER)], -1)
            for k in range(OUTER):
                re, im = z[k]
                if k:
                    cs, sn = twist_in[0, k, rows, :], twist_in[1, k, rows, :]
                    re, im = re * cs - im * sn, re * sn + im * cs
                held[k, 0, rows, :] = re
                held[k, 1, rows, :] = im
            return 0

        lax.fori_loop(0, span // 8, radix, 0)
        return 0

    lax.fori_loop(0, chunks, forward_columns, 0)

    def middle(j, _):
        pair = jnp.concatenate([held[2 * j + i].reshape(2 * INNER, INNER) for i in range(2)], axis=1)
        spectrum = three_pass((colh_ref[...], coll_ref[...]), split_value(pair), ((1,), (0,)))
        for i in range(2):
            k = 2 * j + i
            mine = spectrum[:, i * INNER : (i + 1) * INNER]
            fields = jnp.concatenate(
                [
                    jnp.concatenate([mine[:INNER] * kern[f, k], mine[INNER:] * kern[f, k]], axis=0)
                    for f in range(2)
                ],
                axis=1,
            )
            result = three_pass((backh_ref[...], backl_ref[...]), split_value(fields), ((1,), (0,)))
            cs, sn = twist_in[0, k], twist_in[1, k]
            for f in range(2):
                at = slice(f * INNER, (f + 1) * INNER)
                re, im = result[:INNER, at], result[INNER:, at]
                back[f, k, 0] = re * cs + im * sn
                back[f, k, 1] = im * cs - re * sn
        return 0

    lax.fori_loop(0, OUTER // 2, middle, 0)

    def inverse_columns(q, _):
        f, c = q // chunks, q % chunks

        def radix(t, _):
            rows = pl.ds(pl.multiple_of(c * span + t * 8, 8), 8)
            x = fft_list([(back[f, k, 0, rows, :], back[f, k, 1, rows, :]) for k in range(OUTER)], 1)
            for n in range(OUTER):
                leaving[n, f, 0, rows, :] = x[n][0]
                leaving[n, f, 1, rows, :] = x[n][1]
            return 0

        lax.fori_loop(0, span // 8, radix, 0)
        each_peer(lambda o: back_copy(f, c, o, to_peer(o), me).start())
        for part in range(2):
            landed[me, f, part, rows_of(c), :] = leaving[me, f, part, rows_of(c), :]
        return 0

    lax.fori_loop(0, 2 * chunks, inverse_columns, 0)

    for f, out_ref in enumerate((one_ref, two_ref)):

        def inverse_rows(c, _):
            each_peer(lambda o: back_copy(f, c, o, from_peer(o), from_peer(o)).wait_recv())

            def block(b, _):
                value = jnp.concatenate(
                    [
                        jnp.concatenate(
                            [landed[2 * b + p, f, part, rows_of(c), :] for part in range(2)], axis=1
                        )
                        for p in range(2)
                    ],
                    axis=0,
                )
                held_inv[b] = three_pass(
                    split_value(value), (high_ref[b], low_ref[b]), ((1,), (1,))
                ).reshape(2, span, 2 * INNER)
                return 0

            lax.fori_loop(0, HALF_BLOCKS, block, 0)

            def radix(t, _):
                near = pl.ds(pl.multiple_of(t * 8, 8), 8)
                rows = pl.ds(pl.multiple_of(c * span + t * 8, 8), 8)
                z = [None] * OUTER
                last = HALF_BLOCKS - 1
                z[0] = (held_inv[last, 0, near, :INNER], held_inv[last, 1, near, :INNER])
                z[HALF_BLOCKS] = (held_inv[last, 0, near, INNER:], held_inv[last, 1, near, INNER:])
                for k in range(1, HALF_BLOCKS):
                    ar, ai = held_inv[k - 1, 0, near, :INNER], held_inv[k - 1, 0, near, INNER:]
                    br, bi = held_inv[k - 1, 1, near, :INNER], held_inv[k - 1, 1, near, INNER:]
                    z[k] = (ar - bi, ai + br)
                    z[OUTER - k] = (ar + bi, br - ai)
                x = fft_list(z, 1)
                for n in range(OUTER):
                    for p in range(2):
                        out_ref[p, rows, n * INNER : (n + 1) * INNER] = x[n][p]
                return 0

            lax.fori_loop(0, span // 8, radix, 0)
            return 0

        lax.fori_loop(0, chunks, inverse_rows, 0)

    def drain(c, _):
        each_peer(lambda o: go_copy(c, o, to_peer(o), me).wait_send())
        for f in range(2):
            each_peer(lambda o: back_copy(f, c, o, to_peer(o), me).wait_send())
        return 0

    lax.fori_loop(0, chunks, drain, 0)


def call(body, outs, scratch=(), smem=(0,), count=1, megabytes=48, flops=0, group=None):
    space = [
        pl.BlockSpec(memory_space=pltpu.SMEM if i in smem else pltpu.VMEM) for i in range(count)
    ]
    return pl.pallas_call(
        body,
        out_shape=outs,
        in_specs=space,
        out_specs=jax.tree.map(lambda _: pl.BlockSpec(memory_space=pltpu.VMEM), outs),
        scratch_shapes=list(scratch),
        compiler_params=pltpu.CompilerParams(
            vmem_limit_bytes=megabytes << 20,
            collective_id=group,
            has_side_effects=group is not None,
        ),
        cost_estimate=pl.CostEstimate(flops=flops, bytes_accessed=4 << 20, transcendentals=0),
    )


def shape(*dims):
    return jax.ShapeDtypeStruct(dims, jnp.float32)


def local_fast(block_tile, cell_index, masses, plane_coef, plane_dist, source_inv):
    groups = lax.axis_size("pix")
    me = lax.axis_index("pix")
    mine_shell = lax.axis_index("shell")
    planes, local_tiles, per_tile = cell_index.shape
    slab = L // groups
    per_owner = slab // TR * (L // TC)
    cap = max(1, 2 * local_tiles // groups)

    pairs = [(0, 1)]
    other = lax.ppermute(jnp.concatenate([plane_coef, plane_dist]), "shell", pairs)
    other_coef = jnp.where(mine_shell > 0, other[:planes], 0.0)
    other_dist = other[planes:]

    earlier = jnp.arange(local_tiles)[:, None] < jnp.arange(local_tiles)[None, :]
    wanted = me * cap + jnp.arange(cap)

    def routes(tiles):
        table = tiles.reshape(planes, groups, local_tiles)
        owner = table // per_owner
        same_owner = owner[:, :, :, None] == owner[:, :, None, :]
        rank = jnp.sum(jnp.where(same_owner & earlier[None, None], 1, 0), axis=2)
        slot = owner * cap + rank
        here = slot[:, :, None, :] == wanted[None, None, :, None]
        local_index = table - me * per_owner
        place = jnp.sum(jnp.where(here, local_index[:, :, None, :] + 1, 0), axis=3)
        place = jnp.where(place > 0, place - 1, per_owner).reshape(planes, groups * cap)
        return slot, place

    slot, place = routes(block_tile)
    _, other_place = routes(lax.ppermute(block_tile, "shell", pairs))
    my_slots = lax.dynamic_index_in_dim(slot, me, axis=1, keepdims=False)

    half = per_tile // TC
    as_lists = lambda part: part.astype(jnp.float32).reshape(planes, local_tiles, half, TC)
    lists = jnp.concatenate([as_lists(cell_index), as_lists(masses)], axis=2)
    outgoing = call(
        pack_kernel, [shape(groups, (cap + 1) * 2 * half, TC)] * planes, count=2, flops=1 << 20
    )(my_slots, lists)
    size = (cap + 1) * 2 * half
    dma = lambda *dims: pltpu.SemaphoreType.DMA(dims)
    swapped = call(
        swap_lists_kernel,
        [shape(groups, size, TC)] * (2 * planes),
        [dma(planes, groups)] * 4 + [dma(planes)],
        smem=(),
        count=planes,
        flops=1 << 30,
        group=0,
    )(*outgoing)

    own = plane_coef[None, :] * (1.0 - source_inv[:, None] * plane_dist[None, :])
    own = jnp.where(jnp.arange(planes)[None, :] <= jnp.arange(planes)[:, None], own, 0.0)
    before = other_coef[None, :] * (1.0 - source_inv[:, None] * other_dist[None, :])
    mix = jnp.concatenate([own, before], axis=1)

    routed = [place[p] for p in range(planes)] + [other_place[p] for p in range(planes)]
    convergence = call(
        partial(assemble_kernel, 2 * half),
        shape(planes, slab, L),
        [pltpu.VMEM((2 * planes, per_owner + 1, TR, TC), jnp.float32)],
        smem=tuple(range(2 * planes + 1)),
        count=4 * planes + 1,
        flops=1 << 32,
    )(mix, *routed, *swapped)

    row_high, row_low = row_tables()
    columns = jnp.asarray(block_columns().astype(np.float32))
    mine = lax.dynamic_index_in_dim(columns, me // planes, axis=0, keepdims=False)
    special = (me // planes == HALF_BLOCKS - 1) & (mine > 0)
    weight = jnp.where(special, 2.0, 1.0) / (L * L)
    signed = jnp.where(mine >= L // 2, mine - L, mine)
    col_info = jnp.stack([signed, weight])
    col_high, col_low = column_tables()
    tw_real, tw_imag = twiddle_tables()
    span = slab // CHUNKS
    vmem = lambda *dims: pltpu.VMEM(dims, jnp.float32)
    shear_one, shear_two = call(
        shear_kernel,
        [shape(planes, slab, L)] * 2,
        [
            vmem(HALF_BLOCKS, planes, span, 2 * INNER),
            vmem(groups, 2, slab, INNER),
            vmem(groups, 2, slab, INNER),
            vmem(OUTER, 2, INNER, INNER),
            vmem(2, OUTER, INNER, INNER),
            vmem(2, OUTER, INNER, INNER),
            vmem(2, OUTER, 2, INNER, INNER),
            vmem(groups, 2, 2, slab, INNER),
            vmem(groups, 2, 2, slab, INNER),
            vmem(HALF_BLOCKS, planes, span, 2 * INNER),
            dma(CHUNKS, groups),
            dma(CHUNKS, groups),
            dma(2, CHUNKS, groups),
            dma(2, CHUNKS, groups),
        ],
        smem=(),
        count=10,
        flops=1 << 32,
        group=1,
    )(
        convergence, col_info, jnp.asarray(tw_real), jnp.asarray(tw_imag), row_high, row_low,
        col_high, col_low, col_high.T.copy(), col_low.T.copy(),
    )
    return convergence, shear_one, shear_two


def solution(mesh):
    placed = (
        P("shell", None),
        P("shell", "pix", None),
        P("shell", "pix", None),
        P("shell"),
        P("shell"),
        P("shell"),
    )
    shells, groups = mesh.shape["shell"], mesh.shape["pix"]

    def body(block_tile, cell_index, *rest):
        fits = (
            shells == 2
            and cell_index.shape[0] == 2
            and groups == OUTER
            and cell_index.shape[2] % (4 * TC) == 0
        )
        return (local_fast if fits else local)(block_tile, cell_index, *rest)

    return jax.shard_map(
        body,
        mesh=mesh,
        in_specs=placed,
        out_specs=(P("shell", "pix", None), P("shell", "pix", None), P("shell", "pix", None)),
        check_vma=False,
    )
```

```python
from functools import partial
import math

import jax
import jax.numpy as jnp
from jax import lax
from jax.experimental import pallas as pl
from jax.experimental.pallas import tpu as pltpu
from jax.sharding import PartitionSpec as P
import numpy as np

L = 2048
TR = 16
TC = 128


HIGHEST = lax.Precision.HIGHEST


def entering(value, axis, join, neutral):
    count, mine = (lax.axis_size(axis), lax.axis_index(axis))
    pieces = jax.tree.map(lambda part: lax.all_gather(part, axis), value)
    running = jax.tree.map(
        lambda part, zero: jnp.full_like(part, 0) + jnp.asarray(zero, part.dtype), value, neutral
    )

    def lap(position, running):
        longer = join(running, jax.tree.map(lambda part: part[position], pieces))
        return jax.tree.map(lambda new, old: jnp.where(position < mine, new, old), longer, running)

    return lax.fori_loop(0, count - 1, lap, running)


def dft_table(left_size, right_size, period, sign_value):
    left_idx = jnp.arange(left_size)[:, None]
    right_idx = jnp.arange(right_size)[None, :]
    angle = 2.0 * math.pi / period * (left_idx * right_idx % period).astype(jnp.float32)
    return (jnp.cos(angle), sign_value * jnp.sin(angle))


def mix_outer(table, real_part, imag_part):
    cosine, sine_part = table
    contract = partial(jnp.einsum, "ab,...bc->...ac", precision=HIGHEST)
    return (
        contract(cosine, real_part) - contract(sine_part, imag_part),
        contract(sine_part, real_part) + contract(cosine, imag_part),
    )


def mix_inner(table, real_part, imag_part):
    cosine, sine_part = table
    product = partial(jnp.matmul, precision=HIGHEST)
    return (
        product(real_part, cosine) - product(imag_part, sine_part),
        product(real_part, sine_part) + product(imag_part, cosine),
    )


def twist(table, real_part, imag_part):
    cosine, sine_part = table
    return (real_part * cosine - imag_part * sine_part, real_part * sine_part + imag_part * cosine)


def transform_last(real_part, imag_part, sign_value):
    length = real_part.shape[-1]
    inner = math.gcd(length, 128)
    outer = length // inner
    leading = real_part.shape[:-1]
    real_part = real_part.reshape(leading + (outer, inner))
    imag_part = imag_part.reshape(leading + (outer, inner))
    outer_table = dft_table(outer, outer, outer, sign_value)
    inner_table = dft_table(inner, inner, inner, sign_value)
    twiddle = dft_table(outer, inner, length, sign_value)
    if sign_value < 0:
        real_part, imag_part = mix_outer(outer_table, real_part, imag_part)
        real_part, imag_part = twist(twiddle, real_part, imag_part)
        real_part, imag_part = mix_inner(inner_table, real_part, imag_part)
    else:
        real_part, imag_part = mix_inner(inner_table, real_part, imag_part)
        real_part, imag_part = twist(twiddle, real_part, imag_part)
        real_part, imag_part = mix_outer(outer_table, real_part, imag_part)
    return (real_part.reshape(leading + (length,)), imag_part.reshape(leading + (length,)))


def frequency_of(position, length):
    inner = math.gcd(length, 128)
    outer = length // inner
    frequency = position // inner + outer * (position % inner)
    signed = jnp.where(frequency >= length // 2, frequency - length, frequency).astype(jnp.float32)
    keep_mask = (frequency != length // 2).astype(jnp.float32)
    return (signed, keep_mask)


def add_pairs(earlier_pair, later_pair):
    return (earlier_pair[0] + later_pair[0], earlier_pair[1] + later_pair[1])


def deposit_group(item):
    cell_ids, weights = item
    tile_rows = cell_ids // TC
    tile_cols = cell_ids % TC
    row_hot = jnp.where(
        tile_rows[:, None, :] == jnp.arange(TR)[None, :, None],
        weights[:, None, :],
        jnp.zeros((), jnp.bfloat16),
    )
    col_hot = (tile_cols[:, :, None] == jnp.arange(TC)[None, None, :]).astype(jnp.bfloat16)
    return jnp.einsum("grk,gkc->grc", row_hot, col_hot, preferred_element_type=jnp.float32)


def rows_to_sending(packed, groups, slab, cols_own):
    count, fields = (packed.shape[0], packed.shape[1])
    return (
        packed.reshape(count, fields, slab, groups, cols_own)
        .transpose(3, 0, 1, 4, 2)
        .reshape(groups, count, fields, cols_own * slab)
    )


def arrived_to_columns(arrived, groups, slab, cols_own):
    count, fields = (arrived.shape[1], arrived.shape[2])
    return (
        arrived.reshape(groups, count, fields, cols_own, slab)
        .transpose(1, 2, 3, 0, 4)
        .reshape(count, fields, cols_own, groups * slab)
    )


def columns_to_sending(stacked, groups, slab, cols_own):
    count, fields = (stacked.shape[0], stacked.shape[1])
    return (
        stacked.reshape(count, fields, cols_own, groups, slab)
        .transpose(3, 0, 1, 2, 4)
        .reshape(groups, count, fields, cols_own * slab)
    )


def landed_to_rows(landed, groups, slab, cols_own):
    count, fields = (landed.shape[1], landed.shape[2])
    return (
        landed.reshape(groups, count, fields, cols_own, slab)
        .transpose(1, 2, 4, 0, 3)
        .reshape(count, fields, slab, groups * cols_own)
    )


def local(block_tile, cell_index, masses, plane_coef, plane_dist, source_inv):
    groups = lax.axis_size("pix")
    my_index = lax.axis_index("pix")
    planes, local_tiles, per_tile = cell_index.shape
    slab = L // groups
    per_owner = slab // TR * (L // TC)
    cap = max(1, 2 * local_tiles // groups)
    flat = TR * TC
    batch_tiles = 8
    deposited = lax.map(
        deposit_group,
        (cell_index.reshape(-1, batch_tiles, per_tile), masses.reshape(-1, batch_tiles, per_tile)),
    )
    tile_sums = deposited.reshape(planes, local_tiles, flat)
    table = block_tile.reshape(planes, groups, local_tiles)
    owner = table // per_owner
    earlier = jnp.arange(local_tiles)[:, None] < jnp.arange(local_tiles)[None, :]
    same_owner = owner[:, :, :, None] == owner[:, :, None, :]
    rank = jnp.sum(jnp.where(same_owner & earlier[None, None], 1, 0), axis=2)
    slot = owner * cap + rank
    my_slots = lax.dynamic_index_in_dim(slot, my_index, axis=1, keepdims=False)
    slot_grid = jnp.arange(groups)[:, None] * cap + jnp.arange(cap)[None, :]
    send_hot = (my_slots[:, None, None, :] == slot_grid[None, :, :, None]).astype(jnp.float32)
    outgoing = jnp.einsum("pnct,ptf->npcf", send_hot, tile_sums, precision=HIGHEST)
    incoming = lax.all_to_all(outgoing, "pix", split_axis=0, concat_axis=0, tiled=True)
    local_index = table - my_index * per_owner
    is_mine = owner == my_index
    tile_hot = (is_mine[..., None] & (local_index[..., None] == jnp.arange(per_owner))).astype(
        jnp.float32
    )
    slot_hot = (rank[..., None] == jnp.arange(cap)).astype(jnp.float32)
    placing = jnp.einsum("pstl,pstc->plsc", tile_hot, slot_hot, precision=HIGHEST)
    slab_tiles = jnp.einsum("plsc,spcf->plf", placing, incoming, precision=HIGHEST)
    density = (
        slab_tiles.reshape(planes, slab // TR, L // TC, TR, TC)
        .transpose(0, 1, 3, 2, 4)
        .reshape(planes, slab, L)
    )
    total = lax.psum(jnp.sum(density, axis=(1, 2)), "pix")
    contrast = density / (total / (L * L))[:, None, None] - 1.0
    near_local = jnp.cumsum(plane_coef[:, None, None] * contrast, axis=0)
    far_local = jnp.cumsum((plane_coef * plane_dist)[:, None, None] * contrast, axis=0)
    blank = jnp.zeros((slab, L), jnp.float32)
    near_before, far_before = entering(
        (near_local[-1], far_local[-1]), "shell", add_pairs, (blank, blank)
    )
    convergence = near_before + near_local - source_inv[:, None, None] * (far_before + far_local)
    cols_own = L // groups
    wave_x, keep_x = frequency_of(my_index * cols_own + jnp.arange(cols_own), L)
    wave_y, keep_y = frequency_of(jnp.arange(L), L)
    wave_x = wave_x[:, None]
    wave_y = wave_y[None, :]
    both_keep = keep_x[:, None] * keep_y[None, :]
    wave_power = jnp.maximum(wave_x * wave_x + wave_y * wave_y, 1.0)
    kernel_one = both_keep * (wave_x * wave_x - wave_y * wave_y) / wave_power
    kernel_two = both_keep * 2.0 * wave_x * wave_y / wave_power
    scale = 1.0 / (L * L)
    spec_real, spec_imag = transform_last(convergence[0::2], convergence[1::2], -1.0)
    sending = rows_to_sending(jnp.stack([spec_real, spec_imag], axis=1), groups, slab, cols_own)
    arrived = lax.all_to_all(sending, "pix", split_axis=0, concat_axis=0, tiled=True)
    columns = arrived_to_columns(arrived, groups, slab, cols_own)
    row_real, row_imag = transform_last(columns[:, 0], columns[:, 1], -1.0)
    first_real, first_imag = transform_last(row_real * kernel_one, row_imag * kernel_one, 1.0)
    second_real, second_imag = transform_last(row_real * kernel_two, row_imag * kernel_two, 1.0)
    stacked = jnp.stack([first_real, first_imag, second_real, second_imag], axis=1)
    landed = lax.all_to_all(
        columns_to_sending(stacked, groups, slab, cols_own),
        "pix",
        split_axis=0,
        concat_axis=0,
        tiled=True,
    )
    row_layout = landed_to_rows(landed, groups, slab, cols_own)
    even_one, odd_one = transform_last(row_layout[:, 0], row_layout[:, 1], 1.0)
    even_two, odd_two = transform_last(row_layout[:, 2], row_layout[:, 3], 1.0)
    shear_one = jnp.stack([even_one, odd_one], axis=1).reshape(planes, slab, L)
    shear_two = jnp.stack([even_two, odd_two], axis=1).reshape(planes, slab, L)
    return (convergence, shear_one * scale, shear_two * scale)


INNER = 128
OUTER = L // INNER
HALF_BLOCKS = OUTER // 2
CHUNKS = 4
MESH = pl.DeviceIdType.MESH


def block_columns():
    cols = np.zeros((HALF_BLOCKS, INNER), np.int64)
    for b in range(HALF_BLOCKS - 1):
        cols[b] = b + 1 + OUTER * np.arange(INNER)
    half = np.arange(INNER // 2)
    cols[-1] = np.concatenate([OUTER * half, HALF_BLOCKS + OUTER * half])
    return cols


def split_table(table):
    high = table.astype(jnp.bfloat16)
    low = (table - high.astype(np.float64)).astype(jnp.bfloat16)
    return high, low


def row_tables():
    n2 = np.arange(INNER)
    out = np.zeros((HALF_BLOCKS, 2 * INNER, 2 * INNER))
    cols = block_columns()
    for b in range(HALF_BLOCKS):
        angle = 2 * np.pi / L * ((n2[:, None] * cols[b][None, :]) % L)
        co, si = np.cos(angle), np.sin(angle)
        if b < HALF_BLOCKS - 1:
            out[b] = np.block([[co, -si], [si, co]])
        else:
            h = INNER // 2
            out[b, :INNER, :h] = co[:, :h]
            out[b, :INNER, INNER : INNER + h] = -si[:, :h]
            out[b, INNER:, h:INNER] = co[:, h:]
            out[b, INNER:, INNER + h :] = -si[:, h:]
    return split_table(out)


def row_order(slab):
    at = np.arange(slab)
    rows = slab // TR
    return (at % rows) * TR + at // rows


def column_table(order):
    idx = np.arange(INNER)
    angle = 2 * np.pi / INNER * ((idx[:, None] * order[None, :]) % INNER)
    co, si = np.cos(angle), np.sin(angle)
    return np.block([[co, si], [-si, co]])


def twiddle_tables(order):
    out = []
    for rows in (order, np.arange(INNER)):
        angle = 2 * np.pi / L * (np.arange(OUTER)[:, None] * rows[None, :])
        out += [np.cos(angle), -np.sin(angle)]
    return np.stack(out).astype(np.float32)


def times_root(value, k, n, sign):
    re, im = value
    k = k % n
    if k == 0:
        return value
    if 4 * k == n:
        return (-im, re) if sign > 0 else (im, -re)
    angle = 2 * math.pi * k / n
    c, s = math.cos(angle), sign * math.sin(angle)
    if 8 * k == n or 8 * k == 3 * n:
        if c > 0:
            return ((re - im) * c, (re + im) * c) if sign > 0 else ((re + im) * c, (im - re) * c)
        c = -c
        return ((re + im) * -c, (re - im) * c) if sign > 0 else ((im - re) * c, (re + im) * -c)
    return (re * c - im * s, re * s + im * c)


def fft_list(values, sign):
    n = len(values)
    if n == 1:
        return values
    even = fft_list(values[0::2], sign)
    odd = fft_list(values[1::2], sign)
    odd = [times_root(v, k, n, sign) for k, v in enumerate(odd)]
    return [(a[0] + b[0], a[1] + b[1]) for a, b in zip(even, odd)] + [
        (a[0] - b[0], a[1] - b[1]) for a, b in zip(even, odd)
    ]


def split_value(value):
    high = value.astype(jnp.bfloat16)
    return high, (value - high.astype(jnp.float32)).astype(jnp.bfloat16)


def three_pass(left, right, dims):
    dot = lambda a, b: lax.dot_general(a, b, (dims, ((), ())), preferred_element_type=jnp.float32)
    return dot(left[0], right[0]) + (dot(left[0], right[1]) + dot(left[1], right[0]))


def flipped(me, mask):
    for bit in (1, 2, 4, 8):
        me = me + ((mask // bit) % 2) * (bit - 2 * bit * ((me // bit) % 2))
    return me


def pack_kernel(tile_ref, coef_ref, dist_ref, cell_ref, mass_ref, *refs):
    out_refs, (wide, taken) = refs[:-2], refs[-2:]
    planes, tiles, per_tile = cell_ref.shape
    half = per_tile // TC
    size = 2 * half
    groups, rows, _ = out_refs[0].shape
    cap = rows // size - 1
    per_owner = L // groups // TR * (L // TC)
    me = lax.axis_index("pix")
    lane = lax.broadcasted_iota(jnp.int32, (1, TC), 1)
    for p in range(planes):
        out_ref = out_refs[p]
        for i in range(half):
            at = slice(i * TC, (i + 1) * TC)
            wide[i] = cell_ref[p, :, at].astype(jnp.float32)
            wide[half + i] = mass_ref[p, :, at].astype(jnp.float32)
        out_ref[...] = jnp.zeros_like(out_ref)
        total = jnp.sum(jnp.sum(wide[half:], axis=0), axis=0, keepdims=True)
        total = jnp.sum(total, axis=1, keepdims=True)
        tail = jnp.where(lane < cap, -1.0, jnp.where(lane == cap, total, 0.0))
        tail = jnp.where(lane == cap + 1, coef_ref[p], tail)
        tail = jnp.where(lane == cap + 2, dist_ref[p], tail)
        out_ref[:, cap * size :, :] = jnp.broadcast_to(tail[None], (groups, size, TC))

        def clear(o, _):
            taken[o] = 0
            return 0

        lax.fori_loop(0, groups, clear, 0)

        def tile(t, _):
            b = tile_ref[p, me * tiles + t]
            owner = b // per_owner
            rank = taken[owner]
            taken[owner] = rank + 1
            for i in range(size):
                out_ref[owner, pl.ds(rank * size + i, 1), :] = wide[i, pl.ds(t, 1), :]
            where_at = (b - owner * per_owner).astype(jnp.float32)
            old = out_ref[owner, cap * size : cap * size + 1, :]
            out_ref[owner, cap * size : cap * size + 1, :] = jnp.where(lane == rank, where_at, old)
            return 0

        lax.fori_loop(0, tiles, tile, 0)


def signal_all(peers):
    barrier = pltpu.get_barrier_semaphore()
    for peer in peers:
        pl.semaphore_signal(barrier, inc=1, device_id=peer, device_id_type=MESH)
    pl.semaphore_wait(barrier, len(peers))


def remote(source, target, send, recv, peer):
    return pltpu.make_async_remote_copy(
        src_ref=source,
        dst_ref=target,
        send_sem=send,
        recv_sem=recv,
        device_id=peer,
        device_id_type=MESH,
    )


def lensing_kernel(
    out0, out1, inv_ref, twist_ref, high_ref, low_ref, colh_ref, coll_ref, backh_ref, backl_ref,
    conv_ref, one_ref, two_ref,
    box, slots, place, field, held_row, sending, arrived, held, twist_in, kern, back, leaving, landed,
    lsend, lrecv, psend, precv, fsend, frecv, rsend, rrecv,
):
    out_refs = (out0, out1)
    planes = 2
    groups, message, _ = out0.shape
    slab = L // groups
    half = 4
    size = 2 * half
    cap = message // size - 1
    span = held_row.shape[2]
    chunks = slab // span
    pitch = slots.shape[1] // (cap * groups)
    tile_rows = slab // TR
    me, shell = lax.axis_index("pix"), lax.axis_index("shell")
    signal_all([{"pix": flipped(me, m)} for m in range(1, groups)] + [{"shell": 1 - shell}])

    def direct(p, m):
        peer = flipped(me, m)
        return remote(
            out_refs[p].at[peer], box.at[p, me], lsend.at[p, m], lrecv.at[p, m], {"pix": peer}
        )

    def landing(p, m):
        peer = flipped(me, m)
        return remote(
            out_refs[p].at[peer], box.at[p, peer], lsend.at[p, m], lrecv.at[p, m], {"pix": peer}
        )

    def onward(p, m):
        source = flipped(me, m)
        first = out_refs[p].at[me] if isinstance(m, int) and m == 0 else box.at[p, source]
        return remote(first, box.at[planes + p, source], psend.at[p, m], precv.at[p, m], {"shell": 1 - shell})

    for low, high in ((1, groups // 2), (groups // 2, groups)):
        for p in range(planes):

            def start(m, _):
                direct(p, m).start()
                return 0

            lax.fori_loop(low, high, start, 0)
    for p in range(planes):
        onward(p, 0).start()
        box[p, me] = out_refs[p][me]

    signed_v, weight = column_info(me, groups)
    inner_id = lax.broadcasted_iota(jnp.int32, (INNER, INNER), 0)

    def prepare(k, _):
        for i in range(4):
            twist_in[i, k] = jnp.broadcast_to(twist_ref[i, pl.ds(k, 1), :], (INNER, INNER)).T
        u = k + OUTER * inner_id
        signed_u = jnp.where(u >= L // 2, u - L, u).astype(jnp.float32)
        scale = jnp.where(u == L // 2, 0.0, weight)
        uu, vv = signed_u * signed_u, signed_v * signed_v
        over = scale / jnp.maximum(uu + vv, 1.0)
        kern[0, k] = (vv - uu) * over
        kern[1, k] = 2.0 * signed_v * signed_u * over
        return 0

    as_small = lambda ids: ids.astype(jnp.float32).astype(jnp.bfloat16)
    short, narrow = 2 * TR, TC // 2
    row_id = as_small(lax.broadcasted_iota(jnp.int32, (short, TC), 0))
    col_id = as_small(lax.broadcasted_iota(jnp.int32, (narrow, TC), 0))
    one, zero = jnp.ones((), jnp.bfloat16), jnp.zeros((), jnp.bfloat16)

    def deposit(q, s):
        for c in range(cap):
            entry = box[q, s, c * size : (c + 1) * size, :]
            cells = entry[:half].astype(jnp.int32)
            cell_rows = as_small(cells // TC + TR * ((cells // narrow) % 2))
            cell_cols = as_small(cells % narrow)
            weights = entry[half:].astype(jnp.bfloat16)
            row_hot, col_hot = [], []
            for i in range(half):
                row_hot.append(jnp.where(row_id == cell_rows[i : i + 1], weights[i : i + 1], zero))
                col_hot.append(jnp.where(col_id == cell_cols[i : i + 1], one, zero))
            sums = lax.dot_general(
                jnp.concatenate(row_hot, axis=1),
                jnp.concatenate(col_hot, axis=1),
                (((1,), (1,)), ((), ())),
                preferred_element_type=jnp.float32,
            )
            at = pl.ds(pl.multiple_of((c * groups + s) * pitch, 8), TR)
            slots[q, at, :] = jnp.concatenate([sums[:TR], sums[TR:]], axis=1)

    def near_block(m):
        def one_plane(p, _):
            deposit(p, flipped(me, m))
            return 0

        lax.fori_loop(0, planes, one_plane, 0)

    def far_block(m):
        for p in range(planes):
            onward(p, m).wait_recv()

        def one_plane(p, _):
            deposit(planes + p, flipped(me, m))
            return 0

        lax.fori_loop(0, planes, one_plane, 0)

    def take(m):
        for p in range(planes):
            landing(p, m).wait_recv()
            onward(p, m).start()

    lag = 4
    near_block(0)
    lax.fori_loop(0, OUTER, prepare, 0)

    def early(m, _):
        take(m)
        near_block(m)
        return 0

    lax.fori_loop(1, lag, early, 0)

    def steady(m, _):
        take(m)
        near_block(m)
        far_block(m - lag)
        return 0

    lax.fori_loop(lag, groups, steady, 0)

    def late(m, _):
        far_block(m)
        return 0

    lax.fori_loop(groups - lag, groups, late, 0)

    lane_id = lax.broadcasted_iota(jnp.int32, (groups, TC), 1)
    tile_id = ((lane_id % tile_rows) * OUTER + lane_id // tile_rows).astype(jnp.float32)
    gains, shifts = [[], []], [0.0, 0.0]
    for q in range(2 * planes):
        tails = box[q, :, cap * size, :]
        hot = [jnp.where(tails[:, c : c + 1] == tile_id, 1.0, 0.0) for c in range(cap)]
        place[q] = jnp.concatenate(hot, axis=0).T.astype(jnp.bfloat16)
        total = jnp.sum(tails[:, cap : cap + 1], axis=0, keepdims=True)
        coef, dist = tails[0:1, cap + 1 : cap + 2], tails[0:1, cap + 2 : cap + 3]
        for i in range(planes):
            mixed = coef * (1.0 - inv_ref[i] * dist)
            if q >= planes:
                mixed = jnp.where(shell > 0, mixed, 0.0)
            elif q > i:
                mixed = jnp.zeros_like(mixed)
            gains[i].append(mixed * ((L * L) / total))
            shifts[i] = shifts[i] + mixed

    def rows_of(c):
        return pl.ds(pl.multiple_of(c * span, span), span)

    def go_copy(c, m, arriving=False):
        peer = flipped(me, m)
        return remote(
            sending.at[peer, :, rows_of(c), :],
            arrived.at[peer if arriving else me, :, rows_of(c), :],
            fsend.at[c, m],
            frecv.at[c, m],
            {"pix": peer},
        )

    def back_copy(f, c, m, arriving=False):
        peer = flipped(me, m)
        return remote(
            leaving.at[peer, f, :, rows_of(c), :],
            landed.at[peer if arriving else me, f, :, rows_of(c), :],
            rsend.at[f, c, m],
            rrecv.at[f, c, m],
            {"pix": peer},
        )

    def each_peer(action):
        def step(m, _):
            action(m)
            return 0

        lax.fori_loop(1, groups, step, 0)

    def field_rows(r, n):
        return pl.ds(pl.multiple_of(r * TC + n * tile_rows, tile_rows), tile_rows)

    def forward_rows(c, _):
        def mass_rows(j, _):
            r = c * (span // tile_rows) + 2 * j
            sums = []
            for q in range(2 * planes):
                pair = jnp.concatenate(
                    [slots[q, pl.ds(r + i, cap * groups, stride=pitch), :] for i in range(2)], axis=1
                )
                high = pair.astype(jnp.bfloat16)
                rest = pair - high.astype(jnp.float32)
                middle = rest.astype(jnp.bfloat16)
                low = (rest - middle.astype(jnp.float32)).astype(jnp.bfloat16)
                dot = lambda part: jnp.dot(place[q], part, preferred_element_type=jnp.float32)
                sums.append(dot(high) + (dot(middle) + dot(low)))
            for i in range(planes):
                value = gains[i][0] * sums[0]
                for q in range(1, 2 * planes):
                    value = value + gains[i][q] * sums[q]
                value = value - shifts[i]
                for e in range(2):
                    at = pl.ds(pl.multiple_of((r + e) * TC, TC), TC)
                    field[i, at, :] = value[:, e * TC : (e + 1) * TC]
            return 0

        lax.fori_loop(0, span // tile_rows // 2, mass_rows, 0)

        def radix(j, _):
            r = c * (span // tile_rows) + j
            near = pl.ds(pl.multiple_of(j * tile_rows, tile_rows), tile_rows)
            z = fft_list(
                [
                    tuple(field[i, field_rows(r, n), :] for i in range(2))
                    for n in range(OUTER)
                ],
                -1,
            )
            for k in range(1, HALF_BLOCKS):
                (ar, ai), (br, bi) = z[k], z[OUTER - k]
                held_row[k - 1, 0, near, :INNER] = 0.5 * (ar + br)
                held_row[k - 1, 0, near, INNER:] = 0.5 * (ai - bi)
                held_row[k - 1, 1, near, :INNER] = 0.5 * (ai + bi)
                held_row[k - 1, 1, near, INNER:] = 0.5 * (br - ar)
            for p in range(2):
                held_row[HALF_BLOCKS - 1, p, near, :INNER] = z[0][p]
                held_row[HALF_BLOCKS - 1, p, near, INNER:] = z[HALF_BLOCKS][p]
            return 0

        lax.fori_loop(0, span // tile_rows, radix, 0)

        def block(j, _):
            b = (me // 2 + 1 + j) % HALF_BLOCKS
            value = held_row[b].reshape(2 * span, 2 * INNER)
            result = three_pass(split_value(value), (high_ref[b], low_ref[b]), ((1,), (0,)))
            for p in range(2):
                for part in range(2):
                    sending[2 * b + p, part, rows_of(c), :] = result[
                        p * span : (p + 1) * span, part * INNER : (part + 1) * INNER
                    ]
            return 0

        lax.fori_loop(0, HALF_BLOCKS, block, 0)
        each_peer(lambda m: go_copy(c, m).start())
        for part in range(2):
            arrived[me, part, rows_of(c), :] = sending[me, part, rows_of(c), :]
        return 0

    lax.fori_loop(0, chunks, forward_rows, 0)

    def show(t, _):
        for i in range(planes):
            for n in range(OUTER):
                for r in range(0, TR, 8):
                    rows = pl.ds(pl.multiple_of(t * TR + r, 8), 8)
                    held_at = pl.ds(r * TC + n * tile_rows + t, 8, stride=TC)
                    conv_ref[i, rows, n * TC : (n + 1) * TC] = field[i, held_at, :]
        return 0

    lax.fori_loop(0, tile_rows, show, 0)

    def forward_columns(c, _):
        each_peer(lambda m: go_copy(c, m, True).wait_recv())

        def radix(t, _):
            rows = pl.ds(pl.multiple_of(c * span + t * 8, 8), 8)
            z = fft_list([(arrived[n, 0, rows, :], arrived[n, 1, rows, :]) for n in range(OUTER)], -1)
            for k in range(OUTER):
                re, im = z[k]
                if k:
                    cs, sn = twist_in[0, k, rows, :], twist_in[1, k, rows, :]
                    re, im = re * cs - im * sn, re * sn + im * cs
                held[k, 0, rows, :] = re
                held[k, 1, rows, :] = im
            return 0

        lax.fori_loop(0, span // 8, radix, 0)
        return 0

    lax.fori_loop(0, chunks, forward_columns, 0)

    def middle(j, _):
        pair = jnp.concatenate([held[2 * j + i].reshape(2 * INNER, INNER) for i in range(2)], axis=1)
        spectrum = three_pass((colh_ref[...], coll_ref[...]), split_value(pair), ((1,), (0,)))
        for i in range(2):
            k = 2 * j + i
            mine = spectrum[:, i * INNER : (i + 1) * INNER]
            fields = jnp.concatenate(
                [
                    jnp.concatenate([mine[:INNER] * kern[f, k], mine[INNER:] * kern[f, k]], axis=0)
                    for f in range(2)
                ],
                axis=1,
            )
            result = three_pass((backh_ref[...], backl_ref[...]), split_value(fields), ((1,), (0,)))
            cs, sn = twist_in[2, k], twist_in[3, k]
            for f in range(2):
                at = slice(f * INNER, (f + 1) * INNER)
                re, im = result[:INNER, at], result[INNER:, at]
                back[f, k, 0] = re * cs + im * sn
                back[f, k, 1] = im * cs - re * sn
        return 0

    lax.fori_loop(0, OUTER // 2, middle, 0)

    def inverse_columns(q, _):
        f, c = q // chunks, q % chunks

        def radix(t, _):
            rows = pl.ds(pl.multiple_of(c * span + t * 8, 8), 8)
            x = fft_list([(back[f, k, 0, rows, :], back[f, k, 1, rows, :]) for k in range(OUTER)], 1)
            for n in range(OUTER):
                leaving[n, f, 0, rows, :] = x[n][0]
                leaving[n, f, 1, rows, :] = x[n][1]
            return 0

        lax.fori_loop(0, span // 8, radix, 0)
        each_peer(lambda m: back_copy(f, c, m).start())
        for part in range(2):
            landed[me, f, part, rows_of(c), :] = leaving[me, f, part, rows_of(c), :]
        return 0

    lax.fori_loop(0, 2 * chunks, inverse_columns, 0)

    for f, out_ref in enumerate((one_ref, two_ref)):

        def inverse_rows(c, _):
            each_peer(lambda m: back_copy(f, c, m, True).wait_recv())

            def block(b, _):
                value = jnp.concatenate(
                    [
                        jnp.concatenate(
                            [landed[2 * b + p, f, part, rows_of(c), :] for part in range(2)], axis=1
                        )
                        for p in range(2)
                    ],
                    axis=0,
                )
                held_row[b] = three_pass(
                    split_value(value), (high_ref[b], low_ref[b]), ((1,), (1,))
                ).reshape(2, span, 2 * INNER)
                return 0

            lax.fori_loop(0, HALF_BLOCKS, block, 0)

            def radix(t, _):
                near = pl.ds(pl.multiple_of(t * 8, 8), 8)
                rows = pl.ds(pl.multiple_of(c * span + t * 8, 8), 8)
                z = [None] * OUTER
                last = HALF_BLOCKS - 1
                z[0] = (held_row[last, 0, near, :INNER], held_row[last, 1, near, :INNER])
                z[HALF_BLOCKS] = (held_row[last, 0, near, INNER:], held_row[last, 1, near, INNER:])
                for k in range(1, HALF_BLOCKS):
                    ar, ai = held_row[k - 1, 0, near, :INNER], held_row[k - 1, 0, near, INNER:]
                    br, bi = held_row[k - 1, 1, near, :INNER], held_row[k - 1, 1, near, INNER:]
                    z[k] = (ar - bi, ai + br)
                    z[OUTER - k] = (ar + bi, br - ai)
                x = fft_list(z, 1)
                for n in range(OUTER):
                    for p in range(2):
                        out_ref[p, rows, n * INNER : (n + 1) * INNER] = x[n][p]
                return 0

            lax.fori_loop(0, span // 8, radix, 0)
            return 0

        lax.fori_loop(0, chunks, inverse_rows, 0)

    def drain(c, _):
        each_peer(lambda m: go_copy(c, m).wait_send())
        for f in range(2):
            each_peer(lambda m: back_copy(f, c, m).wait_send())
        return 0

    lax.fori_loop(0, chunks, drain, 0)
    for p in range(planes):
        onward(p, 0).wait_send()

        def settle(m, _):
            direct(p, m).wait_send()
            onward(p, m).wait_send()
            return 0

        lax.fori_loop(1, groups, settle, 0)


def column_info(me, groups):
    lane = lax.broadcasted_iota(jnp.int32, (1, INNER), 1)
    b = me // 2
    last = b == HALF_BLOCKS - 1
    upper = lane // (INNER // 2)
    folded = OUTER * (lane - upper * (INNER // 2)) + HALF_BLOCKS * upper
    mine = jnp.where(last, folded, b + 1 + OUTER * lane)
    weight = jnp.where(last & (mine > 0), 2.0, 1.0) / (L * L)
    return jnp.where(mine >= L // 2, mine - L, mine).astype(jnp.float32), weight


def call(body, outs, scratch=(), smem=(0,), count=1, megabytes=48, flops=0, group=None):
    space = [
        pl.BlockSpec(memory_space=pltpu.SMEM if i in smem else pltpu.VMEM) for i in range(count)
    ]
    return pl.pallas_call(
        body,
        out_shape=outs,
        in_specs=space,
        out_specs=jax.tree.map(lambda _: pl.BlockSpec(memory_space=pltpu.VMEM), outs),
        scratch_shapes=list(scratch),
        compiler_params=pltpu.CompilerParams(
            vmem_limit_bytes=megabytes << 20,
            collective_id=group,
            has_side_effects=group is not None,
        ),
        cost_estimate=pl.CostEstimate(flops=flops, bytes_accessed=4 << 20, transcendentals=0),
    )


def shape(*dims):
    return jax.ShapeDtypeStruct(dims, jnp.float32)


def local_fast(block_tile, cell_index, masses, plane_coef, plane_dist, source_inv):
    groups = lax.axis_size("pix")
    planes, local_tiles, per_tile = cell_index.shape
    slab = L // groups
    cap = max(1, 2 * local_tiles // groups)
    size = 2 * per_tile // TC
    message = (cap + 1) * size
    vmem = lambda *dims: pltpu.VMEM(dims, jnp.float32)
    dma = lambda *dims: pltpu.SemaphoreType.DMA(dims)
    outgoing = call(
        pack_kernel,
        [shape(groups, message, TC)] * planes,
        [vmem(size, local_tiles, TC), pltpu.SMEM((groups,), jnp.int32)],
        smem=(0, 1, 2),
        count=5,
        flops=1 << 20,
    )(block_tile, plane_coef, plane_dist, cell_index, masses)

    order = row_order(slab)
    row_high, row_low = row_tables()
    forth, natural = column_table(order), column_table(np.arange(INNER))
    col_high, col_low = split_table(forth)
    back_high, back_low = split_table(natural.T)
    span = slab // CHUNKS
    pitch = 3 * TR // 2
    return call(
        lensing_kernel,
        [shape(planes, slab, L)] * 3,
        [
            vmem(2 * planes, groups, message, TC),
            vmem(2 * planes, cap * groups * pitch, TC),
            pltpu.VMEM((2 * planes, TC, TC), jnp.bfloat16),
            vmem(planes, TR * TC, TC),
            vmem(HALF_BLOCKS, planes, span, 2 * INNER),
            vmem(groups, 2, slab, INNER),
            vmem(groups, 2, slab, INNER),
            vmem(OUTER, 2, INNER, INNER),
            vmem(4, OUTER, INNER, INNER),
            vmem(2, OUTER, INNER, INNER),
            vmem(2, OUTER, 2, INNER, INNER),
            vmem(groups, 2, 2, slab, INNER),
            vmem(groups, 2, 2, slab, INNER),
            dma(planes, groups),
            dma(planes, groups),
            dma(planes, groups),
            dma(planes, groups),
            dma(CHUNKS, groups),
            dma(CHUNKS, groups),
            dma(2, CHUNKS, groups),
            dma(2, CHUNKS, groups),
        ],
        smem=(2,),
        count=10,
        megabytes=58,
        flops=1 << 32,
        group=0,
    )(
        *outgoing, source_inv, jnp.asarray(twiddle_tables(order)), row_high, row_low,
        col_high, col_low, back_high, back_low,
    )


def solution(mesh):
    placed = (
        P("shell", None),
        P("shell", "pix", None),
        P("shell", "pix", None),
        P("shell"),
        P("shell"),
        P("shell"),
    )
    shells, groups = mesh.shape["shell"], mesh.shape["pix"]

    def body(block_tile, cell_index, *rest):
        fits = (
            shells == 2
            and cell_index.shape[0] == 2
            and groups == OUTER
            and cell_index.shape[2] == 4 * TC
            and cell_index.shape[1] * 2 == groups * 8
        )
        return (local_fast if fits else local)(block_tile, cell_index, *rest)

    return jax.shard_map(
        body,
        mesh=mesh,
        in_specs=placed,
        out_specs=(P("shell", "pix", None), P("shell", "pix", None), P("shell", "pix", None)),
        check_vma=False,
    )
```

```python
from functools import partial
import math

import jax
import jax.numpy as jnp
from jax import lax
from jax.experimental import pallas as pl
from jax.experimental.pallas import tpu as pltpu
from jax.sharding import PartitionSpec as P
import numpy as np

L = 2048
TR = 16
TC = 128


HIGHEST = lax.Precision.HIGHEST


def entering(value, axis, join, neutral):
    count, mine = (lax.axis_size(axis), lax.axis_index(axis))
    pieces = jax.tree.map(lambda part: lax.all_gather(part, axis), value)
    running = jax.tree.map(
        lambda part, zero: jnp.full_like(part, 0) + jnp.asarray(zero, part.dtype), value, neutral
    )

    def lap(position, running):
        longer = join(running, jax.tree.map(lambda part: part[position], pieces))
        return jax.tree.map(lambda new, old: jnp.where(position < mine, new, old), longer, running)

    return lax.fori_loop(0, count - 1, lap, running)


def dft_table(left_size, right_size, period, sign_value):
    left_idx = jnp.arange(left_size)[:, None]
    right_idx = jnp.arange(right_size)[None, :]
    angle = 2.0 * math.pi / period * (left_idx * right_idx % period).astype(jnp.float32)
    return (jnp.cos(angle), sign_value * jnp.sin(angle))


def mix_outer(table, real_part, imag_part):
    cosine, sine_part = table
    contract = partial(jnp.einsum, "ab,...bc->...ac", precision=HIGHEST)
    return (
        contract(cosine, real_part) - contract(sine_part, imag_part),
        contract(sine_part, real_part) + contract(cosine, imag_part),
    )


def mix_inner(table, real_part, imag_part):
    cosine, sine_part = table
    product = partial(jnp.matmul, precision=HIGHEST)
    return (
        product(real_part, cosine) - product(imag_part, sine_part),
        product(real_part, sine_part) + product(imag_part, cosine),
    )


def twist(table, real_part, imag_part):
    cosine, sine_part = table
    return (real_part * cosine - imag_part * sine_part, real_part * sine_part + imag_part * cosine)


def transform_last(real_part, imag_part, sign_value):
    length = real_part.shape[-1]
    inner = math.gcd(length, 128)
    outer = length // inner
    leading = real_part.shape[:-1]
    real_part = real_part.reshape(leading + (outer, inner))
    imag_part = imag_part.reshape(leading + (outer, inner))
    outer_table = dft_table(outer, outer, outer, sign_value)
    inner_table = dft_table(inner, inner, inner, sign_value)
    twiddle = dft_table(outer, inner, length, sign_value)
    if sign_value < 0:
        real_part, imag_part = mix_outer(outer_table, real_part, imag_part)
        real_part, imag_part = twist(twiddle, real_part, imag_part)
        real_part, imag_part = mix_inner(inner_table, real_part, imag_part)
    else:
        real_part, imag_part = mix_inner(inner_table, real_part, imag_part)
        real_part, imag_part = twist(twiddle, real_part, imag_part)
        real_part, imag_part = mix_outer(outer_table, real_part, imag_part)
    return (real_part.reshape(leading + (length,)), imag_part.reshape(leading + (length,)))


def frequency_of(position, length):
    inner = math.gcd(length, 128)
    outer = length // inner
    frequency = position // inner + outer * (position % inner)
    signed = jnp.where(frequency >= length // 2, frequency - length, frequency).astype(jnp.float32)
    keep_mask = (frequency != length // 2).astype(jnp.float32)
    return (signed, keep_mask)


def add_pairs(earlier_pair, later_pair):
    return (earlier_pair[0] + later_pair[0], earlier_pair[1] + later_pair[1])


def deposit_group(item):
    cell_ids, weights = item
    tile_rows = cell_ids // TC
    tile_cols = cell_ids % TC
    row_hot = jnp.where(
        tile_rows[:, None, :] == jnp.arange(TR)[None, :, None],
        weights[:, None, :],
        jnp.zeros((), jnp.bfloat16),
    )
    col_hot = (tile_cols[:, :, None] == jnp.arange(TC)[None, None, :]).astype(jnp.bfloat16)
    return jnp.einsum("grk,gkc->grc", row_hot, col_hot, preferred_element_type=jnp.float32)


def rows_to_sending(packed, groups, slab, cols_own):
    count, fields = (packed.shape[0], packed.shape[1])
    return (
        packed.reshape(count, fields, slab, groups, cols_own)
        .transpose(3, 0, 1, 4, 2)
        .reshape(groups, count, fields, cols_own * slab)
    )


def arrived_to_columns(arrived, groups, slab, cols_own):
    count, fields = (arrived.shape[1], arrived.shape[2])
    return (
        arrived.reshape(groups, count, fields, cols_own, slab)
        .transpose(1, 2, 3, 0, 4)
        .reshape(count, fields, cols_own, groups * slab)
    )


def columns_to_sending(stacked, groups, slab, cols_own):
    count, fields = (stacked.shape[0], stacked.shape[1])
    return (
        stacked.reshape(count, fields, cols_own, groups, slab)
        .transpose(3, 0, 1, 2, 4)
        .reshape(groups, count, fields, cols_own * slab)
    )


def landed_to_rows(landed, groups, slab, cols_own):
    count, fields = (landed.shape[1], landed.shape[2])
    return (
        landed.reshape(groups, count, fields, cols_own, slab)
        .transpose(1, 2, 4, 0, 3)
        .reshape(count, fields, slab, groups * cols_own)
    )


def local(block_tile, cell_index, masses, plane_coef, plane_dist, source_inv):
    groups = lax.axis_size("pix")
    my_index = lax.axis_index("pix")
    planes, local_tiles, per_tile = cell_index.shape
    slab = L // groups
    per_owner = slab // TR * (L // TC)
    cap = max(1, 2 * local_tiles // groups)
    flat = TR * TC
    batch_tiles = 8
    deposited = lax.map(
        deposit_group,
        (cell_index.reshape(-1, batch_tiles, per_tile), masses.reshape(-1, batch_tiles, per_tile)),
    )
    tile_sums = deposited.reshape(planes, local_tiles, flat)
    table = block_tile.reshape(planes, groups, local_tiles)
    owner = table // per_owner
    earlier = jnp.arange(local_tiles)[:, None] < jnp.arange(local_tiles)[None, :]
    same_owner = owner[:, :, :, None] == owner[:, :, None, :]
    rank = jnp.sum(jnp.where(same_owner & earlier[None, None], 1, 0), axis=2)
    slot = owner * cap + rank
    my_slots = lax.dynamic_index_in_dim(slot, my_index, axis=1, keepdims=False)
    slot_grid = jnp.arange(groups)[:, None] * cap + jnp.arange(cap)[None, :]
    send_hot = (my_slots[:, None, None, :] == slot_grid[None, :, :, None]).astype(jnp.float32)
    outgoing = jnp.einsum("pnct,ptf->npcf", send_hot, tile_sums, precision=HIGHEST)
    incoming = lax.all_to_all(outgoing, "pix", split_axis=0, concat_axis=0, tiled=True)
    local_index = table - my_index * per_owner
    is_mine = owner == my_index
    tile_hot = (is_mine[..., None] & (local_index[..., None] == jnp.arange(per_owner))).astype(
        jnp.float32
    )
    slot_hot = (rank[..., None] == jnp.arange(cap)).astype(jnp.float32)
    placing = jnp.einsum("pstl,pstc->plsc", tile_hot, slot_hot, precision=HIGHEST)
    slab_tiles = jnp.einsum("plsc,spcf->plf", placing, incoming, precision=HIGHEST)
    density = (
        slab_tiles.reshape(planes, slab // TR, L // TC, TR, TC)
        .transpose(0, 1, 3, 2, 4)
        .reshape(planes, slab, L)
    )
    total = lax.psum(jnp.sum(density, axis=(1, 2)), "pix")
    contrast = density / (total / (L * L))[:, None, None] - 1.0
    near_local = jnp.cumsum(plane_coef[:, None, None] * contrast, axis=0)
    far_local = jnp.cumsum((plane_coef * plane_dist)[:, None, None] * contrast, axis=0)
    blank = jnp.zeros((slab, L), jnp.float32)
    near_before, far_before = entering(
        (near_local[-1], far_local[-1]), "shell", add_pairs, (blank, blank)
    )
    convergence = near_before + near_local - source_inv[:, None, None] * (far_before + far_local)
    cols_own = L // groups
    wave_x, keep_x = frequency_of(my_index * cols_own + jnp.arange(cols_own), L)
    wave_y, keep_y = frequency_of(jnp.arange(L), L)
    wave_x = wave_x[:, None]
    wave_y = wave_y[None, :]
    both_keep = keep_x[:, None] * keep_y[None, :]
    wave_power = jnp.maximum(wave_x * wave_x + wave_y * wave_y, 1.0)
    kernel_one = both_keep * (wave_x * wave_x - wave_y * wave_y) / wave_power
    kernel_two = both_keep * 2.0 * wave_x * wave_y / wave_power
    scale = 1.0 / (L * L)
    spec_real, spec_imag = transform_last(convergence[0::2], convergence[1::2], -1.0)
    sending = rows_to_sending(jnp.stack([spec_real, spec_imag], axis=1), groups, slab, cols_own)
    arrived = lax.all_to_all(sending, "pix", split_axis=0, concat_axis=0, tiled=True)
    columns = arrived_to_columns(arrived, groups, slab, cols_own)
    row_real, row_imag = transform_last(columns[:, 0], columns[:, 1], -1.0)
    first_real, first_imag = transform_last(row_real * kernel_one, row_imag * kernel_one, 1.0)
    second_real, second_imag = transform_last(row_real * kernel_two, row_imag * kernel_two, 1.0)
    stacked = jnp.stack([first_real, first_imag, second_real, second_imag], axis=1)
    landed = lax.all_to_all(
        columns_to_sending(stacked, groups, slab, cols_own),
        "pix",
        split_axis=0,
        concat_axis=0,
        tiled=True,
    )
    row_layout = landed_to_rows(landed, groups, slab, cols_own)
    even_one, odd_one = transform_last(row_layout[:, 0], row_layout[:, 1], 1.0)
    even_two, odd_two = transform_last(row_layout[:, 2], row_layout[:, 3], 1.0)
    shear_one = jnp.stack([even_one, odd_one], axis=1).reshape(planes, slab, L)
    shear_two = jnp.stack([even_two, odd_two], axis=1).reshape(planes, slab, L)
    return (convergence, shear_one * scale, shear_two * scale)


INNER = 128
OUTER = L // INNER
HALF_BLOCKS = OUTER // 2
CHUNKS = 4
MESH = pl.DeviceIdType.MESH


def block_columns():
    cols = np.zeros((HALF_BLOCKS, INNER), np.int64)
    for b in range(HALF_BLOCKS - 1):
        cols[b] = b + 1 + OUTER * np.arange(INNER)
    half = np.arange(INNER // 2)
    cols[-1] = np.concatenate([OUTER * half, HALF_BLOCKS + OUTER * half])
    return cols


def split_table(table):
    high = table.astype(jnp.bfloat16)
    low = (table - high.astype(np.float64)).astype(jnp.bfloat16)
    return high, low


def row_tables():
    n2 = np.arange(INNER)
    out = np.zeros((HALF_BLOCKS, 2 * INNER, 2 * INNER))
    cols = block_columns()
    for b in range(HALF_BLOCKS):
        angle = 2 * np.pi / L * ((n2[:, None] * cols[b][None, :]) % L)
        co, si = np.cos(angle), np.sin(angle)
        if b < HALF_BLOCKS - 1:
            out[b] = np.block([[co, -si], [si, co]])
        else:
            h = INNER // 2
            out[b, :INNER, :h] = co[:, :h]
            out[b, :INNER, INNER : INNER + h] = -si[:, :h]
            out[b, INNER:, h:INNER] = co[:, h:]
            out[b, INNER:, INNER + h :] = -si[:, h:]
    return split_table(out)


def row_order(slab):
    at = np.arange(slab)
    rows = slab // TR
    return (at % rows) * TR + at // rows


def column_table(order):
    idx = np.arange(INNER)
    angle = 2 * np.pi / INNER * ((idx[:, None] * order[None, :]) % INNER)
    co, si = np.cos(angle), np.sin(angle)
    return np.block([[co, si], [-si, co]])


def twiddle_tables(order):
    out = []
    for rows in (order, np.arange(INNER)):
        angle = 2 * np.pi / L * (np.arange(OUTER)[:, None] * rows[None, :])
        out += [np.cos(angle), -np.sin(angle)]
    return np.stack(out).astype(np.float32)


def times_root(value, k, n, sign):
    re, im = value
    k = k % n
    if k == 0:
        return value
    if 4 * k == n:
        return (-im, re) if sign > 0 else (im, -re)
    angle = 2 * math.pi * k / n
    c, s = math.cos(angle), sign * math.sin(angle)
    if 8 * k == n or 8 * k == 3 * n:
        if c > 0:
            return ((re - im) * c, (re + im) * c) if sign > 0 else ((re + im) * c, (im - re) * c)
        c = -c
        return ((re + im) * -c, (re - im) * c) if sign > 0 else ((im - re) * c, (re + im) * -c)
    return (re * c - im * s, re * s + im * c)


def fft_list(values, sign):
    n = len(values)
    if n == 1:
        return values
    even = fft_list(values[0::2], sign)
    odd = fft_list(values[1::2], sign)
    odd = [times_root(v, k, n, sign) for k, v in enumerate(odd)]
    return [(a[0] + b[0], a[1] + b[1]) for a, b in zip(even, odd)] + [
        (a[0] - b[0], a[1] - b[1]) for a, b in zip(even, odd)
    ]


def split_value(value):
    high = value.astype(jnp.bfloat16)
    return high, (value - high.astype(jnp.float32)).astype(jnp.bfloat16)


def three_pass(left, right, dims):
    dot = lambda a, b: lax.dot_general(a, b, (dims, ((), ())), preferred_element_type=jnp.float32)
    return dot(left[0], right[0]) + (dot(left[0], right[1]) + dot(left[1], right[0]))


def partners(me):
    steps = [(bit, bit - 2 * bit * ((me // bit) % 2)) for bit in (1, 2, 4, 8)]

    def flipped(mask):
        peer = me
        for bit, step in steps:
            if not isinstance(mask, int):
                peer = peer + ((mask // bit) % 2) * step
            elif mask & bit:
                peer = peer + step
        return peer

    return flipped


def fetch(pairs, sems):
    copies = [pltpu.make_async_copy(a, b, sems.at[i]) for i, (a, b) in enumerate(pairs)]
    for copy in copies:
        copy.start()
    return copies


def pack_kernel(tile_in, cell_in, mass_in, *refs):
    planes, tiles, per_tile = cell_in.shape
    out_refs = refs[:planes]
    tile_ref, cell_ref, mass_ref, wide, taken, sems = refs[planes:]
    copies = fetch(((tile_in, tile_ref), (cell_in, cell_ref), (mass_in, mass_ref)), sems)
    half = per_tile // TC
    size = 2 * half
    groups, rows, _ = out_refs[0].shape
    cap = rows // size - 1
    per_owner = L // groups // TR * (L // TC)
    me = lax.axis_index("pix")
    lane = lax.broadcasted_iota(jnp.int32, (1, TC), 1)
    for out_ref in out_refs:
        out_ref[...] = jnp.zeros_like(out_ref)
    for copy in copies:
        copy.wait()
    for p in range(planes):
        out_ref = out_refs[p]
        for i in range(half):
            at = slice(i * TC, (i + 1) * TC)
            wide[i] = cell_ref[p, :, at].astype(jnp.float32)
            wide[half + i] = mass_ref[p, :, at].astype(jnp.float32)
        total = jnp.sum(jnp.sum(wide[half:], axis=0), axis=0, keepdims=True)
        total = jnp.sum(total, axis=1, keepdims=True)
        tail = jnp.where(lane < cap, -1.0, jnp.where(lane == cap, total, 0.0))
        out_ref[:, cap * size :, :] = jnp.broadcast_to(tail[None], (groups, size, TC))

        def clear(o, _):
            taken[o] = 0
            return 0

        lax.fori_loop(0, groups, clear, 0)

        def tile(t, _):
            b = tile_ref[p, me * tiles + t]
            owner = b // per_owner
            rank = taken[owner]
            taken[owner] = rank + 1
            for i in range(size):
                out_ref[owner, pl.ds(rank * size + i, 1), :] = wide[i, pl.ds(t, 1), :]
            where_at = (b - owner * per_owner).astype(jnp.float32)
            old = out_ref[owner, cap * size : cap * size + 1, :]
            out_ref[owner, cap * size : cap * size + 1, :] = jnp.where(lane == rank, where_at, old)
            return 0

        lax.fori_loop(0, tiles, tile, 0, unroll=4)


def signal_all(peers):
    barrier = pltpu.get_barrier_semaphore()
    for peer in peers:
        pl.semaphore_signal(barrier, inc=1, device_id=peer, device_id_type=MESH)
    pl.semaphore_wait(barrier, len(peers))


def remote(source, target, send, recv, peer):
    return pltpu.make_async_remote_copy(
        src_ref=source,
        dst_ref=target,
        send_sem=send,
        recv_sem=recv,
        device_id=peer,
        device_id_type=MESH,
    )


def lensing_kernel(
    out0, out1, coef_in, dist_in, inv_in, twist_in_ref, high_in, low_in, colh_in, coll_in, backh_in, backl_in,
    conv_ref, one_ref, two_ref,
    coef_ref, dist_ref, inv_ref, twist_ref, high_ref, low_ref, colh_ref, coll_ref, backh_ref, backl_ref,
    tsem, note, far_note, note_sems,
    box, slots, place, field, held_row, sending, arrived, held, twist_in, kern, back, leaving, landed,
    lsend, lrecv, psend, precv, fsend, frecv, rsend, rrecv,
):
    out_refs = (out0, out1)
    planes = 2
    groups, message, _ = out0.shape
    slab = L // groups
    half = 4
    size = 2 * half
    cap = message // size - 1
    span = held_row.shape[2]
    chunks = slab // span
    pitch = slots.shape[1] // (cap * groups)
    tile_rows = slab // TR
    me, shell = lax.axis_index("pix"), lax.axis_index("shell")
    flipped = partners(me)
    tables = fetch(
        zip(
            (coef_in, dist_in, inv_in, twist_in_ref, high_in, low_in, colh_in, coll_in, backh_in, backl_in),
            (coef_ref, dist_ref, inv_ref, twist_ref, high_ref, low_ref, colh_ref, coll_ref, backh_ref, backl_ref),
        ),
        tsem,
    )
    for copy in tables[:3]:
        copy.wait()
    note[...] = jnp.zeros_like(note)
    for p in range(planes):
        note[p : p + 1, :] = jnp.full((1, TC), coef_ref[p], jnp.float32)
        note[planes + p : planes + p + 1, :] = jnp.full((1, TC), dist_ref[p], jnp.float32)
    signal_all([{"pix": flipped(m)} for m in range(1, groups)] + [{"shell": 1 - shell}])

    sent = pl.ds(0, cap * size + 1)

    def direct(p, m):
        peer = flipped(m)
        return remote(
            out_refs[p].at[peer, sent], box.at[p, me, sent], lsend.at[p, m], lrecv.at[p, m], {"pix": peer}
        )

    def landing(p, m):
        peer = flipped(m)
        return remote(
            out_refs[p].at[peer, sent], box.at[p, peer, sent], lsend.at[p, m], lrecv.at[p, m], {"pix": peer}
        )

    def onward(p, m):
        source = flipped(m)
        first = out_refs[p].at[me, sent] if isinstance(m, int) and m == 0 else box.at[p, source, sent]
        return remote(first, box.at[planes + p, source, sent], psend.at[p, m], precv.at[p, m], {"shell": 1 - shell})

    for m in range(1, groups):
        for p in range(planes):
            direct(p, m).start()
    told = remote(note, far_note, note_sems.at[0], note_sems.at[1], {"shell": 1 - shell})
    told.start()
    for p in range(planes):
        onward(p, 0).start()
        box[p, me] = out_refs[p][me]

    signed_v, weight = column_info(me, groups)
    inner_id = lax.broadcasted_iota(jnp.int32, (INNER, INNER), 0)

    def prepare(k, _):
        for i in range(4):
            twist_in[i, k] = jnp.broadcast_to(twist_ref[i, pl.ds(k, 1), :], (INNER, INNER)).T
        u = k + OUTER * inner_id
        signed_u = jnp.where(u >= L // 2, u - L, u).astype(jnp.float32)
        scale = jnp.where(u == L // 2, 0.0, weight)
        uu, vv = signed_u * signed_u, signed_v * signed_v
        over = scale / jnp.maximum(uu + vv, 1.0)
        kern[0, k] = (vv - uu) * over
        kern[1, k] = 2.0 * signed_v * signed_u * over
        return 0

    as_small = lambda ids: ids.astype(jnp.float32).astype(jnp.bfloat16)
    short, narrow = 2 * TR, TC // 2
    row_id = as_small(lax.broadcasted_iota(jnp.int32, (short, TC), 0))
    col_id = as_small(lax.broadcasted_iota(jnp.int32, (narrow, TC), 0))
    one, zero = jnp.ones((), jnp.bfloat16), jnp.zeros((), jnp.bfloat16)

    def deposit(q, s):
        for c in range(cap):
            entry = box[q, s, c * size : (c + 1) * size, :]
            cells = entry[:half].astype(jnp.int32)
            cell_rows = as_small(cells // TC + TR * ((cells // narrow) % 2))
            cell_cols = as_small(cells % narrow)
            weights = entry[half:].astype(jnp.bfloat16)
            row_hot, col_hot = [], []
            for i in range(half):
                row_hot.append(jnp.where(row_id == cell_rows[i : i + 1], weights[i : i + 1], zero))
                col_hot.append(jnp.where(col_id == cell_cols[i : i + 1], one, zero))
            sums = lax.dot_general(
                jnp.concatenate(row_hot, axis=1),
                jnp.concatenate(col_hot, axis=1),
                (((1,), (1,)), ((), ())),
                preferred_element_type=jnp.float32,
            )
            at = pl.ds(pl.multiple_of((c * groups + s) * pitch, 8), TR)
            slots[q, at, :] = jnp.concatenate([sums[:TR], sums[TR:]], axis=1)

    def near_block(m):
        def one_plane(p, _):
            deposit(p, flipped(m))
            return 0

        lax.fori_loop(0, planes, one_plane, 0)

    def far_block(m):
        for p in range(planes):
            onward(p, m).wait_recv()

        def one_plane(p, _):
            deposit(planes + p, flipped(m))
            return 0

        lax.fori_loop(0, planes, one_plane, 0)

    def take(m):
        for p in range(planes):
            landing(p, m).wait_recv()
            onward(p, m).start()

    lag = 4
    near_block(0)

    def early(m, _):
        take(m)
        near_block(m)
        return 0

    lax.fori_loop(1, lag, early, 0)

    def steady(m, _):
        take(m)
        near_block(m)
        far_block(m - lag)
        return 0

    lax.fori_loop(lag, groups, steady, 0)

    def late(m, _):
        far_block(m)
        return 0

    lax.fori_loop(groups - lag, groups, late, 0)

    for copy in tables[3:]:
        copy.wait()
    told.wait()
    lane_id = lax.broadcasted_iota(jnp.int32, (groups, TC), 1)
    tile_id = ((lane_id % tile_rows) * OUTER + lane_id // tile_rows).astype(jnp.float32)
    gains, shifts = [[], []], [0.0, 0.0]
    for q in range(2 * planes):
        tails = box[q, :, cap * size, :]
        hot = [jnp.where(tails[:, c : c + 1] == tile_id, 1.0, 0.0) for c in range(cap)]
        place[q] = jnp.concatenate(hot, axis=0).T.astype(jnp.bfloat16)
        total = jnp.sum(tails[:, cap : cap + 1], axis=0, keepdims=True)
        notes, p = (note, q) if q < planes else (far_note, q - planes)
        coef, dist = notes[p : p + 1, 0:1], notes[planes + p : planes + p + 1, 0:1]
        for i in range(planes):
            mixed = coef * (1.0 - inv_ref[i] * dist)
            if q >= planes:
                mixed = jnp.where(shell > 0, mixed, 0.0)
            elif q > i:
                mixed = jnp.zeros_like(mixed)
            gains[i].append(mixed * ((L * L) / total))
            shifts[i] = shifts[i] + mixed

    def rows_of(c):
        return pl.ds(pl.multiple_of(c * span, span), span)

    peers = groups - 1

    def go_start(c):
        for m in range(1, groups):
            peer = flipped(m)
            remote(
                sending.at[peer, :, rows_of(c), :],
                arrived.at[me, :, rows_of(c), :],
                fsend.at[c],
                frecv.at[c],
                {"pix": peer},
            ).start()

    def go_all(c):
        return remote(
            sending.at[pl.ds(0, peers), :, rows_of(c), :],
            arrived.at[pl.ds(0, peers), :, rows_of(c), :],
            fsend.at[c],
            frecv.at[c],
            {"pix": flipped(1)},
        )

    def back_start(f, c):
        for m in range(1, groups):
            peer = flipped(m)
            remote(
                leaving.at[peer, f, :, rows_of(c), :],
                landed.at[me, f, :, rows_of(c), :],
                rsend.at[f, c],
                rrecv.at[f, c],
                {"pix": peer},
            ).start()

    def back_all(f, c):
        return remote(
            leaving.at[pl.ds(0, peers), f, :, rows_of(c), :],
            landed.at[pl.ds(0, peers), f, :, rows_of(c), :],
            rsend.at[f, c],
            rrecv.at[f, c],
            {"pix": flipped(1)},
        )

    def field_rows(r, n):
        return pl.ds(pl.multiple_of(r * TC + n * tile_rows, tile_rows), tile_rows)

    def forward_rows(c, _):
        def mass_rows(j, _):
            r = c * (span // tile_rows) + 2 * j
            sums = []
            for q in range(2 * planes):
                pair = jnp.concatenate(
                    [slots[q, pl.ds(r + i, cap * groups, stride=pitch), :] for i in range(2)], axis=1
                )
                high = pair.astype(jnp.bfloat16)
                rest = pair - high.astype(jnp.float32)
                middle = rest.astype(jnp.bfloat16)
                low = (rest - middle.astype(jnp.float32)).astype(jnp.bfloat16)
                dot = lambda part: jnp.dot(place[q], part, preferred_element_type=jnp.float32)
                sums.append(dot(high) + (dot(middle) + dot(low)))
            for i in range(planes):
                value = gains[i][0] * sums[0]
                for q in range(1, 2 * planes):
                    value = value + gains[i][q] * sums[q]
                value = value - shifts[i]
                for e in range(2):
                    at = pl.ds(pl.multiple_of((r + e) * TC, TC), TC)
                    field[i, at, :] = value[:, e * TC : (e + 1) * TC]
            return 0

        lax.fori_loop(0, span // tile_rows // 2, mass_rows, 0)

        def radix(j, _):
            r = c * (span // tile_rows) + j
            near = pl.ds(pl.multiple_of(j * tile_rows, tile_rows), tile_rows)
            z = fft_list(
                [
                    tuple(field[i, field_rows(r, n), :] for i in range(2))
                    for n in range(OUTER)
                ],
                -1,
            )
            for k in range(1, HALF_BLOCKS):
                (ar, ai), (br, bi) = z[k], z[OUTER - k]
                held_row[k - 1, 0, near, :INNER] = 0.5 * (ar + br)
                held_row[k - 1, 0, near, INNER:] = 0.5 * (ai - bi)
                held_row[k - 1, 1, near, :INNER] = 0.5 * (ai + bi)
                held_row[k - 1, 1, near, INNER:] = 0.5 * (br - ar)
            for p in range(2):
                held_row[HALF_BLOCKS - 1, p, near, :INNER] = z[0][p]
                held_row[HALF_BLOCKS - 1, p, near, INNER:] = z[HALF_BLOCKS][p]
            return 0

        lax.fori_loop(0, span // tile_rows, radix, 0)

        def block(j, _):
            b = (me // 2 + 1 + j) % HALF_BLOCKS
            value = held_row[b].reshape(2 * span, 2 * INNER)
            result = three_pass(split_value(value), (high_ref[b], low_ref[b]), ((1,), (0,)))
            for p in range(2):
                for part in range(2):
                    sending[2 * b + p, part, rows_of(c), :] = result[
                        p * span : (p + 1) * span, part * INNER : (part + 1) * INNER
                    ]
            return 0

        lax.fori_loop(0, HALF_BLOCKS, block, 0)
        go_start(c)
        for part in range(2):
            arrived[me, part, rows_of(c), :] = sending[me, part, rows_of(c), :]
        return 0

    lax.fori_loop(0, chunks, forward_rows, 0)

    def show(t, _):
        for i in range(planes):
            for n in range(OUTER):
                for r in range(0, TR, 8):
                    rows = pl.ds(pl.multiple_of(t * TR + r, 8), 8)
                    held_at = pl.ds(r * TC + n * tile_rows + t, 8, stride=TC)
                    conv_ref[i, rows, n * TC : (n + 1) * TC] = field[i, held_at, :]
        return 0

    lax.fori_loop(0, tile_rows, show, 0)
    lax.fori_loop(0, OUTER, prepare, 0)
    for p in range(planes):
        onward(p, 0).wait_send()

        def settle(m, _):
            direct(p, m).wait_send()
            onward(p, m).wait_send()
            return 0

        lax.fori_loop(1, groups, settle, 0)

    def forward_columns(c, _):
        go_all(c).wait_recv()

        def radix(t, _):
            rows = pl.ds(pl.multiple_of(c * span + t * 8, 8), 8)
            z = fft_list([(arrived[n, 0, rows, :], arrived[n, 1, rows, :]) for n in range(OUTER)], -1)
            for k in range(OUTER):
                re, im = z[k]
                if k:
                    cs, sn = twist_in[0, k, rows, :], twist_in[1, k, rows, :]
                    re, im = re * cs - im * sn, re * sn + im * cs
                held[k, 0, rows, :] = re
                held[k, 1, rows, :] = im
            return 0

        lax.fori_loop(0, span // 8, radix, 0)
        return 0

    lax.fori_loop(0, chunks, forward_columns, 0)
    for c in range(chunks):
        go_all(c).wait_send()

    def middle(j, _):
        pair = jnp.concatenate([held[2 * j + i].reshape(2 * INNER, INNER) for i in range(2)], axis=1)
        spectrum = three_pass((colh_ref[...], coll_ref[...]), split_value(pair), ((1,), (0,)))
        for i in range(2):
            k = 2 * j + i
            mine = spectrum[:, i * INNER : (i + 1) * INNER]
            fields = jnp.concatenate(
                [
                    jnp.concatenate([mine[:INNER] * kern[f, k], mine[INNER:] * kern[f, k]], axis=0)
                    for f in range(2)
                ],
                axis=1,
            )
            result = three_pass((backh_ref[...], backl_ref[...]), split_value(fields), ((1,), (0,)))
            cs, sn = twist_in[2, k], twist_in[3, k]
            for f in range(2):
                at = slice(f * INNER, (f + 1) * INNER)
                re, im = result[:INNER, at], result[INNER:, at]
                back[f, k, 0] = re * cs + im * sn
                back[f, k, 1] = im * cs - re * sn
        return 0

    lax.fori_loop(0, OUTER // 2, middle, 0)

    def inverse_columns(q, _):
        f, c = q // chunks, q % chunks

        def radix(t, _):
            rows = pl.ds(pl.multiple_of(c * span + t * 8, 8), 8)
            x = fft_list([(back[f, k, 0, rows, :], back[f, k, 1, rows, :]) for k in range(OUTER)], 1)
            for n in range(OUTER):
                leaving[n, f, 0, rows, :] = x[n][0]
                leaving[n, f, 1, rows, :] = x[n][1]
            return 0

        lax.fori_loop(0, span // 8, radix, 0)
        back_start(f, c)
        for part in range(2):
            landed[me, f, part, rows_of(c), :] = leaving[me, f, part, rows_of(c), :]
        return 0

    lax.fori_loop(0, 2 * chunks, inverse_columns, 0)

    for f, out_ref in enumerate((one_ref, two_ref)):

        def inverse_rows(c, _):
            back_all(f, c).wait_recv()

            def block(b, _):
                value = jnp.concatenate(
                    [
                        jnp.concatenate(
                            [landed[2 * b + p, f, part, rows_of(c), :] for part in range(2)], axis=1
                        )
                        for p in range(2)
                    ],
                    axis=0,
                )
                held_row[b] = three_pass(
                    split_value(value), (high_ref[b], low_ref[b]), ((1,), (1,))
                ).reshape(2, span, 2 * INNER)
                return 0

            lax.fori_loop(0, HALF_BLOCKS, block, 0)

            def radix(t, _):
                near = pl.ds(pl.multiple_of(t * 8, 8), 8)
                rows = pl.ds(pl.multiple_of(c * span + t * 8, 8), 8)
                z = [None] * OUTER
                last = HALF_BLOCKS - 1
                z[0] = (held_row[last, 0, near, :INNER], held_row[last, 1, near, :INNER])
                z[HALF_BLOCKS] = (held_row[last, 0, near, INNER:], held_row[last, 1, near, INNER:])
                for k in range(1, HALF_BLOCKS):
                    ar, ai = held_row[k - 1, 0, near, :INNER], held_row[k - 1, 0, near, INNER:]
                    br, bi = held_row[k - 1, 1, near, :INNER], held_row[k - 1, 1, near, INNER:]
                    z[k] = (ar - bi, ai + br)
                    z[OUTER - k] = (ar + bi, br - ai)
                x = fft_list(z, 1)
                for n in range(OUTER):
                    for p in range(2):
                        out_ref[p, rows, n * INNER : (n + 1) * INNER] = x[n][p]
                return 0

            lax.fori_loop(0, span // 8, radix, 0)
            return 0

        lax.fori_loop(0, chunks, inverse_rows, 0)

    for c in range(chunks):
        for f in range(2):
            back_all(f, c).wait_send()


def place_kernel(*refs):
    count = (len(refs) - 1) // 2
    for copy in fetch(zip(refs[:count], refs[count:-1]), refs[-1]):
        copy.wait()


def column_info(me, groups):
    lane = lax.broadcasted_iota(jnp.int32, (1, INNER), 1)
    b = me // 2
    last = b == HALF_BLOCKS - 1
    upper = lane // (INNER // 2)
    folded = OUTER * (lane - upper * (INNER // 2)) + HALF_BLOCKS * upper
    mine = jnp.where(last, folded, b + 1 + OUTER * lane)
    weight = jnp.where(last & (mine > 0), 2.0, 1.0) / (L * L)
    return jnp.where(mine >= L // 2, mine - L, mine).astype(jnp.float32), weight


def call(body, outs, scratch=(), smem=(0,), count=1, megabytes=48, flops=0, group=None, hbm=(), out_space=pltpu.VMEM):
    space = [
        pl.BlockSpec(
            memory_space=pltpu.SMEM if i in smem else pltpu.HBM if i in hbm else pltpu.VMEM
        )
        for i in range(count)
    ]
    return pl.pallas_call(
        body,
        out_shape=outs,
        in_specs=space,
        out_specs=jax.tree.map(lambda _: pl.BlockSpec(memory_space=out_space), outs),
        scratch_shapes=list(scratch),
        compiler_params=pltpu.CompilerParams(
            vmem_limit_bytes=megabytes << 20,
            collective_id=group,
            has_side_effects=group is not None,
        ),
        cost_estimate=pl.CostEstimate(flops=flops, bytes_accessed=4 << 20, transcendentals=0),
    )


def shape(*dims):
    return jax.ShapeDtypeStruct(dims, jnp.float32)


def local_fast(block_tile, cell_index, masses, plane_coef, plane_dist, source_inv):
    groups = lax.axis_size("pix")
    planes, local_tiles, per_tile = cell_index.shape
    slab = L // groups
    cap = max(1, 2 * local_tiles // groups)
    size = 2 * per_tile // TC
    message = (cap + 1) * size
    vmem = lambda *dims: pltpu.VMEM(dims, jnp.float32)
    dma = lambda *dims: pltpu.SemaphoreType.DMA(dims)
    outgoing = call(
        pack_kernel,
        [shape(groups, message, TC)] * planes,
        [
            pltpu.SMEM(block_tile.shape, jnp.int32),
            pltpu.VMEM(cell_index.shape, jnp.int32),
            pltpu.VMEM(masses.shape, jnp.bfloat16),
            vmem(size, local_tiles, TC),
            pltpu.SMEM((groups,), jnp.int32),
            dma(3),
        ],
        smem=(),
        hbm=(0, 1, 2),
        count=3,
        megabytes=16,
        flops=1 << 32,
    )(block_tile, cell_index, masses)

    order = row_order(slab)
    row_high, row_low = row_tables()
    forth, natural = column_table(order), column_table(np.arange(INNER))
    col_high, col_low = split_table(forth)
    back_high, back_low = split_table(natural.T)
    span = slab // CHUNKS
    pitch = 3 * TR // 2
    tables = [jnp.asarray(twiddle_tables(order)), row_high, row_low, col_high, col_low, back_high, back_low]
    results = call(
        lensing_kernel,
        [shape(planes, slab, L)] * 3,
        [pltpu.SMEM(source_inv.shape, jnp.float32)] * 3
        + [pltpu.VMEM(table.shape, table.dtype) for table in tables]
        + [
            dma(3 + len(tables)),
            vmem(8, TC),
            vmem(8, TC),
            dma(2),
            vmem(2 * planes, groups, message, TC),
            vmem(2 * planes, cap * groups * pitch, TC),
            pltpu.VMEM((2 * planes, TC, TC), jnp.bfloat16),
            vmem(planes, TR * TC, TC),
            vmem(HALF_BLOCKS, planes, span, 2 * INNER),
            vmem(groups, 2, slab, INNER),
            vmem(groups, 2, slab, INNER),
            vmem(OUTER, 2, INNER, INNER),
            vmem(4, OUTER, INNER, INNER),
            vmem(2, OUTER, INNER, INNER),
            vmem(2, OUTER, 2, INNER, INNER),
            vmem(groups, 2, 2, slab, INNER),
            vmem(groups, 2, 2, slab, INNER),
            dma(planes, groups),
            dma(planes, groups),
            dma(planes, groups),
            dma(planes, groups),
            dma(CHUNKS),
            dma(CHUNKS),
            dma(2, CHUNKS),
            dma(2, CHUNKS),
        ],
        smem=(),
        hbm=tuple(range(2, 12)),
        count=12,
        megabytes=40,
        flops=1 << 32,
        group=0,
    )(*outgoing, plane_coef, plane_dist, source_inv, *tables)
    return call(
        place_kernel,
        [shape(planes, slab, L)] * 3,
        [dma(3)],
        smem=(),
        out_space=pltpu.HBM,
        count=3,
        megabytes=16,
        flops=1 << 20,
    )(*results)


def solution(mesh):
    placed = (
        P("shell", None),
        P("shell", "pix", None),
        P("shell", "pix", None),
        P("shell"),
        P("shell"),
        P("shell"),
    )
    shells, groups = mesh.shape["shell"], mesh.shape["pix"]

    def body(block_tile, cell_index, *rest):
        fits = (
            shells == 2
            and cell_index.shape[0] == 2
            and groups == OUTER
            and cell_index.shape[2] == 4 * TC
            and cell_index.shape[1] * 2 == groups * 8
        )
        return (local_fast if fits else local)(block_tile, cell_index, *rest)

    return jax.shard_map(
        body,
        mesh=mesh,
        in_specs=placed,
        out_specs=(P("shell", "pix", None), P("shell", "pix", None), P("shell", "pix", None)),
        check_vma=False,
    )
```

```python
from functools import partial
import math

import jax
import jax.numpy as jnp
from jax import lax
from jax.experimental import pallas as pl
from jax.experimental.pallas import tpu as pltpu
from jax.sharding import PartitionSpec as P
import numpy as np

L = 2048
TR = 16
TC = 128


HIGHEST = lax.Precision.HIGHEST


def entering(value, axis, join, neutral):
    count, mine = (lax.axis_size(axis), lax.axis_index(axis))
    pieces = jax.tree.map(lambda part: lax.all_gather(part, axis), value)
    running = jax.tree.map(
        lambda part, zero: jnp.full_like(part, 0) + jnp.asarray(zero, part.dtype), value, neutral
    )

    def lap(position, running):
        longer = join(running, jax.tree.map(lambda part: part[position], pieces))
        return jax.tree.map(lambda new, old: jnp.where(position < mine, new, old), longer, running)

    return lax.fori_loop(0, count - 1, lap, running)


def dft_table(left_size, right_size, period, sign_value):
    left_idx = jnp.arange(left_size)[:, None]
    right_idx = jnp.arange(right_size)[None, :]
    angle = 2.0 * math.pi / period * (left_idx * right_idx % period).astype(jnp.float32)
    return (jnp.cos(angle), sign_value * jnp.sin(angle))


def mix_outer(table, real_part, imag_part):
    cosine, sine_part = table
    contract = partial(jnp.einsum, "ab,...bc->...ac", precision=HIGHEST)
    return (
        contract(cosine, real_part) - contract(sine_part, imag_part),
        contract(sine_part, real_part) + contract(cosine, imag_part),
    )


def mix_inner(table, real_part, imag_part):
    cosine, sine_part = table
    product = partial(jnp.matmul, precision=HIGHEST)
    return (
        product(real_part, cosine) - product(imag_part, sine_part),
        product(real_part, sine_part) + product(imag_part, cosine),
    )


def twist(table, real_part, imag_part):
    cosine, sine_part = table
    return (real_part * cosine - imag_part * sine_part, real_part * sine_part + imag_part * cosine)


def transform_last(real_part, imag_part, sign_value):
    length = real_part.shape[-1]
    inner = math.gcd(length, 128)
    outer = length // inner
    leading = real_part.shape[:-1]
    real_part = real_part.reshape(leading + (outer, inner))
    imag_part = imag_part.reshape(leading + (outer, inner))
    outer_table = dft_table(outer, outer, outer, sign_value)
    inner_table = dft_table(inner, inner, inner, sign_value)
    twiddle = dft_table(outer, inner, length, sign_value)
    if sign_value < 0:
        real_part, imag_part = mix_outer(outer_table, real_part, imag_part)
        real_part, imag_part = twist(twiddle, real_part, imag_part)
        real_part, imag_part = mix_inner(inner_table, real_part, imag_part)
    else:
        real_part, imag_part = mix_inner(inner_table, real_part, imag_part)
        real_part, imag_part = twist(twiddle, real_part, imag_part)
        real_part, imag_part = mix_outer(outer_table, real_part, imag_part)
    return (real_part.reshape(leading + (length,)), imag_part.reshape(leading + (length,)))


def frequency_of(position, length):
    inner = math.gcd(length, 128)
    outer = length // inner
    frequency = position // inner + outer * (position % inner)
    signed = jnp.where(frequency >= length // 2, frequency - length, frequency).astype(jnp.float32)
    keep_mask = (frequency != length // 2).astype(jnp.float32)
    return (signed, keep_mask)


def add_pairs(earlier_pair, later_pair):
    return (earlier_pair[0] + later_pair[0], earlier_pair[1] + later_pair[1])


def deposit_group(item):
    cell_ids, weights = item
    tile_rows = cell_ids // TC
    tile_cols = cell_ids % TC
    row_hot = jnp.where(
        tile_rows[:, None, :] == jnp.arange(TR)[None, :, None],
        weights[:, None, :],
        jnp.zeros((), jnp.bfloat16),
    )
    col_hot = (tile_cols[:, :, None] == jnp.arange(TC)[None, None, :]).astype(jnp.bfloat16)
    return jnp.einsum("grk,gkc->grc", row_hot, col_hot, preferred_element_type=jnp.float32)


def rows_to_sending(packed, groups, slab, cols_own):
    count, fields = (packed.shape[0], packed.shape[1])
    return (
        packed.reshape(count, fields, slab, groups, cols_own)
        .transpose(3, 0, 1, 4, 2)
        .reshape(groups, count, fields, cols_own * slab)
    )


def arrived_to_columns(arrived, groups, slab, cols_own):
    count, fields = (arrived.shape[1], arrived.shape[2])
    return (
        arrived.reshape(groups, count, fields, cols_own, slab)
        .transpose(1, 2, 3, 0, 4)
        .reshape(count, fields, cols_own, groups * slab)
    )


def columns_to_sending(stacked, groups, slab, cols_own):
    count, fields = (stacked.shape[0], stacked.shape[1])
    return (
        stacked.reshape(count, fields, cols_own, groups, slab)
        .transpose(3, 0, 1, 2, 4)
        .reshape(groups, count, fields, cols_own * slab)
    )


def landed_to_rows(landed, groups, slab, cols_own):
    count, fields = (landed.shape[1], landed.shape[2])
    return (
        landed.reshape(groups, count, fields, cols_own, slab)
        .transpose(1, 2, 4, 0, 3)
        .reshape(count, fields, slab, groups * cols_own)
    )


def local(block_tile, cell_index, masses, plane_coef, plane_dist, source_inv):
    groups = lax.axis_size("pix")
    my_index = lax.axis_index("pix")
    planes, local_tiles, per_tile = cell_index.shape
    slab = L // groups
    per_owner = slab // TR * (L // TC)
    cap = max(1, 2 * local_tiles // groups)
    flat = TR * TC
    batch_tiles = 8
    deposited = lax.map(
        deposit_group,
        (cell_index.reshape(-1, batch_tiles, per_tile), masses.reshape(-1, batch_tiles, per_tile)),
    )
    tile_sums = deposited.reshape(planes, local_tiles, flat)
    table = block_tile.reshape(planes, groups, local_tiles)
    owner = table // per_owner
    earlier = jnp.arange(local_tiles)[:, None] < jnp.arange(local_tiles)[None, :]
    same_owner = owner[:, :, :, None] == owner[:, :, None, :]
    rank = jnp.sum(jnp.where(same_owner & earlier[None, None], 1, 0), axis=2)
    slot = owner * cap + rank
    my_slots = lax.dynamic_index_in_dim(slot, my_index, axis=1, keepdims=False)
    slot_grid = jnp.arange(groups)[:, None] * cap + jnp.arange(cap)[None, :]
    send_hot = (my_slots[:, None, None, :] == slot_grid[None, :, :, None]).astype(jnp.float32)
    outgoing = jnp.einsum("pnct,ptf->npcf", send_hot, tile_sums, precision=HIGHEST)
    incoming = lax.all_to_all(outgoing, "pix", split_axis=0, concat_axis=0, tiled=True)
    local_index = table - my_index * per_owner
    is_mine = owner == my_index
    tile_hot = (is_mine[..., None] & (local_index[..., None] == jnp.arange(per_owner))).astype(
        jnp.float32
    )
    slot_hot = (rank[..., None] == jnp.arange(cap)).astype(jnp.float32)
    placing = jnp.einsum("pstl,pstc->plsc", tile_hot, slot_hot, precision=HIGHEST)
    slab_tiles = jnp.einsum("plsc,spcf->plf", placing, incoming, precision=HIGHEST)
    density = (
        slab_tiles.reshape(planes, slab // TR, L // TC, TR, TC)
        .transpose(0, 1, 3, 2, 4)
        .reshape(planes, slab, L)
    )
    total = lax.psum(jnp.sum(density, axis=(1, 2)), "pix")
    contrast = density / (total / (L * L))[:, None, None] - 1.0
    near_local = jnp.cumsum(plane_coef[:, None, None] * contrast, axis=0)
    far_local = jnp.cumsum((plane_coef * plane_dist)[:, None, None] * contrast, axis=0)
    blank = jnp.zeros((slab, L), jnp.float32)
    near_before, far_before = entering(
        (near_local[-1], far_local[-1]), "shell", add_pairs, (blank, blank)
    )
    convergence = near_before + near_local - source_inv[:, None, None] * (far_before + far_local)
    cols_own = L // groups
    wave_x, keep_x = frequency_of(my_index * cols_own + jnp.arange(cols_own), L)
    wave_y, keep_y = frequency_of(jnp.arange(L), L)
    wave_x = wave_x[:, None]
    wave_y = wave_y[None, :]
    both_keep = keep_x[:, None] * keep_y[None, :]
    wave_power = jnp.maximum(wave_x * wave_x + wave_y * wave_y, 1.0)
    kernel_one = both_keep * (wave_x * wave_x - wave_y * wave_y) / wave_power
    kernel_two = both_keep * 2.0 * wave_x * wave_y / wave_power
    scale = 1.0 / (L * L)
    spec_real, spec_imag = transform_last(convergence[0::2], convergence[1::2], -1.0)
    sending = rows_to_sending(jnp.stack([spec_real, spec_imag], axis=1), groups, slab, cols_own)
    arrived = lax.all_to_all(sending, "pix", split_axis=0, concat_axis=0, tiled=True)
    columns = arrived_to_columns(arrived, groups, slab, cols_own)
    row_real, row_imag = transform_last(columns[:, 0], columns[:, 1], -1.0)
    first_real, first_imag = transform_last(row_real * kernel_one, row_imag * kernel_one, 1.0)
    second_real, second_imag = transform_last(row_real * kernel_two, row_imag * kernel_two, 1.0)
    stacked = jnp.stack([first_real, first_imag, second_real, second_imag], axis=1)
    landed = lax.all_to_all(
        columns_to_sending(stacked, groups, slab, cols_own),
        "pix",
        split_axis=0,
        concat_axis=0,
        tiled=True,
    )
    row_layout = landed_to_rows(landed, groups, slab, cols_own)
    even_one, odd_one = transform_last(row_layout[:, 0], row_layout[:, 1], 1.0)
    even_two, odd_two = transform_last(row_layout[:, 2], row_layout[:, 3], 1.0)
    shear_one = jnp.stack([even_one, odd_one], axis=1).reshape(planes, slab, L)
    shear_two = jnp.stack([even_two, odd_two], axis=1).reshape(planes, slab, L)
    return (convergence, shear_one * scale, shear_two * scale)


INNER = 128
OUTER = L // INNER
HALF_BLOCKS = OUTER // 2
CHUNKS = 4
MESH = pl.DeviceIdType.MESH


def block_columns():
    cols = np.zeros((HALF_BLOCKS, INNER), np.int64)
    for b in range(HALF_BLOCKS - 1):
        cols[b] = b + 1 + OUTER * np.arange(INNER)
    half = np.arange(INNER // 2)
    cols[-1] = np.concatenate([OUTER * half, HALF_BLOCKS + OUTER * half])
    return cols


def split_table(table):
    high = table.astype(jnp.bfloat16)
    low = (table - high.astype(np.float64)).astype(jnp.bfloat16)
    return high, low


def row_tables(chunks):
    n2 = np.arange(INNER)
    out = np.zeros((HALF_BLOCKS, 2 * INNER, 2 * INNER))
    cols = block_columns()
    for b in range(HALF_BLOCKS):
        angle = 2 * np.pi / L * ((n2[:, None] * cols[b][None, :]) % L)
        co, si = np.cos(angle), np.sin(angle)
        if b < HALF_BLOCKS - 1:
            out[b] = np.block([[co, -si], [si, co]])
        else:
            h = INNER // 2
            out[b, :INNER, :h] = co[:, :h]
            out[b, :INNER, INNER : INNER + h] = -si[:, :h]
            out[b, INNER:, h:INNER] = co[:, h:]
            out[b, INNER:, INNER + h :] = -si[:, h:]
    out = out.reshape(HALF_BLOCKS, 2 * INNER, 2, chunks, INNER // chunks)
    return split_table(out.transpose(0, 3, 2, 4, 1).reshape(HALF_BLOCKS, 2 * INNER, 2 * INNER))


def row_order(slab):
    at = np.arange(slab)
    rows = slab // TR
    return (at % rows) * TR + at // rows


def column_table(order):
    idx = np.arange(INNER)
    angle = 2 * np.pi / INNER * ((idx[:, None] * order[None, :]) % INNER)
    co, si = np.cos(angle), np.sin(angle)
    return np.block([[co, si], [-si, co]])


def twiddle_tables(order):
    out = []
    for rows in (order, np.arange(INNER)):
        angle = 2 * np.pi / L * (np.arange(OUTER)[:, None] * rows[None, :])
        out += [np.cos(angle), -np.sin(angle)]
    return np.stack(out).astype(np.float32)


def times_root(value, k, n, sign):
    re, im = value
    k = k % n
    if k == 0:
        return value
    if 4 * k == n:
        return (-im, re) if sign > 0 else (im, -re)
    angle = 2 * math.pi * k / n
    c, s = math.cos(angle), sign * math.sin(angle)
    if 8 * k == n or 8 * k == 3 * n:
        if c > 0:
            return ((re - im) * c, (re + im) * c) if sign > 0 else ((re + im) * c, (im - re) * c)
        c = -c
        return ((re + im) * -c, (re - im) * c) if sign > 0 else ((im - re) * c, (re + im) * -c)
    return (re * c - im * s, re * s + im * c)


def fft_list(values, sign):
    n = len(values)
    if n == 1:
        return values
    even = fft_list(values[0::2], sign)
    odd = fft_list(values[1::2], sign)
    odd = [times_root(v, k, n, sign) for k, v in enumerate(odd)]
    return [(a[0] + b[0], a[1] + b[1]) for a, b in zip(even, odd)] + [
        (a[0] - b[0], a[1] - b[1]) for a, b in zip(even, odd)
    ]


def split_value(value):
    high = value.astype(jnp.bfloat16)
    return high, (value - high.astype(jnp.float32)).astype(jnp.bfloat16)


def three_pass(left, right, dims):
    dot = lambda a, b: lax.dot_general(a, b, (dims, ((), ())), preferred_element_type=jnp.float32)
    return dot(left[0], right[0]) + (dot(left[0], right[1]) + dot(left[1], right[0]))


def partners(me):
    steps = [(bit, bit - 2 * bit * ((me // bit) % 2)) for bit in (1, 2, 4, 8)]

    def flipped(mask):
        peer = me
        for bit, step in steps:
            if not isinstance(mask, int):
                peer = peer + ((mask // bit) % 2) * step
            elif mask & bit:
                peer = peer + step
        return peer

    return flipped


def fetch(pairs, sems):
    copies = [pltpu.make_async_copy(a, b, sems.at[i]) for i, (a, b) in enumerate(pairs)]
    for copy in copies:
        copy.start()
    return copies


def pack_kernel(tile_in, cell_in, mass_in, *refs):
    planes, tiles, per_tile = cell_in.shape
    out_refs = refs[:planes]
    tile_ref, cell_ref, mass_ref, wide, taken, sems = refs[planes:]
    copies = fetch(((tile_in, tile_ref), (cell_in, cell_ref), (mass_in, mass_ref)), sems)
    half = per_tile // TC
    size = 2 * half
    groups, rows, _ = out_refs[0].shape
    cap = rows // size - 1
    per_owner = L // groups // TR * (L // TC)
    me = lax.axis_index("pix")
    lane = lax.broadcasted_iota(jnp.int32, (1, TC), 1)
    for out_ref in out_refs:
        out_ref[...] = jnp.zeros_like(out_ref)
    for copy in copies:
        copy.wait()
    for p in range(planes):
        out_ref = out_refs[p]
        for i in range(half):
            at = slice(i * TC, (i + 1) * TC)
            wide[i] = cell_ref[p, :, at].astype(jnp.float32)
            wide[half + i] = mass_ref[p, :, at].astype(jnp.float32)
        total = jnp.sum(jnp.sum(wide[half:], axis=0), axis=0, keepdims=True)
        total = jnp.sum(total, axis=1, keepdims=True)
        tail = jnp.where(lane < cap, -1.0, jnp.where(lane == cap, total, 0.0))
        out_ref[:, cap * size :, :] = jnp.broadcast_to(tail[None], (groups, size, TC))

        def clear(o, _):
            taken[o] = 0
            return 0

        lax.fori_loop(0, groups, clear, 0)

        def tile(t, _):
            b = tile_ref[p, me * tiles + t]
            owner = b // per_owner
            rank = taken[owner]
            taken[owner] = rank + 1
            for i in range(size):
                out_ref[owner, pl.ds(rank * size + i, 1), :] = wide[i, pl.ds(t, 1), :]
            where_at = (b - owner * per_owner).astype(jnp.float32)
            old = out_ref[owner, cap * size : cap * size + 1, :]
            out_ref[owner, cap * size : cap * size + 1, :] = jnp.where(lane == rank, where_at, old)
            return 0

        lax.fori_loop(0, tiles, tile, 0, unroll=4)


def signal_all(peers):
    barrier = pltpu.get_barrier_semaphore()
    for peer in peers:
        pl.semaphore_signal(barrier, inc=1, device_id=peer, device_id_type=MESH)
    pl.semaphore_wait(barrier, len(peers))


def remote(source, target, send, recv, peer):
    return pltpu.make_async_remote_copy(
        src_ref=source,
        dst_ref=target,
        send_sem=send,
        recv_sem=recv,
        device_id=peer,
        device_id_type=MESH,
    )


def lensing_kernel(
    out0, out1, coef_in, dist_in, inv_in, twist_in_ref, high_in, low_in, colh_in, coll_in, backh_in, backl_in,
    conv_ref, one_ref, two_ref,
    coef_ref, dist_ref, inv_ref, twist_ref, high_ref, low_ref, colh_ref, coll_ref, backh_ref, backl_ref,
    tsem, note, far_note, note_sems,
    box, slots, place, field, held_row, sending, arrived, held, kern, back, leaving, landed, total_rows,
    lsend, lrecv, psend, precv, fsend, frecv, rsend, rrecv,
):
    out_refs = (out0, out1)
    planes = 2
    groups, message, _ = out0.shape
    slab = L // groups
    half = 4
    size = 2 * half
    cap = message // size - 1
    chunks = sending.shape[1]
    span = INNER // chunks
    both = chunks - 1
    flip = groups // 2
    pitch = slots.shape[1] // (cap * groups)
    tile_rows = slab // TR
    me, shell = lax.axis_index("pix"), lax.axis_index("shell")
    flipped = partners(me)
    tables = fetch(
        zip(
            (coef_in, dist_in, inv_in, twist_in_ref, high_in, low_in, colh_in, coll_in, backh_in, backl_in),
            (coef_ref, dist_ref, inv_ref, twist_ref, high_ref, low_ref, colh_ref, coll_ref, backh_ref, backl_ref),
        ),
        tsem,
    )
    for copy in tables[:3]:
        copy.wait()
    note[...] = jnp.zeros_like(note)
    for p in range(planes):
        note[p : p + 1, :] = jnp.full((1, TC), coef_ref[p], jnp.float32)
        note[planes + p : planes + p + 1, :] = jnp.full((1, TC), dist_ref[p], jnp.float32)
    signal_all([{"pix": flipped(m)} for m in range(1, groups)] + [{"shell": 1 - shell}])

    sent = pl.ds(0, cap * size + 1)

    def direct(p, m):
        peer = flipped(m)
        return remote(
            out_refs[p].at[peer, sent], box.at[p, me, sent], lsend.at[p, m], lrecv.at[p, m], {"pix": peer}
        )

    def landing(p, m):
        peer = flipped(m)
        return remote(
            out_refs[p].at[peer, sent], box.at[p, peer, sent], lsend.at[p, m], lrecv.at[p, m], {"pix": peer}
        )

    def onward(p, m):
        source = flipped(m)
        first = out_refs[p].at[me, sent] if isinstance(m, int) and m == 0 else box.at[p, source, sent]
        return remote(first, box.at[planes + p, source, sent], psend.at[p, m], precv.at[p, m], {"shell": 1 - shell})

    for m in range(1, groups):
        for p in range(planes):
            direct(p, m).start()
    told = remote(note, far_note, note_sems.at[0], note_sems.at[1], {"shell": 1 - shell})
    told.start()
    for p in range(planes):
        onward(p, 0).start()
        box[p, me] = out_refs[p][me]

    own_lines, mirror_lines = column_info(me), column_info((me + flip) % groups)
    signed_v, weight = (
        jnp.concatenate([ours, theirs[both * span :]], axis=0)
        for ours, theirs in zip(own_lines, mirror_lines)
    )
    inner_id = lax.broadcasted_iota(jnp.int32, (INNER + span, INNER), 1)

    def prepare(k, _):
        u = k + OUTER * inner_id
        signed_u = jnp.where(u >= L // 2, u - L, u).astype(jnp.float32)
        scale = jnp.where(u == L // 2, 0.0, weight)
        uu, vv = signed_u * signed_u, signed_v * signed_v
        over = scale / jnp.maximum(uu + vv, 1.0)
        kern[0, k] = (vv - uu) * over
        kern[1, k] = 2.0 * signed_v * signed_u * over
        return 0

    as_small = lambda ids: ids.astype(jnp.float32).astype(jnp.bfloat16)
    short, narrow = 2 * TR, TC // 2
    row_id = as_small(lax.broadcasted_iota(jnp.int32, (short, TC), 0))
    col_id = as_small(lax.broadcasted_iota(jnp.int32, (narrow, TC), 0))
    one, zero = jnp.ones((), jnp.bfloat16), jnp.zeros((), jnp.bfloat16)

    def deposit(q, s):
        for c in range(cap):
            entry = box[q, s, c * size : (c + 1) * size, :]
            cells = entry[:half].astype(jnp.int32)
            cell_rows = as_small(cells // TC + TR * ((cells // narrow) % 2))
            cell_cols = as_small(cells % narrow)
            weights = entry[half:].astype(jnp.bfloat16)
            row_hot, col_hot = [], []
            for i in range(half):
                row_hot.append(jnp.where(row_id == cell_rows[i : i + 1], weights[i : i + 1], zero))
                col_hot.append(jnp.where(col_id == cell_cols[i : i + 1], one, zero))
            sums = lax.dot_general(
                jnp.concatenate(row_hot, axis=1),
                jnp.concatenate(col_hot, axis=1),
                (((1,), (1,)), ((), ())),
                preferred_element_type=jnp.float32,
            )
            at = pl.ds(pl.multiple_of((c * groups + s) * pitch, 8), TR)
            slots[q, at, :] = jnp.concatenate([sums[:TR], sums[TR:]], axis=1)

    def near_block(m):
        def one_plane(p, _):
            deposit(p, flipped(m))
            return 0

        lax.fori_loop(0, planes, one_plane, 0)

    def far_block(m):
        for p in range(planes):
            onward(p, m).wait_recv()

        def one_plane(p, _):
            deposit(planes + p, flipped(m))
            return 0

        lax.fori_loop(0, planes, one_plane, 0)

    def take(m):
        for p in range(planes):
            landing(p, m).wait_recv()
            onward(p, m).start()

    lag = 4
    near_block(0)

    def early(m, _):
        take(m)
        near_block(m)
        return 0

    lax.fori_loop(1, lag, early, 0)

    def steady(m, _):
        take(m)
        near_block(m)
        far_block(m - lag)
        return 0

    lax.fori_loop(lag, groups, steady, 0)

    def late(m, _):
        far_block(m)
        return 0

    lax.fori_loop(groups - lag, groups, late, 0)

    for copy in tables[3:]:
        copy.wait()
    told.wait_recv()
    lane_id = lax.broadcasted_iota(jnp.int32, (groups, TC), 1)
    tile_id = ((lane_id % tile_rows) * OUTER + lane_id // tile_rows).astype(jnp.float32)
    gains, shifts = [[], []], [0.0, 0.0]
    for q in range(2 * planes):
        tails = box[q, :, cap * size, :]
        hot = [jnp.where(tails[:, c : c + 1] == tile_id, 1.0, 0.0) for c in range(cap)]
        place[q] = jnp.concatenate(hot, axis=0).T.astype(jnp.bfloat16)
        total = jnp.sum(tails[:, cap : cap + 1], axis=0, keepdims=True)
        notes, p = (note, q) if q < planes else (far_note, q - planes)
        coef, dist = notes[p : p + 1, 0:1], notes[planes + p : planes + p + 1, 0:1]
        for i in range(planes):
            mixed = coef * (1.0 - inv_ref[i] * dist)
            if q >= planes:
                mixed = jnp.where(shell > 0, mixed, 0.0)
            elif q > i:
                mixed = jnp.zeros_like(mixed)
            gains[i].append(mixed * ((L * L) / total))
            shifts[i] = shifts[i] + mixed

    peers = groups - 1

    def go(c, peer):
        source = sending.at[peer, c] if c < chunks else sending.at[(peer + flip) % groups, both]
        return remote(source, arrived.at[me, c], fsend.at[c], frecv.at[c], {"pix": peer})

    def go_all(c):
        every = pl.ds(0, peers)
        return remote(
            sending.at[every, 0], arrived.at[every, c], fsend.at[c], frecv.at[c], {"pix": flipped(1)}
        )

    def home_any(c, count=peers):
        every = pl.ds(0, count)
        return remote(
            leaving.at[every, c], landed.at[every, 0], rsend.at[c], rrecv.at[c], {"pix": flipped(1)}
        )

    def home_all(c):
        return home_any(c, peers if c < both else flip - 1)

    def field_rows(r, n):
        return pl.ds(pl.multiple_of(r * TC + n * tile_rows, tile_rows), tile_rows)

    def mass_rows(j, _):
        r = 2 * j
        sums = []
        for q in range(2 * planes):
            pair = jnp.concatenate(
                [slots[q, pl.ds(r + i, cap * groups, stride=pitch), :] for i in range(2)], axis=1
            )
            high = pair.astype(jnp.bfloat16)
            rest = pair - high.astype(jnp.float32)
            middle = rest.astype(jnp.bfloat16)
            low = (rest - middle.astype(jnp.float32)).astype(jnp.bfloat16)
            dot = lambda part: jnp.dot(place[q], part, preferred_element_type=jnp.float32)
            sums.append(dot(high) + (dot(middle) + dot(low)))
        for i in range(planes):
            value = gains[i][0] * sums[0]
            for q in range(1, 2 * planes):
                value = value + gains[i][q] * sums[q]
            value = value - shifts[i]
            for e in range(2):
                at = pl.ds(pl.multiple_of((r + e) * TC, TC), TC)
                field[i, at, :] = value[:, e * TC : (e + 1) * TC]
        return 0

    lax.fori_loop(0, TR // 2, mass_rows, 0)

    def row_radix(r, _):
        near = pl.ds(pl.multiple_of(r * tile_rows, tile_rows), tile_rows)
        z = fft_list(
            [tuple(field[i, field_rows(r, n), :] for i in range(2)) for n in range(OUTER)], -1
        )
        for k in range(1, HALF_BLOCKS):
            (ar, ai), (br, bi) = z[k], z[OUTER - k]
            held_row[k - 1, 0, near, :INNER] = 0.5 * (ar + br)
            held_row[k - 1, 0, near, INNER:] = 0.5 * (ai - bi)
            held_row[k - 1, 1, near, :INNER] = 0.5 * (ai + bi)
            held_row[k - 1, 1, near, INNER:] = 0.5 * (br - ar)
        for p in range(2):
            held_row[HALF_BLOCKS - 1, p, near, :INNER] = z[0][p]
            held_row[HALF_BLOCKS - 1, p, near, INNER:] = z[HALF_BLOCKS][p]
        return 0

    lax.fori_loop(0, TR, row_radix, 0)

    def row_block(b):
        value = held_row[b].reshape(2 * slab, 2 * INNER)
        result = three_pass((high_ref[b], low_ref[b]), split_value(value), ((1,), (1,)))
        for p in range(2):
            for c in range(chunks):
                sending[2 * b + p, c] = result[
                    2 * span * c : 2 * span * (c + 1), p * slab : (p + 1) * slab
                ]

    def send_block(j, _):
        b = (me // 2 + 1 + j) % HALF_BLOCKS
        row_block(b)
        for p in range(2):
            for c in (both, chunks):
                peer = 2 * b + p if c < chunks else (2 * b + p + flip) % groups
                pl.when(peer != me)(lambda: go(c, peer).start())
        return 0

    lax.fori_loop(0, HALF_BLOCKS, send_block, 0)
    for c in range(both):
        for m in range(1, groups):
            go(c, flipped(m)).start()
    for c in range(chunks):
        arrived[me, c] = sending[me, c]
    arrived[me, chunks] = sending[(me + flip) % groups, both]

    def show(t, _):
        for i in range(planes):
            for n in range(OUTER):
                for r in range(0, TR, 8):
                    rows = pl.ds(pl.multiple_of(t * TR + r, 8), 8)
                    held_at = pl.ds(r * TC + n * tile_rows + t, 8, stride=TC)
                    conv_ref[i, rows, n * TC : (n + 1) * TC] = field[i, held_at, :]
        return 0

    lax.fori_loop(0, OUTER, prepare, 0)

    def columns(c):
        for t in range(span // 8):
            at, past = slice(t * 8, t * 8 + 8), slice(span + t * 8, span + t * 8 + 8)
            z = fft_list([(arrived[n, c, at, :], arrived[n, c, past, :]) for n in range(OUTER)], -1)
            for k in range(OUTER):
                re, im = z[k]
                if k:
                    cs, sn = twist_ref[0, k : k + 1, :], twist_ref[1, k : k + 1, :]
                    re, im = re * cs - im * sn, re * sn + im * cs
                rows = slice(k * span + t * 8, k * span + t * 8 + 8)
                held[rows, :INNER] = re
                held[rows, INNER:] = im
        rank = pl.ds(pl.multiple_of(c * span, span), span)
        part = 2 * INNER // span
        for g in range(OUTER // part):
            value = held[g * part * span : (g + 1) * part * span, :]
            spectrum = three_pass(split_value(value), (colh_ref[...], coll_ref[...]), ((1,), (0,)))
            for f in range(2):
                gain = kern[f, g * part : (g + 1) * part, rank, :].reshape(part * span, INNER)
                shaped = spectrum * jnp.concatenate([gain, gain], axis=1)
                result = three_pass(split_value(shaped), (backh_ref[...], backl_ref[...]), ((1,), (0,)))
                for i in range(part):
                    k = g * part + i
                    re, im = result[i * span : (i + 1) * span, :INNER], result[i * span : (i + 1) * span, INNER:]
                    cs, sn = twist_ref[2, k : k + 1, :], twist_ref[3, k : k + 1, :]
                    back[f, k, :, :INNER] = re * cs + im * sn
                    back[f, k, :, INNER:] = im * cs - re * sn
        for f in range(2):
            for t in range(span // 8):
                at, past = slice(t * 8, t * 8 + 8), slice(span + t * 8, span + t * 8 + 8)
                x = fft_list([(back[f, k, at, :INNER], back[f, k, at, INNER:]) for k in range(OUTER)], 1)
                for n in range(OUTER):
                    leaving[n, c, f, at, :] = x[n][0]
                    leaving[n, c, f, past, :] = x[n][1]

    def send_home(c, masks, slot):
        for m in masks:
            peer = flipped(m)
            remote(
                leaving.at[peer, c], landed.at[slot[0], slot[1]], rsend.at[c], rrecv.at[c], {"pix": peer}
            ).start()
        landed[slot[0], slot[1]] = leaving[me, c]

    def shared_columns(c, _):
        go_all(c).wait_recv()
        columns(c)
        send_home(c, range(1, flip), ((me + (c - both) * flip) % groups, both))
        return 0

    lax.fori_loop(both, chunks + 1, shared_columns, 0)

    def single_columns(c, _):
        go_all(c).wait_recv()
        columns(c)
        send_home(c, range(1, groups), (me, c))
        return 0

    lax.fori_loop(0, both, single_columns, 0)
    lax.fori_loop(0, tile_rows, show, 0)
    for c in range(chunks + 1):
        go_all(c).wait_send()
    told.wait_send()
    for p in range(planes):
        onward(p, 0).wait_send()

        def settle(m, _):
            direct(p, m).wait_send()
            onward(p, m).wait_send()
            return 0

        lax.fori_loop(1, groups, settle, 0)

    def gather(c, first):
        def block(b, _):
            at = pl.ds(pl.multiple_of(c * 2 * span, 2 * span), 2 * span)
            high, low = high_ref[b, at, :], low_ref[b, at, :]
            table = jnp.concatenate([high, high, low], axis=0)
            for f in range(2):
                value = jnp.concatenate([landed[2 * b + p, c, f] for p in range(2)], axis=1)
                top, rest = split_value(value)
                result = lax.dot_general(
                    jnp.concatenate([top, rest, top], axis=0),
                    table,
                    (((0,), (0,)), ((), ())),
                    preferred_element_type=jnp.float32,
                ).reshape(2, slab, 2 * INNER)
                total_rows[f, b] = result if first else total_rows[f, b] + result
            return 0

        lax.fori_loop(0, HALF_BLOCKS, block, 0)

    home_all(both).wait_recv()
    home_all(chunks).wait_recv()
    gather(both, True)

    def more(c, _):
        home_any(c).wait_recv()
        gather(c, False)
        return 0

    lax.fori_loop(0, both, more, 0)
    for f, out_ref in enumerate((one_ref, two_ref)):

        def radix(t, _):
            rows = pl.ds(pl.multiple_of(t * 8, 8), 8)
            at = lambda k, p, part: total_rows[f, k, p, rows, part * INNER : (part + 1) * INNER]
            z = [None] * OUTER
            last = HALF_BLOCKS - 1
            z[0] = (at(last, 0, 0), at(last, 1, 0))
            z[HALF_BLOCKS] = (at(last, 0, 1), at(last, 1, 1))
            for k in range(1, HALF_BLOCKS):
                ar, ai = at(k - 1, 0, 0), at(k - 1, 0, 1)
                br, bi = at(k - 1, 1, 0), at(k - 1, 1, 1)
                z[k] = (ar - bi, ai + br)
                z[OUTER - k] = (ar + bi, br - ai)
            x = fft_list(z, 1)
            for n in range(OUTER):
                for p in range(2):
                    out_ref[p, rows, n * INNER : (n + 1) * INNER] = x[n][p]
            return 0

        lax.fori_loop(0, slab // 8, radix, 0)
    for c in range(chunks + 1):
        home_all(c).wait_send()


def place_kernel(*refs):
    count = (len(refs) - 1) // 2
    for copy in fetch(zip(refs[:count], refs[count:-1]), refs[-1]):
        copy.wait()


def column_info(me):
    line = lax.broadcasted_iota(jnp.int32, (INNER, INNER), 0)
    b = me // 2
    last = b == HALF_BLOCKS - 1
    upper = line // (INNER // 2)
    folded = OUTER * (line - upper * (INNER // 2)) + HALF_BLOCKS * upper
    mine = jnp.where(last, folded, b + 1 + OUTER * line)
    weight = jnp.where(last & (mine > 0), 2.0, 1.0) / (L * L)
    return jnp.where(mine >= L // 2, mine - L, mine).astype(jnp.float32), weight


def call(body, outs, scratch=(), smem=(0,), count=1, megabytes=48, flops=0, group=None, hbm=(), out_space=pltpu.VMEM):
    space = [
        pl.BlockSpec(
            memory_space=pltpu.SMEM if i in smem else pltpu.HBM if i in hbm else pltpu.VMEM
        )
        for i in range(count)
    ]
    return pl.pallas_call(
        body,
        out_shape=outs,
        in_specs=space,
        out_specs=jax.tree.map(lambda _: pl.BlockSpec(memory_space=out_space), outs),
        scratch_shapes=list(scratch),
        compiler_params=pltpu.CompilerParams(
            vmem_limit_bytes=megabytes << 20,
            collective_id=group,
            has_side_effects=group is not None,
        ),
        cost_estimate=pl.CostEstimate(flops=flops, bytes_accessed=4 << 20, transcendentals=0),
    )


def shape(*dims):
    return jax.ShapeDtypeStruct(dims, jnp.float32)


def local_fast(block_tile, cell_index, masses, plane_coef, plane_dist, source_inv):
    groups = lax.axis_size("pix")
    planes, local_tiles, per_tile = cell_index.shape
    slab = L // groups
    cap = max(1, 2 * local_tiles // groups)
    size = 2 * per_tile // TC
    message = (cap + 1) * size
    vmem = lambda *dims: pltpu.VMEM(dims, jnp.float32)
    dma = lambda *dims: pltpu.SemaphoreType.DMA(dims)
    outgoing = call(
        pack_kernel,
        [shape(groups, message, TC)] * planes,
        [
            pltpu.SMEM(block_tile.shape, jnp.int32),
            pltpu.VMEM(cell_index.shape, jnp.int32),
            pltpu.VMEM(masses.shape, jnp.bfloat16),
            vmem(size, local_tiles, TC),
            pltpu.SMEM((groups,), jnp.int32),
            dma(3),
        ],
        smem=(),
        hbm=(0, 1, 2),
        count=3,
        megabytes=16,
        flops=1 << 32,
    )(block_tile, cell_index, masses)

    order = row_order(slab)
    row_high, row_low = row_tables(CHUNKS)
    col_high, col_low = split_table(column_table(order).T)
    back_high, back_low = split_table(column_table(np.arange(INNER)))
    span = INNER // CHUNKS
    pitch = 3 * TR // 2
    tables = [jnp.asarray(twiddle_tables(order)), row_high, row_low, col_high, col_low, back_high, back_low]
    results = call(
        lensing_kernel,
        [shape(planes, slab, L)] * 3,
        [pltpu.SMEM(source_inv.shape, jnp.float32)] * 3
        + [pltpu.VMEM(table.shape, table.dtype) for table in tables]
        + [
            dma(3 + len(tables)),
            vmem(8, TC),
            vmem(8, TC),
            dma(2),
            vmem(2 * planes, groups, message, TC),
            vmem(2 * planes, cap * groups * pitch, TC),
            pltpu.VMEM((2 * planes, TC, TC), jnp.bfloat16),
            vmem(planes, TR * TC, TC),
            vmem(HALF_BLOCKS, planes, slab, 2 * INNER),
            vmem(groups, CHUNKS, 2 * span, slab),
            vmem(groups, CHUNKS + 1, 2 * span, slab),
            vmem(OUTER * span, 2 * INNER),
            vmem(2, OUTER, INNER + span, INNER),
            vmem(2, OUTER, span, 2 * INNER),
            vmem(groups, CHUNKS + 1, 2, 2 * span, slab),
            vmem(groups, CHUNKS, 2, 2 * span, slab),
            vmem(2, HALF_BLOCKS, planes, slab, 2 * INNER),
            dma(planes, groups),
            dma(planes, groups),
            dma(planes, groups),
            dma(planes, groups),
            dma(CHUNKS + 1),
            dma(CHUNKS + 1),
            dma(CHUNKS + 1),
            dma(CHUNKS + 1),
        ],
        smem=(),
        hbm=tuple(range(2, 12)),
        count=12,
        megabytes=40,
        flops=1 << 32,
        group=0,
    )(*outgoing, plane_coef, plane_dist, source_inv, *tables)
    return call(
        place_kernel,
        [shape(planes, slab, L)] * 3,
        [dma(3)],
        smem=(),
        out_space=pltpu.HBM,
        count=3,
        megabytes=16,
        flops=1 << 20,
    )(*results)


def solution(mesh):
    placed = (
        P("shell", None),
        P("shell", "pix", None),
        P("shell", "pix", None),
        P("shell"),
        P("shell"),
        P("shell"),
    )
    shells, groups = mesh.shape["shell"], mesh.shape["pix"]

    def body(block_tile, cell_index, *rest):
        fits = (
            shells == 2
            and cell_index.shape[0] == 2
            and groups == OUTER
            and cell_index.shape[2] == 4 * TC
            and cell_index.shape[1] * 2 == groups * 8
        )
        return (local_fast if fits else local)(block_tile, cell_index, *rest)

    return jax.shard_map(
        body,
        mesh=mesh,
        in_specs=placed,
        out_specs=(P("shell", "pix", None), P("shell", "pix", None), P("shell", "pix", None)),
        check_vma=False,
    )
```

```python
from functools import partial
import math

import jax
import jax.numpy as jnp
from jax import lax
from jax.experimental import pallas as pl
from jax.experimental.pallas import tpu as pltpu
from jax.sharding import PartitionSpec as P
import numpy as np

L = 2048
TR = 16
TC = 128


HIGHEST = lax.Precision.HIGHEST


def entering(value, axis, join, neutral):
    count, mine = (lax.axis_size(axis), lax.axis_index(axis))
    pieces = jax.tree.map(lambda part: lax.all_gather(part, axis), value)
    running = jax.tree.map(
        lambda part, zero: jnp.full_like(part, 0) + jnp.asarray(zero, part.dtype), value, neutral
    )

    def lap(position, running):
        longer = join(running, jax.tree.map(lambda part: part[position], pieces))
        return jax.tree.map(lambda new, old: jnp.where(position < mine, new, old), longer, running)

    return lax.fori_loop(0, count - 1, lap, running)


def dft_table(left_size, right_size, period, sign_value):
    left_idx = jnp.arange(left_size)[:, None]
    right_idx = jnp.arange(right_size)[None, :]
    angle = 2.0 * math.pi / period * (left_idx * right_idx % period).astype(jnp.float32)
    return (jnp.cos(angle), sign_value * jnp.sin(angle))


def mix_outer(table, real_part, imag_part):
    cosine, sine_part = table
    contract = partial(jnp.einsum, "ab,...bc->...ac", precision=HIGHEST)
    return (
        contract(cosine, real_part) - contract(sine_part, imag_part),
        contract(sine_part, real_part) + contract(cosine, imag_part),
    )


def mix_inner(table, real_part, imag_part):
    cosine, sine_part = table
    product = partial(jnp.matmul, precision=HIGHEST)
    return (
        product(real_part, cosine) - product(imag_part, sine_part),
        product(real_part, sine_part) + product(imag_part, cosine),
    )


def twist(table, real_part, imag_part):
    cosine, sine_part = table
    return (real_part * cosine - imag_part * sine_part, real_part * sine_part + imag_part * cosine)


def transform_last(real_part, imag_part, sign_value):
    length = real_part.shape[-1]
    inner = math.gcd(length, 128)
    outer = length // inner
    leading = real_part.shape[:-1]
    real_part = real_part.reshape(leading + (outer, inner))
    imag_part = imag_part.reshape(leading + (outer, inner))
    outer_table = dft_table(outer, outer, outer, sign_value)
    inner_table = dft_table(inner, inner, inner, sign_value)
    twiddle = dft_table(outer, inner, length, sign_value)
    if sign_value < 0:
        real_part, imag_part = mix_outer(outer_table, real_part, imag_part)
        real_part, imag_part = twist(twiddle, real_part, imag_part)
        real_part, imag_part = mix_inner(inner_table, real_part, imag_part)
    else:
        real_part, imag_part = mix_inner(inner_table, real_part, imag_part)
        real_part, imag_part = twist(twiddle, real_part, imag_part)
        real_part, imag_part = mix_outer(outer_table, real_part, imag_part)
    return (real_part.reshape(leading + (length,)), imag_part.reshape(leading + (length,)))


def frequency_of(position, length):
    inner = math.gcd(length, 128)
    outer = length // inner
    frequency = position // inner + outer * (position % inner)
    signed = jnp.where(frequency >= length // 2, frequency - length, frequency).astype(jnp.float32)
    keep_mask = (frequency != length // 2).astype(jnp.float32)
    return (signed, keep_mask)


def add_pairs(earlier_pair, later_pair):
    return (earlier_pair[0] + later_pair[0], earlier_pair[1] + later_pair[1])


def deposit_group(item):
    cell_ids, weights = item
    tile_rows = cell_ids // TC
    tile_cols = cell_ids % TC
    row_hot = jnp.where(
        tile_rows[:, None, :] == jnp.arange(TR)[None, :, None],
        weights[:, None, :],
        jnp.zeros((), jnp.bfloat16),
    )
    col_hot = (tile_cols[:, :, None] == jnp.arange(TC)[None, None, :]).astype(jnp.bfloat16)
    return jnp.einsum("grk,gkc->grc", row_hot, col_hot, preferred_element_type=jnp.float32)


def rows_to_sending(packed, groups, slab, cols_own):
    count, fields = (packed.shape[0], packed.shape[1])
    return (
        packed.reshape(count, fields, slab, groups, cols_own)
        .transpose(3, 0, 1, 4, 2)
        .reshape(groups, count, fields, cols_own * slab)
    )


def arrived_to_columns(arrived, groups, slab, cols_own):
    count, fields = (arrived.shape[1], arrived.shape[2])
    return (
        arrived.reshape(groups, count, fields, cols_own, slab)
        .transpose(1, 2, 3, 0, 4)
        .reshape(count, fields, cols_own, groups * slab)
    )


def columns_to_sending(stacked, groups, slab, cols_own):
    count, fields = (stacked.shape[0], stacked.shape[1])
    return (
        stacked.reshape(count, fields, cols_own, groups, slab)
        .transpose(3, 0, 1, 2, 4)
        .reshape(groups, count, fields, cols_own * slab)
    )


def landed_to_rows(landed, groups, slab, cols_own):
    count, fields = (landed.shape[1], landed.shape[2])
    return (
        landed.reshape(groups, count, fields, cols_own, slab)
        .transpose(1, 2, 4, 0, 3)
        .reshape(count, fields, slab, groups * cols_own)
    )


def local(block_tile, cell_index, masses, plane_coef, plane_dist, source_inv):
    groups = lax.axis_size("pix")
    my_index = lax.axis_index("pix")
    planes, local_tiles, per_tile = cell_index.shape
    slab = L // groups
    per_owner = slab // TR * (L // TC)
    cap = max(1, 2 * local_tiles // groups)
    flat = TR * TC
    batch_tiles = 8
    deposited = lax.map(
        deposit_group,
        (cell_index.reshape(-1, batch_tiles, per_tile), masses.reshape(-1, batch_tiles, per_tile)),
    )
    tile_sums = deposited.reshape(planes, local_tiles, flat)
    table = block_tile.reshape(planes, groups, local_tiles)
    owner = table // per_owner
    earlier = jnp.arange(local_tiles)[:, None] < jnp.arange(local_tiles)[None, :]
    same_owner = owner[:, :, :, None] == owner[:, :, None, :]
    rank = jnp.sum(jnp.where(same_owner & earlier[None, None], 1, 0), axis=2)
    slot = owner * cap + rank
    my_slots = lax.dynamic_index_in_dim(slot, my_index, axis=1, keepdims=False)
    slot_grid = jnp.arange(groups)[:, None] * cap + jnp.arange(cap)[None, :]
    send_hot = (my_slots[:, None, None, :] == slot_grid[None, :, :, None]).astype(jnp.float32)
    outgoing = jnp.einsum("pnct,ptf->npcf", send_hot, tile_sums, precision=HIGHEST)
    incoming = lax.all_to_all(outgoing, "pix", split_axis=0, concat_axis=0, tiled=True)
    local_index = table - my_index * per_owner
    is_mine = owner == my_index
    tile_hot = (is_mine[..., None] & (local_index[..., None] == jnp.arange(per_owner))).astype(
        jnp.float32
    )
    slot_hot = (rank[..., None] == jnp.arange(cap)).astype(jnp.float32)
    placing = jnp.einsum("pstl,pstc->plsc", tile_hot, slot_hot, precision=HIGHEST)
    slab_tiles = jnp.einsum("plsc,spcf->plf", placing, incoming, precision=HIGHEST)
    density = (
        slab_tiles.reshape(planes, slab // TR, L // TC, TR, TC)
        .transpose(0, 1, 3, 2, 4)
        .reshape(planes, slab, L)
    )
    total = lax.psum(jnp.sum(density, axis=(1, 2)), "pix")
    contrast = density / (total / (L * L))[:, None, None] - 1.0
    near_local = jnp.cumsum(plane_coef[:, None, None] * contrast, axis=0)
    far_local = jnp.cumsum((plane_coef * plane_dist)[:, None, None] * contrast, axis=0)
    blank = jnp.zeros((slab, L), jnp.float32)
    near_before, far_before = entering(
        (near_local[-1], far_local[-1]), "shell", add_pairs, (blank, blank)
    )
    convergence = near_before + near_local - source_inv[:, None, None] * (far_before + far_local)
    cols_own = L // groups
    wave_x, keep_x = frequency_of(my_index * cols_own + jnp.arange(cols_own), L)
    wave_y, keep_y = frequency_of(jnp.arange(L), L)
    wave_x = wave_x[:, None]
    wave_y = wave_y[None, :]
    both_keep = keep_x[:, None] * keep_y[None, :]
    wave_power = jnp.maximum(wave_x * wave_x + wave_y * wave_y, 1.0)
    kernel_one = both_keep * (wave_x * wave_x - wave_y * wave_y) / wave_power
    kernel_two = both_keep * 2.0 * wave_x * wave_y / wave_power
    scale = 1.0 / (L * L)
    spec_real, spec_imag = transform_last(convergence[0::2], convergence[1::2], -1.0)
    sending = rows_to_sending(jnp.stack([spec_real, spec_imag], axis=1), groups, slab, cols_own)
    arrived = lax.all_to_all(sending, "pix", split_axis=0, concat_axis=0, tiled=True)
    columns = arrived_to_columns(arrived, groups, slab, cols_own)
    row_real, row_imag = transform_last(columns[:, 0], columns[:, 1], -1.0)
    first_real, first_imag = transform_last(row_real * kernel_one, row_imag * kernel_one, 1.0)
    second_real, second_imag = transform_last(row_real * kernel_two, row_imag * kernel_two, 1.0)
    stacked = jnp.stack([first_real, first_imag, second_real, second_imag], axis=1)
    landed = lax.all_to_all(
        columns_to_sending(stacked, groups, slab, cols_own),
        "pix",
        split_axis=0,
        concat_axis=0,
        tiled=True,
    )
    row_layout = landed_to_rows(landed, groups, slab, cols_own)
    even_one, odd_one = transform_last(row_layout[:, 0], row_layout[:, 1], 1.0)
    even_two, odd_two = transform_last(row_layout[:, 2], row_layout[:, 3], 1.0)
    shear_one = jnp.stack([even_one, odd_one], axis=1).reshape(planes, slab, L)
    shear_two = jnp.stack([even_two, odd_two], axis=1).reshape(planes, slab, L)
    return (convergence, shear_one * scale, shear_two * scale)


INNER = 128
OUTER = L // INNER
HALF_BLOCKS = OUTER // 2
CHUNKS = 4
SHARED = 3
MESH = pl.DeviceIdType.MESH


def block_columns():
    cols = np.zeros((HALF_BLOCKS, INNER), np.int64)
    for b in range(HALF_BLOCKS - 1):
        cols[b] = b + 1 + OUTER * np.arange(INNER)
    half = np.arange(INNER // 2)
    cols[-1] = np.concatenate([OUTER * half, HALF_BLOCKS + OUTER * half])
    return cols


def split_table(table):
    high = table.astype(jnp.bfloat16)
    low = (table - high.astype(np.float64)).astype(jnp.bfloat16)
    return high, low


def row_tables(chunks):
    n2 = np.arange(INNER)
    out = np.zeros((HALF_BLOCKS, 2 * INNER, 2 * INNER))
    cols = block_columns()
    for b in range(HALF_BLOCKS):
        angle = 2 * np.pi / L * ((n2[:, None] * cols[b][None, :]) % L)
        co, si = np.cos(angle), np.sin(angle)
        if b < HALF_BLOCKS - 1:
            out[b] = np.block([[co, -si], [si, co]])
        else:
            h = INNER // 2
            out[b, :INNER, :h] = co[:, :h]
            out[b, :INNER, INNER : INNER + h] = -si[:, :h]
            out[b, INNER:, h:INNER] = co[:, h:]
            out[b, INNER:, INNER + h :] = -si[:, h:]
    out = out.reshape(HALF_BLOCKS, 2 * INNER, 2, chunks, INNER // chunks)
    return split_table(out.transpose(0, 3, 2, 4, 1).reshape(HALF_BLOCKS, 2 * INNER, 2 * INNER))


def row_order(slab):
    at = np.arange(slab)
    rows = slab // TR
    return (at % rows) * TR + at // rows


def column_table(order):
    idx = np.arange(INNER)
    angle = 2 * np.pi / INNER * ((idx[:, None] * order[None, :]) % INNER)
    co, si = np.cos(angle), np.sin(angle)
    return np.block([[co, si], [-si, co]])


def twiddle_tables(order):
    out = []
    for rows in (order, np.arange(INNER)):
        angle = 2 * np.pi / L * (np.arange(OUTER)[:, None] * rows[None, :])
        out += [np.cos(angle), -np.sin(angle)]
    return np.stack(out).astype(np.float32)


def times_root(value, k, n, sign):
    re, im = value
    k = k % n
    if k == 0:
        return value
    if 4 * k == n:
        return (-im, re) if sign > 0 else (im, -re)
    angle = 2 * math.pi * k / n
    c, s = math.cos(angle), sign * math.sin(angle)
    if 8 * k == n or 8 * k == 3 * n:
        if c > 0:
            return ((re - im) * c, (re + im) * c) if sign > 0 else ((re + im) * c, (im - re) * c)
        c = -c
        return ((re + im) * -c, (re - im) * c) if sign > 0 else ((im - re) * c, (re + im) * -c)
    return (re * c - im * s, re * s + im * c)


def fft_list(values, sign):
    n = len(values)
    if n == 1:
        return values
    even = fft_list(values[0::2], sign)
    odd = fft_list(values[1::2], sign)
    odd = [times_root(v, k, n, sign) for k, v in enumerate(odd)]
    return [(a[0] + b[0], a[1] + b[1]) for a, b in zip(even, odd)] + [
        (a[0] - b[0], a[1] - b[1]) for a, b in zip(even, odd)
    ]


def split_value(value):
    high = value.astype(jnp.bfloat16)
    return high, (value - high.astype(jnp.float32)).astype(jnp.bfloat16)


def three_pass(left, right, dims):
    dot = lambda a, b: lax.dot_general(a, b, (dims, ((), ())), preferred_element_type=jnp.float32)
    return dot(left[0], right[0]) + (dot(left[0], right[1]) + dot(left[1], right[0]))


def partners(me):
    steps = [(bit, bit - 2 * bit * ((me // bit) % 2)) for bit in (1, 2, 4, 8)]

    def flipped(mask):
        peer = me
        for bit, step in steps:
            if not isinstance(mask, int):
                peer = peer + ((mask // bit) % 2) * step
            elif mask & bit:
                peer = peer + step
        return peer

    return flipped


def fetch(pairs, sems):
    copies = [pltpu.make_async_copy(a, b, sems.at[i]) for i, (a, b) in enumerate(pairs)]
    for copy in copies:
        copy.start()
    return copies


def pack_kernel(tile_in, cell_in, mass_in, *refs):
    planes, tiles, per_tile = cell_in.shape
    out_refs = refs[:planes]
    tile_ref, cell_ref, mass_ref, wide, taken, sems = refs[planes:]
    copies = fetch(((tile_in, tile_ref), (cell_in, cell_ref), (mass_in, mass_ref)), sems)
    half = per_tile // TC
    size = 2 * half
    groups, rows, _ = out_refs[0].shape
    cap = rows // size - 1
    per_owner = L // groups // TR * (L // TC)
    me = lax.axis_index("pix")
    lane = lax.broadcasted_iota(jnp.int32, (1, TC), 1)
    for out_ref in out_refs:
        out_ref[...] = jnp.zeros_like(out_ref)
    for copy in copies:
        copy.wait()
    for p in range(planes):
        out_ref = out_refs[p]
        for i in range(half):
            at = slice(i * TC, (i + 1) * TC)
            wide[i] = cell_ref[p, :, at].astype(jnp.float32)
            wide[half + i] = mass_ref[p, :, at].astype(jnp.float32)
        total = jnp.sum(jnp.sum(wide[half:], axis=0), axis=0, keepdims=True)
        total = jnp.sum(total, axis=1, keepdims=True)
        tail = jnp.where(lane < cap, -1.0, jnp.where(lane == cap, total, 0.0))
        out_ref[:, cap * size :, :] = jnp.broadcast_to(tail[None], (groups, size, TC))

        def clear(o, _):
            taken[o] = 0
            return 0

        lax.fori_loop(0, groups, clear, 0)

        def tile(t, _):
            b = tile_ref[p, me * tiles + t]
            owner = b // per_owner
            rank = taken[owner]
            taken[owner] = rank + 1
            for i in range(size):
                out_ref[owner, pl.ds(rank * size + i, 1), :] = wide[i, pl.ds(t, 1), :]
            where_at = (b - owner * per_owner).astype(jnp.float32)
            old = out_ref[owner, cap * size : cap * size + 1, :]
            out_ref[owner, cap * size : cap * size + 1, :] = jnp.where(lane == rank, where_at, old)
            return 0

        lax.fori_loop(0, tiles, tile, 0, unroll=4)


def signal_all(peers):
    barrier = pltpu.get_barrier_semaphore()
    for peer in peers:
        pl.semaphore_signal(barrier, inc=1, device_id=peer, device_id_type=MESH)
    pl.semaphore_wait(barrier, len(peers))


def remote(source, target, send, recv, peer):
    return pltpu.make_async_remote_copy(
        src_ref=source,
        dst_ref=target,
        send_sem=send,
        recv_sem=recv,
        device_id=peer,
        device_id_type=MESH,
    )


def lensing_kernel(
    out0, out1, coef_in, dist_in, inv_in, twist_ref, high_ref, low_ref, colh_ref, coll_ref, backh_ref, backl_ref,
    conv_ref, one_ref, two_ref,
    coef_ref, dist_ref, inv_ref, tsem, note, far_note, note_sems,
    box, slots, place, field, held_row, sending, arrived, held, kern, back, leaving, landed, total_rows,
    lsend, lrecv, psend, precv, fsend, frecv, rsend, rrecv,
):
    out_refs = (out0, out1)
    planes = 2
    groups, message, _ = out0.shape
    slab = L // groups
    half = 4
    size = 2 * half
    cap = message // size - 1
    chunks = sending.shape[1]
    span = INNER // chunks
    single = chunks - SHARED
    units = chunks + SHARED
    flip = groups // 2
    pitch = slots.shape[1] // (cap * groups)
    tile_rows = slab // TR
    me, shell = lax.axis_index("pix"), lax.axis_index("shell")
    flipped = partners(me)
    factors = fetch(((coef_in, coef_ref), (dist_in, dist_ref), (inv_in, inv_ref)), tsem)
    for copy in factors:
        copy.wait()
    note[...] = jnp.zeros_like(note)
    for p in range(planes):
        note[p : p + 1, :] = jnp.full((1, TC), coef_ref[p], jnp.float32)
        note[planes + p : planes + p + 1, :] = jnp.full((1, TC), dist_ref[p], jnp.float32)
    signal_all([{"pix": flipped(m)} for m in range(1, groups)] + [{"shell": 1 - shell}])

    sent = pl.ds(0, cap * size + 1)

    def direct(p, m):
        peer = flipped(m)
        return remote(
            out_refs[p].at[peer, sent], box.at[p, me, sent], lsend.at[p, m], lrecv.at[p, m], {"pix": peer}
        )

    def landing(p, m):
        peer = flipped(m)
        return remote(
            out_refs[p].at[peer, sent], box.at[p, peer, sent], lsend.at[p, m], lrecv.at[p, m], {"pix": peer}
        )

    def onward(p, m):
        source = flipped(m)
        first = out_refs[p].at[me, sent] if isinstance(m, int) and m == 0 else box.at[p, source, sent]
        return remote(first, box.at[planes + p, source, sent], psend.at[p, m], precv.at[p, m], {"shell": 1 - shell})

    for m in range(1, groups):
        for p in range(planes):
            direct(p, m).start()
    told = remote(note, far_note, note_sems.at[0], note_sems.at[1], {"shell": 1 - shell})
    told.start()
    for p in range(planes):
        onward(p, 0).start()
        box[p, me] = out_refs[p][me]

    own_lines, mirror_lines = column_info(me), column_info((me + flip) % groups)
    signed_v, weight = (
        jnp.concatenate([ours, theirs[single * span :]], axis=0)
        for ours, theirs in zip(own_lines, mirror_lines)
    )
    inner_id = lax.broadcasted_iota(jnp.int32, (units * span, INNER), 1)

    def prepare(k, _):
        u = k + OUTER * inner_id
        signed_u = jnp.where(u >= L // 2, u - L, u).astype(jnp.float32)
        scale = jnp.where(u == L // 2, 0.0, weight)
        uu, vv = signed_u * signed_u, signed_v * signed_v
        over = scale / jnp.maximum(uu + vv, 1.0)
        kern[0, k] = (vv - uu) * over
        kern[1, k] = 2.0 * signed_v * signed_u * over
        return 0

    as_small = lambda ids: ids.astype(jnp.float32).astype(jnp.bfloat16)
    short, narrow = 2 * TR, TC // 2
    row_id = as_small(lax.broadcasted_iota(jnp.int32, (short, TC), 0))
    col_id = as_small(lax.broadcasted_iota(jnp.int32, (narrow, TC), 0))
    one, zero = jnp.ones((), jnp.bfloat16), jnp.zeros((), jnp.bfloat16)

    def deposit(q, s):
        for c in range(cap):
            entry = box[q, s, c * size : (c + 1) * size, :]
            cells = entry[:half].astype(jnp.int32)
            cell_rows = as_small(cells // TC + TR * ((cells // narrow) % 2))
            cell_cols = as_small(cells % narrow)
            weights = entry[half:].astype(jnp.bfloat16)
            row_hot, col_hot = [], []
            for i in range(half):
                row_hot.append(jnp.where(row_id == cell_rows[i : i + 1], weights[i : i + 1], zero))
                col_hot.append(jnp.where(col_id == cell_cols[i : i + 1], one, zero))
            sums = lax.dot_general(
                jnp.concatenate(row_hot, axis=1),
                jnp.concatenate(col_hot, axis=1),
                (((1,), (1,)), ((), ())),
                preferred_element_type=jnp.float32,
            )
            at = pl.ds(pl.multiple_of((c * groups + s) * pitch, 8), TR)
            slots[q, at, :] = jnp.concatenate([sums[:TR], sums[TR:]], axis=1)

    def near_block(m):
        def one_plane(p, _):
            deposit(p, flipped(m))
            return 0

        lax.fori_loop(0, planes, one_plane, 0)

    def far_block(m):
        for p in range(planes):
            onward(p, m).wait_recv()

        def one_plane(p, _):
            deposit(planes + p, flipped(m))
            return 0

        lax.fori_loop(0, planes, one_plane, 0)

    def take(m):
        for p in range(planes):
            landing(p, m).wait_recv()
            onward(p, m).start()

    lag = 2
    near_block(0)

    def early(m, _):
        take(m)
        near_block(m)
        return 0

    lax.fori_loop(1, lag, early, 0)

    def steady(m, _):
        take(m)
        near_block(m)
        far_block(m - lag)
        return 0

    lax.fori_loop(lag, groups, steady, 0)

    def late(m, _):
        far_block(m)
        return 0

    lax.fori_loop(groups - lag, groups, late, 0)

    told.wait_recv()
    lane_id = lax.broadcasted_iota(jnp.int32, (groups, TC), 1)
    tile_id = ((lane_id % tile_rows) * OUTER + lane_id // tile_rows).astype(jnp.float32)
    gains, shifts = [[], []], [0.0, 0.0]
    for q in range(2 * planes):
        tails = box[q, :, cap * size, :]
        hot = [jnp.where(tails[:, c : c + 1] == tile_id, 1.0, 0.0) for c in range(cap)]
        place[q] = jnp.concatenate(hot, axis=0).T.astype(jnp.bfloat16)
        total = jnp.sum(tails[:, cap : cap + 1], axis=0, keepdims=True)
        notes, p = (note, q) if q < planes else (far_note, q - planes)
        coef, dist = notes[p : p + 1, 0:1], notes[planes + p : planes + p + 1, 0:1]
        for i in range(planes):
            mixed = coef * (1.0 - inv_ref[i] * dist)
            if q >= planes:
                mixed = jnp.where(shell > 0, mixed, 0.0)
            elif q > i:
                mixed = jnp.zeros_like(mixed)
            gains[i].append(mixed * ((L * L) / total))
            shifts[i] = shifts[i] + mixed

    peers = groups - 1

    def go(c, peer):
        source = sending.at[peer, c] if c < chunks else sending.at[(peer + flip) % groups, c - SHARED]
        return remote(source, arrived.at[me, c], fsend.at[c], frecv.at[c], {"pix": peer})

    def go_all(c):
        every = pl.ds(0, peers)
        return remote(
            sending.at[every, 0], arrived.at[every, c], fsend.at[c], frecv.at[c], {"pix": flipped(1)}
        )

    def home_any(c, count=peers):
        every = pl.ds(0, count)
        return remote(
            leaving.at[every, c], landed.at[every, 0], rsend.at[c], rrecv.at[c], {"pix": flipped(1)}
        )

    def home_all(c):
        return home_any(c, peers if c < single else flip - 1)

    def field_rows(r, n):
        return pl.ds(pl.multiple_of(r * TC + n * tile_rows, tile_rows), tile_rows)

    def mass_rows(j, _):
        r = 2 * j
        sums = []
        for q in range(2 * planes):
            pair = jnp.concatenate(
                [slots[q, pl.ds(r + i, cap * groups, stride=pitch), :] for i in range(2)], axis=1
            )
            high = pair.astype(jnp.bfloat16)
            rest = pair - high.astype(jnp.float32)
            middle = rest.astype(jnp.bfloat16)
            low = (rest - middle.astype(jnp.float32)).astype(jnp.bfloat16)
            dot = lambda part: jnp.dot(place[q], part, preferred_element_type=jnp.float32)
            sums.append(dot(high) + (dot(middle) + dot(low)))
        for i in range(planes):
            value = gains[i][0] * sums[0]
            for q in range(1, 2 * planes):
                value = value + gains[i][q] * sums[q]
            value = value - shifts[i]
            for e in range(2):
                at = pl.ds(pl.multiple_of((r + e) * TC, TC), TC)
                field[i, at, :] = value[:, e * TC : (e + 1) * TC]
        return 0

    lax.fori_loop(0, TR // 2, mass_rows, 0)

    def row_radix(r, _):
        near = pl.ds(pl.multiple_of(r * tile_rows, tile_rows), tile_rows)
        z = fft_list(
            [tuple(field[i, field_rows(r, n), :] for i in range(2)) for n in range(OUTER)], -1
        )
        for k in range(1, HALF_BLOCKS):
            (ar, ai), (br, bi) = z[k], z[OUTER - k]
            held_row[k - 1, 0, near, :INNER] = 0.5 * (ar + br)
            held_row[k - 1, 0, near, INNER:] = 0.5 * (ai - bi)
            held_row[k - 1, 1, near, :INNER] = 0.5 * (ai + bi)
            held_row[k - 1, 1, near, INNER:] = 0.5 * (br - ar)
        for p in range(2):
            held_row[HALF_BLOCKS - 1, p, near, :INNER] = z[0][p]
            held_row[HALF_BLOCKS - 1, p, near, INNER:] = z[HALF_BLOCKS][p]
        return 0

    lax.fori_loop(0, TR, row_radix, 0)

    def row_block(b):
        value = held_row[b].reshape(2 * slab, 2 * INNER)
        result = three_pass((high_ref[b], low_ref[b]), split_value(value), ((1,), (1,)))
        for p in range(2):
            for c in range(chunks):
                sending[2 * b + p, c] = result[
                    2 * span * c : 2 * span * (c + 1), p * slab : (p + 1) * slab
                ]

    def send_block(j, _):
        b = (me // 2 + 1 + j) % HALF_BLOCKS
        row_block(b)
        for p in range(2):
            for c in (single, chunks):
                peer = 2 * b + p if c < chunks else (2 * b + p + flip) % groups
                pl.when(peer != me)(lambda: go(c, peer).start())
        return 0

    lax.fori_loop(0, HALF_BLOCKS, send_block, 0)
    later = [c + i for i in range(1, SHARED) for c in (single, chunks)]
    for c in later + list(range(single)):
        for m in range(1, groups):
            go(c, flipped(m)).start()
    for c in range(chunks):
        arrived[me, c] = sending[me, c]
    for c in range(chunks, units):
        arrived[me, c] = sending[(me + flip) % groups, c - SHARED]

    def show(t, _):
        for i in range(planes):
            for n in range(OUTER):
                for r in range(0, TR, 8):
                    rows = pl.ds(pl.multiple_of(t * TR + r, 8), 8)
                    held_at = pl.ds(r * TC + n * tile_rows + t, 8, stride=TC)
                    conv_ref[i, rows, n * TC : (n + 1) * TC] = field[i, held_at, :]
        return 0

    lax.fori_loop(0, OUTER, prepare, 0)

    def columns(c):
        for t in range(span // 8):
            at, past = slice(t * 8, t * 8 + 8), slice(span + t * 8, span + t * 8 + 8)
            z = fft_list([(arrived[n, c, at, :], arrived[n, c, past, :]) for n in range(OUTER)], -1)
            for k in range(OUTER):
                re, im = z[k]
                if k:
                    cs, sn = twist_ref[0, k : k + 1, :], twist_ref[1, k : k + 1, :]
                    re, im = re * cs - im * sn, re * sn + im * cs
                rows = slice(k * span + t * 8, k * span + t * 8 + 8)
                held[rows, :INNER] = re
                held[rows, INNER:] = im
        rank = pl.ds(pl.multiple_of(c * span, span), span)
        part = 2 * INNER // span
        for g in range(OUTER // part):
            value = held[g * part * span : (g + 1) * part * span, :]
            spectrum = three_pass(split_value(value), (colh_ref[...], coll_ref[...]), ((1,), (0,)))
            for f in range(2):
                gain = kern[f, g * part : (g + 1) * part, rank, :].reshape(part * span, INNER)
                shaped = spectrum * jnp.concatenate([gain, gain], axis=1)
                result = three_pass(split_value(shaped), (backh_ref[...], backl_ref[...]), ((1,), (0,)))
                for i in range(part):
                    k = g * part + i
                    re, im = result[i * span : (i + 1) * span, :INNER], result[i * span : (i + 1) * span, INNER:]
                    cs, sn = twist_ref[2, k : k + 1, :], twist_ref[3, k : k + 1, :]
                    back[f, k, :, :INNER] = re * cs + im * sn
                    back[f, k, :, INNER:] = im * cs - re * sn
        for f in range(2):
            for t in range(span // 8):
                at, past = slice(t * 8, t * 8 + 8), slice(span + t * 8, span + t * 8 + 8)
                x = fft_list([(back[f, k, at, :INNER], back[f, k, at, INNER:]) for k in range(OUTER)], 1)
                for n in range(OUTER):
                    leaving[n, c, f, at, :] = x[n][0]
                    leaving[n, c, f, past, :] = x[n][1]

    def send_home(c, masks, slot):
        for m in masks:
            peer = flipped(m)
            remote(
                leaving.at[peer, c], landed.at[slot[0], slot[1]], rsend.at[c], rrecv.at[c], {"pix": peer}
            ).start()
        landed[slot[0], slot[1]] = leaving[me, c]

    def shared_columns(j, _):
        c = single + j // 2 + (j % 2) * SHARED
        go_all(c).wait_recv()
        columns(c)
        send_home(c, range(1, flip), ((me + (j % 2) * flip) % groups, single + j // 2))
        return 0

    lax.fori_loop(0, 2 * SHARED, shared_columns, 0)

    def single_columns(c, _):
        go_all(c).wait_recv()
        columns(c)
        send_home(c, range(1, groups), (me, c))
        return 0

    lax.fori_loop(0, single, single_columns, 0)
    lax.fori_loop(0, tile_rows, show, 0)
    for c in range(units):
        go_all(c).wait_send()
    told.wait_send()
    for p in range(planes):
        onward(p, 0).wait_send()

        def settle(m, _):
            direct(p, m).wait_send()
            onward(p, m).wait_send()
            return 0

        lax.fori_loop(1, groups, settle, 0)

    def gather(c, first):
        def block(b, _):
            at = pl.ds(pl.multiple_of(c * 2 * span, 2 * span), 2 * span)
            high, low = high_ref[b, at, :], low_ref[b, at, :]
            table = jnp.concatenate([high, high, low], axis=0)
            for f in range(2):
                value = jnp.concatenate([landed[2 * b + p, c, f] for p in range(2)], axis=1)
                top, rest = split_value(value)
                result = lax.dot_general(
                    jnp.concatenate([top, rest, top], axis=0),
                    table,
                    (((0,), (0,)), ((), ())),
                    preferred_element_type=jnp.float32,
                ).reshape(2, slab, 2 * INNER)
                total_rows[f, b] = result if first else total_rows[f, b] + result
            return 0

        lax.fori_loop(0, HALF_BLOCKS, block, 0)

    for c in range(single, chunks):
        home_all(c).wait_recv()
        home_all(c + SHARED).wait_recv()
        gather(c, c == single)

    def more(c, _):
        home_any(c).wait_recv()
        gather(c, False)
        return 0

    lax.fori_loop(0, single, more, 0)
    for f, out_ref in enumerate((one_ref, two_ref)):

        def radix(t, _):
            rows = pl.ds(pl.multiple_of(t * 8, 8), 8)
            at = lambda k, p, part: total_rows[f, k, p, rows, part * INNER : (part + 1) * INNER]
            z = [None] * OUTER
            last = HALF_BLOCKS - 1
            z[0] = (at(last, 0, 0), at(last, 1, 0))
            z[HALF_BLOCKS] = (at(last, 0, 1), at(last, 1, 1))
            for k in range(1, HALF_BLOCKS):
                ar, ai = at(k - 1, 0, 0), at(k - 1, 0, 1)
                br, bi = at(k - 1, 1, 0), at(k - 1, 1, 1)
                z[k] = (ar - bi, ai + br)
                z[OUTER - k] = (ar + bi, br - ai)
            x = fft_list(z, 1)
            for n in range(OUTER):
                for p in range(2):
                    out_ref[p, rows, n * INNER : (n + 1) * INNER] = x[n][p]
            return 0

        lax.fori_loop(0, slab // 8, radix, 0)
    for c in range(units):
        home_all(c).wait_send()


def place_kernel(*refs):
    count = (len(refs) - 1) // 2
    for copy in fetch(zip(refs[:count], refs[count:-1]), refs[-1]):
        copy.wait()


def column_info(me):
    line = lax.broadcasted_iota(jnp.int32, (INNER, INNER), 0)
    b = me // 2
    last = b == HALF_BLOCKS - 1
    upper = line // (INNER // 2)
    folded = OUTER * (line - upper * (INNER // 2)) + HALF_BLOCKS * upper
    mine = jnp.where(last, folded, b + 1 + OUTER * line)
    weight = jnp.where(last & (mine > 0), 2.0, 1.0) / (L * L)
    return jnp.where(mine >= L // 2, mine - L, mine).astype(jnp.float32), weight


def call(body, outs, scratch=(), smem=(0,), count=1, megabytes=48, flops=0, group=None, hbm=(), out_space=pltpu.VMEM):
    space = [
        pl.BlockSpec(
            memory_space=pltpu.SMEM if i in smem else pltpu.HBM if i in hbm else pltpu.VMEM
        )
        for i in range(count)
    ]
    return pl.pallas_call(
        body,
        out_shape=outs,
        in_specs=space,
        out_specs=jax.tree.map(lambda _: pl.BlockSpec(memory_space=out_space), outs),
        scratch_shapes=list(scratch),
        compiler_params=pltpu.CompilerParams(
            vmem_limit_bytes=megabytes << 20,
            collective_id=group,
            has_side_effects=group is not None,
        ),
        cost_estimate=pl.CostEstimate(flops=flops, bytes_accessed=4 << 20, transcendentals=0),
    )


def shape(*dims):
    return jax.ShapeDtypeStruct(dims, jnp.float32)


def local_fast(block_tile, cell_index, masses, plane_coef, plane_dist, source_inv):
    groups = lax.axis_size("pix")
    planes, local_tiles, per_tile = cell_index.shape
    slab = L // groups
    cap = max(1, 2 * local_tiles // groups)
    size = 2 * per_tile // TC
    message = (cap + 1) * size
    vmem = lambda *dims: pltpu.VMEM(dims, jnp.float32)
    dma = lambda *dims: pltpu.SemaphoreType.DMA(dims)
    outgoing = call(
        pack_kernel,
        [shape(groups, message, TC)] * planes,
        [
            pltpu.SMEM(block_tile.shape, jnp.int32),
            pltpu.VMEM(cell_index.shape, jnp.int32),
            pltpu.VMEM(masses.shape, jnp.bfloat16),
            vmem(size, local_tiles, TC),
            pltpu.SMEM((groups,), jnp.int32),
            dma(3),
        ],
        smem=(),
        hbm=(0, 1, 2),
        count=3,
        megabytes=16,
        flops=1 << 32,
    )(block_tile, cell_index, masses)

    order = row_order(slab)
    row_high, row_low = row_tables(CHUNKS)
    col_high, col_low = split_table(column_table(order).T)
    back_high, back_low = split_table(column_table(np.arange(INNER)))
    span = INNER // CHUNKS
    pitch = 3 * TR // 2
    tables = [jnp.asarray(twiddle_tables(order)), row_high, row_low, col_high, col_low, back_high, back_low]
    results = call(
        lensing_kernel,
        [shape(planes, slab, L)] * 3,
        [pltpu.SMEM(source_inv.shape, jnp.float32)] * 3
        + [
            dma(3),
            vmem(8, TC),
            vmem(8, TC),
            dma(2),
            vmem(2 * planes, groups, message, TC),
            vmem(2 * planes, cap * groups * pitch, TC),
            pltpu.VMEM((2 * planes, TC, TC), jnp.bfloat16),
            vmem(planes, TR * TC, TC),
            vmem(HALF_BLOCKS, planes, slab, 2 * INNER),
            vmem(groups, CHUNKS, 2 * span, slab),
            vmem(groups, CHUNKS + SHARED, 2 * span, slab),
            vmem(OUTER * span, 2 * INNER),
            vmem(2, OUTER, INNER + SHARED * span, INNER),
            vmem(2, OUTER, span, 2 * INNER),
            vmem(groups, CHUNKS + SHARED, 2, 2 * span, slab),
            vmem(groups, CHUNKS, 2, 2 * span, slab),
            vmem(2, HALF_BLOCKS, planes, slab, 2 * INNER),
            dma(planes, groups),
            dma(planes, groups),
            dma(planes, groups),
            dma(planes, groups),
            dma(CHUNKS + SHARED),
            dma(CHUNKS + SHARED),
            dma(CHUNKS + SHARED),
            dma(CHUNKS + SHARED),
        ],
        smem=(),
        hbm=(2, 3, 4),
        count=12,
        megabytes=40,
        flops=1 << 32,
        group=0,
    )(*outgoing, plane_coef, plane_dist, source_inv, *tables)
    return call(
        place_kernel,
        [shape(planes, slab, L)] * 3,
        [dma(3)],
        smem=(),
        out_space=pltpu.HBM,
        count=3,
        megabytes=16,
        flops=1 << 20,
    )(*results)


def solution(mesh):
    placed = (
        P("shell", None),
        P("shell", "pix", None),
        P("shell", "pix", None),
        P("shell"),
        P("shell"),
        P("shell"),
    )
    shells, groups = mesh.shape["shell"], mesh.shape["pix"]

    def body(block_tile, cell_index, *rest):
        fits = (
            shells == 2
            and cell_index.shape[0] == 2
            and groups == OUTER
            and cell_index.shape[2] == 4 * TC
            and cell_index.shape[1] * 2 == groups * 8
        )
        return (local_fast if fits else local)(block_tile, cell_index, *rest)

    return jax.shard_map(
        body,
        mesh=mesh,
        in_specs=placed,
        out_specs=(P("shell", "pix", None), P("shell", "pix", None), P("shell", "pix", None)),
        check_vma=False,
    )
```

```python
from functools import partial
import math

import jax
import jax.numpy as jnp
from jax import lax
from jax.experimental import pallas as pl
from jax.experimental.pallas import tpu as pltpu
from jax.sharding import PartitionSpec as P
import numpy as np

L = 2048
TR = 16
TC = 128


HIGHEST = lax.Precision.HIGHEST


def entering(value, axis, join, neutral):
    count, mine = (lax.axis_size(axis), lax.axis_index(axis))
    pieces = jax.tree.map(lambda part: lax.all_gather(part, axis), value)
    running = jax.tree.map(
        lambda part, zero: jnp.full_like(part, 0) + jnp.asarray(zero, part.dtype), value, neutral
    )

    def lap(position, running):
        longer = join(running, jax.tree.map(lambda part: part[position], pieces))
        return jax.tree.map(lambda new, old: jnp.where(position < mine, new, old), longer, running)

    return lax.fori_loop(0, count - 1, lap, running)


def dft_table(left_size, right_size, period, sign_value):
    left_idx = jnp.arange(left_size)[:, None]
    right_idx = jnp.arange(right_size)[None, :]
    angle = 2.0 * math.pi / period * (left_idx * right_idx % period).astype(jnp.float32)
    return (jnp.cos(angle), sign_value * jnp.sin(angle))


def mix_outer(table, real_part, imag_part):
    cosine, sine_part = table
    contract = partial(jnp.einsum, "ab,...bc->...ac", precision=HIGHEST)
    return (
        contract(cosine, real_part) - contract(sine_part, imag_part),
        contract(sine_part, real_part) + contract(cosine, imag_part),
    )


def mix_inner(table, real_part, imag_part):
    cosine, sine_part = table
    product = partial(jnp.matmul, precision=HIGHEST)
    return (
        product(real_part, cosine) - product(imag_part, sine_part),
        product(real_part, sine_part) + product(imag_part, cosine),
    )


def twist(table, real_part, imag_part):
    cosine, sine_part = table
    return (real_part * cosine - imag_part * sine_part, real_part * sine_part + imag_part * cosine)


def transform_last(real_part, imag_part, sign_value):
    length = real_part.shape[-1]
    inner = math.gcd(length, 128)
    outer = length // inner
    leading = real_part.shape[:-1]
    real_part = real_part.reshape(leading + (outer, inner))
    imag_part = imag_part.reshape(leading + (outer, inner))
    outer_table = dft_table(outer, outer, outer, sign_value)
    inner_table = dft_table(inner, inner, inner, sign_value)
    twiddle = dft_table(outer, inner, length, sign_value)
    if sign_value < 0:
        real_part, imag_part = mix_outer(outer_table, real_part, imag_part)
        real_part, imag_part = twist(twiddle, real_part, imag_part)
        real_part, imag_part = mix_inner(inner_table, real_part, imag_part)
    else:
        real_part, imag_part = mix_inner(inner_table, real_part, imag_part)
        real_part, imag_part = twist(twiddle, real_part, imag_part)
        real_part, imag_part = mix_outer(outer_table, real_part, imag_part)
    return (real_part.reshape(leading + (length,)), imag_part.reshape(leading + (length,)))


def frequency_of(position, length):
    inner = math.gcd(length, 128)
    outer = length // inner
    frequency = position // inner + outer * (position % inner)
    signed = jnp.where(frequency >= length // 2, frequency - length, frequency).astype(jnp.float32)
    keep_mask = (frequency != length // 2).astype(jnp.float32)
    return (signed, keep_mask)


def add_pairs(earlier_pair, later_pair):
    return (earlier_pair[0] + later_pair[0], earlier_pair[1] + later_pair[1])


def deposit_group(item):
    cell_ids, weights = item
    tile_rows = cell_ids // TC
    tile_cols = cell_ids % TC
    row_hot = jnp.where(
        tile_rows[:, None, :] == jnp.arange(TR)[None, :, None],
        weights[:, None, :],
        jnp.zeros((), jnp.bfloat16),
    )
    col_hot = (tile_cols[:, :, None] == jnp.arange(TC)[None, None, :]).astype(jnp.bfloat16)
    return jnp.einsum("grk,gkc->grc", row_hot, col_hot, preferred_element_type=jnp.float32)


def rows_to_sending(packed, groups, slab, cols_own):
    count, fields = (packed.shape[0], packed.shape[1])
    return (
        packed.reshape(count, fields, slab, groups, cols_own)
        .transpose(3, 0, 1, 4, 2)
        .reshape(groups, count, fields, cols_own * slab)
    )


def arrived_to_columns(arrived, groups, slab, cols_own):
    count, fields = (arrived.shape[1], arrived.shape[2])
    return (
        arrived.reshape(groups, count, fields, cols_own, slab)
        .transpose(1, 2, 3, 0, 4)
        .reshape(count, fields, cols_own, groups * slab)
    )


def columns_to_sending(stacked, groups, slab, cols_own):
    count, fields = (stacked.shape[0], stacked.shape[1])
    return (
        stacked.reshape(count, fields, cols_own, groups, slab)
        .transpose(3, 0, 1, 2, 4)
        .reshape(groups, count, fields, cols_own * slab)
    )


def landed_to_rows(landed, groups, slab, cols_own):
    count, fields = (landed.shape[1], landed.shape[2])
    return (
        landed.reshape(groups, count, fields, cols_own, slab)
        .transpose(1, 2, 4, 0, 3)
        .reshape(count, fields, slab, groups * cols_own)
    )


def local(block_tile, cell_index, masses, plane_coef, plane_dist, source_inv):
    groups = lax.axis_size("pix")
    my_index = lax.axis_index("pix")
    planes, local_tiles, per_tile = cell_index.shape
    slab = L // groups
    per_owner = slab // TR * (L // TC)
    cap = max(1, 2 * local_tiles // groups)
    flat = TR * TC
    batch_tiles = 8
    deposited = lax.map(
        deposit_group,
        (cell_index.reshape(-1, batch_tiles, per_tile), masses.reshape(-1, batch_tiles, per_tile)),
    )
    tile_sums = deposited.reshape(planes, local_tiles, flat)
    table = block_tile.reshape(planes, groups, local_tiles)
    owner = table // per_owner
    earlier = jnp.arange(local_tiles)[:, None] < jnp.arange(local_tiles)[None, :]
    same_owner = owner[:, :, :, None] == owner[:, :, None, :]
    rank = jnp.sum(jnp.where(same_owner & earlier[None, None], 1, 0), axis=2)
    slot = owner * cap + rank
    my_slots = lax.dynamic_index_in_dim(slot, my_index, axis=1, keepdims=False)
    slot_grid = jnp.arange(groups)[:, None] * cap + jnp.arange(cap)[None, :]
    send_hot = (my_slots[:, None, None, :] == slot_grid[None, :, :, None]).astype(jnp.float32)
    outgoing = jnp.einsum("pnct,ptf->npcf", send_hot, tile_sums, precision=HIGHEST)
    incoming = lax.all_to_all(outgoing, "pix", split_axis=0, concat_axis=0, tiled=True)
    local_index = table - my_index * per_owner
    is_mine = owner == my_index
    tile_hot = (is_mine[..., None] & (local_index[..., None] == jnp.arange(per_owner))).astype(
        jnp.float32
    )
    slot_hot = (rank[..., None] == jnp.arange(cap)).astype(jnp.float32)
    placing = jnp.einsum("pstl,pstc->plsc", tile_hot, slot_hot, precision=HIGHEST)
    slab_tiles = jnp.einsum("plsc,spcf->plf", placing, incoming, precision=HIGHEST)
    density = (
        slab_tiles.reshape(planes, slab // TR, L // TC, TR, TC)
        .transpose(0, 1, 3, 2, 4)
        .reshape(planes, slab, L)
    )
    total = lax.psum(jnp.sum(density, axis=(1, 2)), "pix")
    contrast = density / (total / (L * L))[:, None, None] - 1.0
    near_local = jnp.cumsum(plane_coef[:, None, None] * contrast, axis=0)
    far_local = jnp.cumsum((plane_coef * plane_dist)[:, None, None] * contrast, axis=0)
    blank = jnp.zeros((slab, L), jnp.float32)
    near_before, far_before = entering(
        (near_local[-1], far_local[-1]), "shell", add_pairs, (blank, blank)
    )
    convergence = near_before + near_local - source_inv[:, None, None] * (far_before + far_local)
    cols_own = L // groups
    wave_x, keep_x = frequency_of(my_index * cols_own + jnp.arange(cols_own), L)
    wave_y, keep_y = frequency_of(jnp.arange(L), L)
    wave_x = wave_x[:, None]
    wave_y = wave_y[None, :]
    both_keep = keep_x[:, None] * keep_y[None, :]
    wave_power = jnp.maximum(wave_x * wave_x + wave_y * wave_y, 1.0)
    kernel_one = both_keep * (wave_x * wave_x - wave_y * wave_y) / wave_power
    kernel_two = both_keep * 2.0 * wave_x * wave_y / wave_power
    scale = 1.0 / (L * L)
    spec_real, spec_imag = transform_last(convergence[0::2], convergence[1::2], -1.0)
    sending = rows_to_sending(jnp.stack([spec_real, spec_imag], axis=1), groups, slab, cols_own)
    arrived = lax.all_to_all(sending, "pix", split_axis=0, concat_axis=0, tiled=True)
    columns = arrived_to_columns(arrived, groups, slab, cols_own)
    row_real, row_imag = transform_last(columns[:, 0], columns[:, 1], -1.0)
    first_real, first_imag = transform_last(row_real * kernel_one, row_imag * kernel_one, 1.0)
    second_real, second_imag = transform_last(row_real * kernel_two, row_imag * kernel_two, 1.0)
    stacked = jnp.stack([first_real, first_imag, second_real, second_imag], axis=1)
    landed = lax.all_to_all(
        columns_to_sending(stacked, groups, slab, cols_own),
        "pix",
        split_axis=0,
        concat_axis=0,
        tiled=True,
    )
    row_layout = landed_to_rows(landed, groups, slab, cols_own)
    even_one, odd_one = transform_last(row_layout[:, 0], row_layout[:, 1], 1.0)
    even_two, odd_two = transform_last(row_layout[:, 2], row_layout[:, 3], 1.0)
    shear_one = jnp.stack([even_one, odd_one], axis=1).reshape(planes, slab, L)
    shear_two = jnp.stack([even_two, odd_two], axis=1).reshape(planes, slab, L)
    return (convergence, shear_one * scale, shear_two * scale)


INNER = 128
OUTER = L // INNER
HALF_BLOCKS = OUTER // 2
CHUNKS = 4
SHARED = 3
ALONE_AT = 1
MESH = pl.DeviceIdType.MESH


def block_columns():
    cols = np.zeros((HALF_BLOCKS, INNER), np.int64)
    for b in range(HALF_BLOCKS - 1):
        cols[b] = b + 1 + OUTER * np.arange(INNER)
    half = np.arange(INNER // 2)
    cols[-1] = np.concatenate([OUTER * half, HALF_BLOCKS + OUTER * half])
    return cols


def split_table(table):
    high = table.astype(jnp.bfloat16)
    low = (table - high.astype(np.float64)).astype(jnp.bfloat16)
    return high, low


def row_tables(chunks):
    n2 = np.arange(INNER)
    out = np.zeros((HALF_BLOCKS, 2 * INNER, 2 * INNER))
    cols = block_columns()
    for b in range(HALF_BLOCKS):
        angle = 2 * np.pi / L * ((n2[:, None] * cols[b][None, :]) % L)
        co, si = np.cos(angle), np.sin(angle)
        if b < HALF_BLOCKS - 1:
            out[b] = np.block([[co, -si], [si, co]])
        else:
            h = INNER // 2
            out[b, :INNER, :h] = co[:, :h]
            out[b, :INNER, INNER : INNER + h] = -si[:, :h]
            out[b, INNER:, h:INNER] = co[:, h:]
            out[b, INNER:, INNER + h :] = -si[:, h:]
    out = out.reshape(HALF_BLOCKS, 2 * INNER, 2, chunks, INNER // chunks)
    return split_table(out.transpose(0, 3, 2, 4, 1).reshape(HALF_BLOCKS, 2 * INNER, 2 * INNER))


def row_order(slab):
    at = np.arange(slab)
    rows = slab // TR
    return (at % rows) * TR + at // rows


def column_table(order):
    idx = np.arange(INNER)
    angle = 2 * np.pi / INNER * ((idx[:, None] * order[None, :]) % INNER)
    co, si = np.cos(angle), np.sin(angle)
    return np.block([[co, si], [-si, co]])


def twiddle_tables(order):
    out = []
    for rows in (order, np.arange(INNER)):
        angle = 2 * np.pi / L * (np.arange(OUTER)[:, None] * rows[None, :])
        out += [np.cos(angle), -np.sin(angle)]
    return np.stack(out).astype(np.float32)


def times_root(value, k, n, sign):
    re, im = value
    k = k % n
    if k == 0:
        return value
    if 4 * k == n:
        return (-im, re) if sign > 0 else (im, -re)
    angle = 2 * math.pi * k / n
    c, s = math.cos(angle), sign * math.sin(angle)
    if 8 * k == n or 8 * k == 3 * n:
        if c > 0:
            return ((re - im) * c, (re + im) * c) if sign > 0 else ((re + im) * c, (im - re) * c)
        c = -c
        return ((re + im) * -c, (re - im) * c) if sign > 0 else ((im - re) * c, (re + im) * -c)
    return (re * c - im * s, re * s + im * c)


def fft_list(values, sign):
    n = len(values)
    if n == 1:
        return values
    even = fft_list(values[0::2], sign)
    odd = fft_list(values[1::2], sign)
    odd = [times_root(v, k, n, sign) for k, v in enumerate(odd)]
    return [(a[0] + b[0], a[1] + b[1]) for a, b in zip(even, odd)] + [
        (a[0] - b[0], a[1] - b[1]) for a, b in zip(even, odd)
    ]


def split_value(value):
    high = value.astype(jnp.bfloat16)
    return high, (value - high.astype(jnp.float32)).astype(jnp.bfloat16)


def three_pass(left, right, dims):
    dot = lambda a, b: lax.dot_general(a, b, (dims, ((), ())), preferred_element_type=jnp.float32)
    return dot(left[0], right[0]) + (dot(left[0], right[1]) + dot(left[1], right[0]))


def partners(me):
    steps = [(bit, bit - 2 * bit * ((me // bit) % 2)) for bit in (1, 2, 4, 8)]

    def flipped(mask):
        peer = me
        for bit, step in steps:
            if not isinstance(mask, int):
                peer = peer + ((mask // bit) % 2) * step
            elif mask & bit:
                peer = peer + step
        return peer

    return flipped


def fetch(pairs, sems):
    copies = [pltpu.make_async_copy(a, b, sems.at[i]) for i, (a, b) in enumerate(pairs)]
    for copy in copies:
        copy.start()
    return copies


def pack_kernel(tile_in, cell_in, mass_in, *refs):
    planes, tiles, per_tile = cell_in.shape
    out_refs = refs[:planes]
    tile_ref, cell_ref, mass_ref, wide, taken, sems = refs[planes:]
    copies = fetch(((tile_in, tile_ref), (cell_in, cell_ref), (mass_in, mass_ref)), sems)
    half = per_tile // TC
    size = 2 * half
    groups, rows, _ = out_refs[0].shape
    cap = rows // size - 1
    per_owner = L // groups // TR * (L // TC)
    me = lax.axis_index("pix")
    lane = lax.broadcasted_iota(jnp.int32, (1, TC), 1)
    for out_ref in out_refs:
        out_ref[...] = jnp.zeros_like(out_ref)
    for copy in copies:
        copy.wait()
    for p in range(planes):
        out_ref = out_refs[p]
        for i in range(half):
            at = slice(i * TC, (i + 1) * TC)
            wide[i] = cell_ref[p, :, at].astype(jnp.float32)
            wide[half + i] = mass_ref[p, :, at].astype(jnp.float32)
        total = jnp.sum(jnp.sum(wide[half:], axis=0), axis=0, keepdims=True)
        total = jnp.sum(total, axis=1, keepdims=True)
        tail = jnp.where(lane < cap, -1.0, jnp.where(lane == cap, total, 0.0))
        out_ref[:, cap * size :, :] = jnp.broadcast_to(tail[None], (groups, size, TC))

        def clear(o, _):
            taken[o] = 0
            return 0

        lax.fori_loop(0, groups, clear, 0)

        def tile(t, _):
            b = tile_ref[p, me * tiles + t]
            owner = b // per_owner
            rank = taken[owner]
            taken[owner] = rank + 1
            for i in range(size):
                out_ref[owner, pl.ds(rank * size + i, 1), :] = wide[i, pl.ds(t, 1), :]
            where_at = (b - owner * per_owner).astype(jnp.float32)
            old = out_ref[owner, cap * size : cap * size + 1, :]
            out_ref[owner, cap * size : cap * size + 1, :] = jnp.where(lane == rank, where_at, old)
            return 0

        lax.fori_loop(0, tiles, tile, 0, unroll=4)


def signal_all(peers):
    barrier = pltpu.get_barrier_semaphore()
    for peer in peers:
        pl.semaphore_signal(barrier, inc=1, device_id=peer, device_id_type=MESH)
    pl.semaphore_wait(barrier, len(peers))


def remote(source, target, send, recv, peer):
    return pltpu.make_async_remote_copy(
        src_ref=source,
        dst_ref=target,
        send_sem=send,
        recv_sem=recv,
        device_id=peer,
        device_id_type=MESH,
    )


def lensing_kernel(
    out0, out1, coef_in, dist_in, inv_in, twist_ref, high_ref, low_ref, colh_ref, coll_ref, backh_ref, backl_ref,
    conv_ref, one_ref, two_ref,
    coef_ref, dist_ref, inv_ref, tsem, note, far_note, note_sems,
    box, slots, place, field, held_row, sending, arrived, held, kern, back, leaving, landed, total_rows,
    lsend, lrecv, psend, precv, fsend, frecv, rsend, rrecv,
):
    out_refs = (out0, out1)
    planes = 2
    groups, message, _ = out0.shape
    slab = L // groups
    half = 4
    size = 2 * half
    cap = message // size - 1
    chunks = sending.shape[1]
    span = INNER // chunks
    single = chunks - SHARED
    units = chunks + SHARED
    flip = groups // 2
    pitch = slots.shape[1] // (cap * groups)
    tile_rows = slab // TR
    me, shell = lax.axis_index("pix"), lax.axis_index("shell")
    flipped = partners(me)
    factors = fetch(((coef_in, coef_ref), (dist_in, dist_ref), (inv_in, inv_ref)), tsem)
    for copy in factors:
        copy.wait()
    note[...] = jnp.zeros_like(note)
    for p in range(planes):
        note[p : p + 1, :] = jnp.full((1, TC), coef_ref[p], jnp.float32)
        note[planes + p : planes + p + 1, :] = jnp.full((1, TC), dist_ref[p], jnp.float32)
    signal_all([{"pix": flipped(m)} for m in range(1, groups)] + [{"shell": 1 - shell}])

    sent = pl.ds(0, cap * size + 1)

    def direct(p, m):
        peer = flipped(m)
        return remote(
            out_refs[p].at[peer, sent], box.at[p, me, sent], lsend.at[p, m], lrecv.at[p, m], {"pix": peer}
        )

    def landing(p, m):
        peer = flipped(m)
        return remote(
            out_refs[p].at[peer, sent], box.at[p, peer, sent], lsend.at[p, m], lrecv.at[p, m], {"pix": peer}
        )

    def onward(p, m):
        source = flipped(m)
        first = out_refs[p].at[me, sent] if isinstance(m, int) and m == 0 else box.at[p, source, sent]
        return remote(first, box.at[planes + p, source, sent], psend.at[p, m], precv.at[p, m], {"shell": 1 - shell})

    for m in range(1, groups):
        for p in range(planes):
            direct(p, m).start()
    told = remote(note, far_note, note_sems.at[0], note_sems.at[1], {"shell": 1 - shell})
    told.start()
    for p in range(planes):
        onward(p, 0).start()
        box[p, me] = out_refs[p][me]

    own_lines, mirror_lines = column_info(me), column_info((me + flip) % groups)
    signed_v, weight = (
        jnp.concatenate([ours, theirs[single * span :]], axis=0)
        for ours, theirs in zip(own_lines, mirror_lines)
    )
    inner_id = lax.broadcasted_iota(jnp.int32, (units * span, INNER), 1)

    def prepare(k, _):
        u = k + OUTER * inner_id
        signed_u = jnp.where(u >= L // 2, u - L, u).astype(jnp.float32)
        scale = jnp.where(u == L // 2, 0.0, weight)
        uu, vv = signed_u * signed_u, signed_v * signed_v
        over = scale / jnp.maximum(uu + vv, 1.0)
        kern[0, k] = (vv - uu) * over
        kern[1, k] = 2.0 * signed_v * signed_u * over
        return 0

    as_small = lambda ids: ids.astype(jnp.float32).astype(jnp.bfloat16)
    short, narrow = 2 * TR, TC // 2
    row_id = as_small(lax.broadcasted_iota(jnp.int32, (short, TC), 0))
    col_id = as_small(lax.broadcasted_iota(jnp.int32, (narrow, TC), 0))
    one, zero = jnp.ones((), jnp.bfloat16), jnp.zeros((), jnp.bfloat16)

    def deposit(q, s):
        for c in range(cap):
            entry = box[q, s, c * size : (c + 1) * size, :]
            cells = entry[:half].astype(jnp.int32)
            cell_rows = as_small(cells // TC + TR * ((cells // narrow) % 2))
            cell_cols = as_small(cells % narrow)
            weights = entry[half:].astype(jnp.bfloat16)
            row_hot, col_hot = [], []
            for i in range(half):
                row_hot.append(jnp.where(row_id == cell_rows[i : i + 1], weights[i : i + 1], zero))
                col_hot.append(jnp.where(col_id == cell_cols[i : i + 1], one, zero))
            sums = lax.dot_general(
                jnp.concatenate(row_hot, axis=1),
                jnp.concatenate(col_hot, axis=1),
                (((1,), (1,)), ((), ())),
                preferred_element_type=jnp.float32,
            )
            at = pl.ds(pl.multiple_of((c * groups + s) * pitch, 8), TR)
            slots[q, at, :] = jnp.concatenate([sums[:TR], sums[TR:]], axis=1)

    def near_block(m):
        def one_plane(p, _):
            deposit(p, flipped(m))
            return 0

        lax.fori_loop(0, planes, one_plane, 0)

    def far_block(m):
        for p in range(planes):
            onward(p, m).wait_recv()

        def one_plane(p, _):
            deposit(planes + p, flipped(m))
            return 0

        lax.fori_loop(0, planes, one_plane, 0)

    def take(m):
        for p in range(planes):
            landing(p, m).wait_recv()
            onward(p, m).start()

    lag = 2
    near_block(0)

    def early(m, _):
        take(m)
        near_block(m)
        return 0

    lax.fori_loop(1, lag, early, 0)

    def steady(m, _):
        take(m)
        near_block(m)
        far_block(m - lag)
        return 0

    lax.fori_loop(lag, groups, steady, 0)

    def late(m, _):
        far_block(m)
        return 0

    lax.fori_loop(groups - lag, groups, late, 0)

    told.wait_recv()
    lane_id = lax.broadcasted_iota(jnp.int32, (groups, TC), 1)
    tile_id = ((lane_id % tile_rows) * OUTER + lane_id // tile_rows).astype(jnp.float32)
    gains, shifts = [[], []], [0.0, 0.0]
    for q in range(2 * planes):
        tails = box[q, :, cap * size, :]
        hot = [jnp.where(tails[:, c : c + 1] == tile_id, 1.0, 0.0) for c in range(cap)]
        place[q] = jnp.concatenate(hot, axis=0).T.astype(jnp.bfloat16)
        total = jnp.sum(tails[:, cap : cap + 1], axis=0, keepdims=True)
        notes, p = (note, q) if q < planes else (far_note, q - planes)
        coef, dist = notes[p : p + 1, 0:1], notes[planes + p : planes + p + 1, 0:1]
        for i in range(planes):
            mixed = coef * (1.0 - inv_ref[i] * dist)
            if q >= planes:
                mixed = jnp.where(shell > 0, mixed, 0.0)
            elif q > i:
                mixed = jnp.zeros_like(mixed)
            gains[i].append(mixed * ((L * L) / total))
            shifts[i] = shifts[i] + mixed

    peers = groups - 1

    def go(c, peer):
        source = sending.at[peer, c] if c < chunks else sending.at[(peer + flip) % groups, c - SHARED]
        return remote(source, arrived.at[me, c], fsend.at[c], frecv.at[c], {"pix": peer})

    def go_all(c):
        every = pl.ds(0, peers)
        return remote(
            sending.at[every, 0], arrived.at[every, c], fsend.at[c], frecv.at[c], {"pix": flipped(1)}
        )

    def home_any(c, count=peers):
        every = pl.ds(0, count)
        return remote(
            leaving.at[every, c], landed.at[every, 0], rsend.at[c], rrecv.at[c], {"pix": flipped(1)}
        )

    def home_all(c):
        return home_any(c, peers if c < single else flip - 1)

    def field_rows(r, n):
        return pl.ds(pl.multiple_of(r * TC + n * tile_rows, tile_rows), tile_rows)

    def mass_rows(j, _):
        r = 2 * j
        sums = []
        for q in range(2 * planes):
            pair = jnp.concatenate(
                [slots[q, pl.ds(r + i, cap * groups, stride=pitch), :] for i in range(2)], axis=1
            )
            high = pair.astype(jnp.bfloat16)
            rest = pair - high.astype(jnp.float32)
            middle = rest.astype(jnp.bfloat16)
            low = (rest - middle.astype(jnp.float32)).astype(jnp.bfloat16)
            dot = lambda part: jnp.dot(place[q], part, preferred_element_type=jnp.float32)
            sums.append(dot(high) + (dot(middle) + dot(low)))
        for i in range(planes):
            value = gains[i][0] * sums[0]
            for q in range(1, 2 * planes):
                value = value + gains[i][q] * sums[q]
            value = value - shifts[i]
            for e in range(2):
                at = pl.ds(pl.multiple_of((r + e) * TC, TC), TC)
                field[i, at, :] = value[:, e * TC : (e + 1) * TC]
        return 0

    lax.fori_loop(0, TR // 2, mass_rows, 0)

    def row_radix(r, _):
        near = pl.ds(pl.multiple_of(r * tile_rows, tile_rows), tile_rows)
        z = fft_list(
            [tuple(field[i, field_rows(r, n), :] for i in range(2)) for n in range(OUTER)], -1
        )
        for k in range(1, HALF_BLOCKS):
            (ar, ai), (br, bi) = z[k], z[OUTER - k]
            held_row[k - 1, 0, near, :INNER] = 0.5 * (ar + br)
            held_row[k - 1, 0, near, INNER:] = 0.5 * (ai - bi)
            held_row[k - 1, 1, near, :INNER] = 0.5 * (ai + bi)
            held_row[k - 1, 1, near, INNER:] = 0.5 * (br - ar)
        for p in range(2):
            held_row[HALF_BLOCKS - 1, p, near, :INNER] = z[0][p]
            held_row[HALF_BLOCKS - 1, p, near, INNER:] = z[HALF_BLOCKS][p]
        return 0

    lax.fori_loop(0, TR, row_radix, 0)

    def row_block(b):
        value = held_row[b].reshape(2 * slab, 2 * INNER)
        result = three_pass((high_ref[b], low_ref[b]), split_value(value), ((1,), (1,)))
        for p in range(2):
            for c in range(chunks):
                sending[2 * b + p, c] = result[
                    2 * span * c : 2 * span * (c + 1), p * slab : (p + 1) * slab
                ]

    order = [(single + i, chunks + i) for i in range(SHARED)]
    order[ALONE_AT:ALONE_AT] = [(c,) for c in range(single)]

    def send_block(j, _):
        b = (me // 2 + 1 + j) % HALF_BLOCKS
        row_block(b)
        for p in range(2):
            for c in order[0]:
                peer = 2 * b + p if c < chunks else (2 * b + p + flip) % groups
                pl.when(peer != me)(lambda: go(c, peer).start())
        return 0

    lax.fori_loop(0, HALF_BLOCKS, send_block, 0)
    for c in [c for group in order[1:] for c in group]:
        for m in range(1, groups):
            go(c, flipped(m)).start()
    for c in range(chunks):
        arrived[me, c] = sending[me, c]
    for c in range(chunks, units):
        arrived[me, c] = sending[(me + flip) % groups, c - SHARED]

    def show(t, _):
        for i in range(planes):
            for n in range(OUTER):
                for r in range(0, TR, 8):
                    rows = pl.ds(pl.multiple_of(t * TR + r, 8), 8)
                    held_at = pl.ds(r * TC + n * tile_rows + t, 8, stride=TC)
                    conv_ref[i, rows, n * TC : (n + 1) * TC] = field[i, held_at, :]
        return 0

    lax.fori_loop(0, OUTER, prepare, 0)

    def columns(c):
        for t in range(span // 8):
            at, past = slice(t * 8, t * 8 + 8), slice(span + t * 8, span + t * 8 + 8)
            z = fft_list([(arrived[n, c, at, :], arrived[n, c, past, :]) for n in range(OUTER)], -1)
            for k in range(OUTER):
                re, im = z[k]
                if k:
                    cs, sn = twist_ref[0, k : k + 1, :], twist_ref[1, k : k + 1, :]
                    re, im = re * cs - im * sn, re * sn + im * cs
                rows = slice(k * span + t * 8, k * span + t * 8 + 8)
                held[rows, :INNER] = re
                held[rows, INNER:] = im
        rank = pl.ds(pl.multiple_of(c * span, span), span)
        part = 2 * INNER // span
        for g in range(OUTER // part):
            value = held[g * part * span : (g + 1) * part * span, :]
            spectrum = three_pass(split_value(value), (colh_ref[...], coll_ref[...]), ((1,), (0,)))
            for f in range(2):
                gain = kern[f, g * part : (g + 1) * part, rank, :].reshape(part * span, INNER)
                shaped = spectrum * jnp.concatenate([gain, gain], axis=1)
                result = three_pass(split_value(shaped), (backh_ref[...], backl_ref[...]), ((1,), (0,)))
                for i in range(part):
                    k = g * part + i
                    re, im = result[i * span : (i + 1) * span, :INNER], result[i * span : (i + 1) * span, INNER:]
                    cs, sn = twist_ref[2, k : k + 1, :], twist_ref[3, k : k + 1, :]
                    back[f, k, :, :INNER] = re * cs + im * sn
                    back[f, k, :, INNER:] = im * cs - re * sn
        for f in range(2):
            for t in range(span // 8):
                at, past = slice(t * 8, t * 8 + 8), slice(span + t * 8, span + t * 8 + 8)
                x = fft_list([(back[f, k, at, :INNER], back[f, k, at, INNER:]) for k in range(OUTER)], 1)
                for n in range(OUTER):
                    leaving[n, c, f, at, :] = x[n][0]
                    leaving[n, c, f, past, :] = x[n][1]

    def send_home(c, masks, slot):
        for m in masks:
            peer = flipped(m)
            remote(
                leaving.at[peer, c], landed.at[slot[0], slot[1]], rsend.at[c], rrecv.at[c], {"pix": peer}
            ).start()
        landed[slot[0], slot[1]] = leaving[me, c]

    def shared_columns(j, _):
        c = single + j // 2 + (j % 2) * SHARED
        go_all(c).wait_recv()
        columns(c)
        send_home(c, range(1, flip), ((me + (j % 2) * flip) % groups, single + j // 2))
        return 0

    def single_columns(c, _):
        go_all(c).wait_recv()
        columns(c)
        send_home(c, range(1, groups), (me, c))
        return 0

    lax.fori_loop(0, 2 * ALONE_AT, shared_columns, 0)
    lax.fori_loop(0, single, single_columns, 0)
    lax.fori_loop(2 * ALONE_AT, 2 * SHARED, shared_columns, 0)
    lax.fori_loop(0, tile_rows, show, 0)
    for c in range(units):
        go_all(c).wait_send()
    told.wait_send()
    for p in range(planes):
        onward(p, 0).wait_send()

        def settle(m, _):
            direct(p, m).wait_send()
            onward(p, m).wait_send()
            return 0

        lax.fori_loop(1, groups, settle, 0)

    def gather(c, first):
        def block(b, _):
            at = pl.ds(pl.multiple_of(c * 2 * span, 2 * span), 2 * span)
            high, low = high_ref[b, at, :], low_ref[b, at, :]
            table = jnp.concatenate([high, high, low], axis=0)
            for f in range(2):
                value = jnp.concatenate([landed[2 * b + p, c, f] for p in range(2)], axis=1)
                top, rest = split_value(value)
                result = lax.dot_general(
                    jnp.concatenate([top, rest, top], axis=0),
                    table,
                    (((0,), (0,)), ((), ())),
                    preferred_element_type=jnp.float32,
                ).reshape(2, slab, 2 * INNER)
                total_rows[f, b] = result if first else total_rows[f, b] + result
            return 0

        lax.fori_loop(0, HALF_BLOCKS, block, 0)

    for at, group in enumerate(order):
        for c in group:
            home_all(c).wait_recv()
        gather(group[0], at == 0)
    for f, out_ref in enumerate((one_ref, two_ref)):

        def radix(t, _):
            rows = pl.ds(pl.multiple_of(t * 8, 8), 8)
            at = lambda k, p, part: total_rows[f, k, p, rows, part * INNER : (part + 1) * INNER]
            z = [None] * OUTER
            last = HALF_BLOCKS - 1
            z[0] = (at(last, 0, 0), at(last, 1, 0))
            z[HALF_BLOCKS] = (at(last, 0, 1), at(last, 1, 1))
            for k in range(1, HALF_BLOCKS):
                ar, ai = at(k - 1, 0, 0), at(k - 1, 0, 1)
                br, bi = at(k - 1, 1, 0), at(k - 1, 1, 1)
                z[k] = (ar - bi, ai + br)
                z[OUTER - k] = (ar + bi, br - ai)
            x = fft_list(z, 1)
            for n in range(OUTER):
                for p in range(2):
                    out_ref[p, rows, n * INNER : (n + 1) * INNER] = x[n][p]
            return 0

        lax.fori_loop(0, slab // 8, radix, 0)
    for c in range(units):
        home_all(c).wait_send()


def place_kernel(*refs):
    count = (len(refs) - 1) // 2
    for copy in fetch(zip(refs[:count], refs[count:-1]), refs[-1]):
        copy.wait()


def column_info(me):
    line = lax.broadcasted_iota(jnp.int32, (INNER, INNER), 0)
    b = me // 2
    last = b == HALF_BLOCKS - 1
    upper = line // (INNER // 2)
    folded = OUTER * (line - upper * (INNER // 2)) + HALF_BLOCKS * upper
    mine = jnp.where(last, folded, b + 1 + OUTER * line)
    weight = jnp.where(last & (mine > 0), 2.0, 1.0) / (L * L)
    return jnp.where(mine >= L // 2, mine - L, mine).astype(jnp.float32), weight


def call(body, outs, scratch=(), smem=(0,), count=1, megabytes=48, flops=0, group=None, hbm=(), out_space=pltpu.VMEM):
    space = [
        pl.BlockSpec(
            memory_space=pltpu.SMEM if i in smem else pltpu.HBM if i in hbm else pltpu.VMEM
        )
        for i in range(count)
    ]
    return pl.pallas_call(
        body,
        out_shape=outs,
        in_specs=space,
        out_specs=jax.tree.map(lambda _: pl.BlockSpec(memory_space=out_space), outs),
        scratch_shapes=list(scratch),
        compiler_params=pltpu.CompilerParams(
            vmem_limit_bytes=megabytes << 20,
            collective_id=group,
            has_side_effects=group is not None,
        ),
        cost_estimate=pl.CostEstimate(flops=flops, bytes_accessed=4 << 20, transcendentals=0),
    )


def shape(*dims):
    return jax.ShapeDtypeStruct(dims, jnp.float32)


def local_fast(block_tile, cell_index, masses, plane_coef, plane_dist, source_inv):
    groups = lax.axis_size("pix")
    planes, local_tiles, per_tile = cell_index.shape
    slab = L // groups
    cap = max(1, 2 * local_tiles // groups)
    size = 2 * per_tile // TC
    message = (cap + 1) * size
    vmem = lambda *dims: pltpu.VMEM(dims, jnp.float32)
    dma = lambda *dims: pltpu.SemaphoreType.DMA(dims)
    outgoing = call(
        pack_kernel,
        [shape(groups, message, TC)] * planes,
        [
            pltpu.SMEM(block_tile.shape, jnp.int32),
            pltpu.VMEM(cell_index.shape, jnp.int32),
            pltpu.VMEM(masses.shape, jnp.bfloat16),
            vmem(size, local_tiles, TC),
            pltpu.SMEM((groups,), jnp.int32),
            dma(3),
        ],
        smem=(),
        hbm=(0, 1, 2),
        count=3,
        megabytes=16,
        flops=1 << 32,
    )(block_tile, cell_index, masses)

    order = row_order(slab)
    row_high, row_low = row_tables(CHUNKS)
    col_high, col_low = split_table(column_table(order).T)
    back_high, back_low = split_table(column_table(np.arange(INNER)))
    span = INNER // CHUNKS
    pitch = 3 * TR // 2
    tables = [jnp.asarray(twiddle_tables(order)), row_high, row_low, col_high, col_low, back_high, back_low]
    results = call(
        lensing_kernel,
        [shape(planes, slab, L)] * 3,
        [pltpu.SMEM(source_inv.shape, jnp.float32)] * 3
        + [
            dma(3),
            vmem(8, TC),
            vmem(8, TC),
            dma(2),
            vmem(2 * planes, groups, message, TC),
            vmem(2 * planes, cap * groups * pitch, TC),
            pltpu.VMEM((2 * planes, TC, TC), jnp.bfloat16),
            vmem(planes, TR * TC, TC),
            vmem(HALF_BLOCKS, planes, slab, 2 * INNER),
            vmem(groups, CHUNKS, 2 * span, slab),
            vmem(groups, CHUNKS + SHARED, 2 * span, slab),
            vmem(OUTER * span, 2 * INNER),
            vmem(2, OUTER, INNER + SHARED * span, INNER),
            vmem(2, OUTER, span, 2 * INNER),
            vmem(groups, CHUNKS + SHARED, 2, 2 * span, slab),
            vmem(groups, CHUNKS, 2, 2 * span, slab),
            vmem(2, HALF_BLOCKS, planes, slab, 2 * INNER),
            dma(planes, groups),
            dma(planes, groups),
            dma(planes, groups),
            dma(planes, groups),
            dma(CHUNKS + SHARED),
            dma(CHUNKS + SHARED),
            dma(CHUNKS + SHARED),
            dma(CHUNKS + SHARED),
        ],
        smem=(),
        hbm=(2, 3, 4),
        count=12,
        megabytes=40,
        flops=1 << 32,
        group=0,
    )(*outgoing, plane_coef, plane_dist, source_inv, *tables)
    return call(
        place_kernel,
        [shape(planes, slab, L)] * 3,
        [dma(3)],
        smem=(),
        out_space=pltpu.HBM,
        count=3,
        megabytes=16,
        flops=1 << 20,
    )(*results)


def solution(mesh):
    placed = (
        P("shell", None),
        P("shell", "pix", None),
        P("shell", "pix", None),
        P("shell"),
        P("shell"),
        P("shell"),
    )
    shells, groups = mesh.shape["shell"], mesh.shape["pix"]

    def body(block_tile, cell_index, *rest):
        fits = (
            shells == 2
            and cell_index.shape[0] == 2
            and groups == OUTER
            and cell_index.shape[2] == 4 * TC
            and cell_index.shape[1] * 2 == groups * 8
        )
        return (local_fast if fits else local)(block_tile, cell_index, *rest)

    return jax.shard_map(
        body,
        mesh=mesh,
        in_specs=placed,
        out_specs=(P("shell", "pix", None), P("shell", "pix", None), P("shell", "pix", None)),
        check_vma=False,
    )
```
